128 devices in a mesh: data: 1, chip: 2 (over core), dap: 64 (over z, y, x).
Axes of the slice: x: 4, y: 4, z: 4, core: 2. Of those that a mesh axis runs over, the one named last changes fastest.
Arguments:
- m: bfloat16 [2048, 128, 256], P(('data', 'chip', 'dap'))
- z: bfloat16 [128, 128, 128], P(('data', 'chip', 'dap'))
- msa_mask: int32 [2048, 128], P('data')
- res_mask: int32 [128], P('data')
- w_row_in: bfloat16 [256, 1024], replicated
- w_row_bias: bfloat16 [128, 8], replicated
- w_row_out: bfloat16 [256, 256], replicated
- w_col_in: bfloat16 [256, 1024], replicated
- w_col_out: bfloat16 [256, 256], replicated
- w_opm_in: bfloat16 [256, 64], replicated
- w_opm_out: bfloat16 [1024, 128], replicated
- w_start_in: bfloat16 [128, 512], replicated
- w_start_bias: bfloat16 [128, 4], replicated
- w_start_out: bfloat16 [128, 128], replicated
- w_end_in: bfloat16 [128, 512], replicated
- w_end_bias: bfloat16 [128, 4], replicated
- w_end_out: bfloat16 [128, 128], replicated
Outputs:
- output 1: bfloat16 [2048, 128, 256], P(('data', 'chip', 'dap'))
- output 2: bfloat16 [128, 128, 128], P(('data', 'chip', 'dap'))
All inputs are finite; a program needn't handle non-finite values.
Results may differ from the reference program's by a relative error of at most 0.0148384.
Values are sent between devices in bfloat16 or wider.
A program may use at most 1 GiB of HBM per device.

```python
import jax
import jax.numpy as jnp
from jax import lax

NUM_SEQ = 2048
NUM_RES = 128
C_M = 256
C_Z = 128
HEADS_M = 8
HEAD_M = 32
HEADS_T = 4
HEAD_T = 32
OPM = 32


def layer_norm(x):
    values = x.astype(jnp.float32)
    centred = values - jnp.mean(values, axis=-1, keepdims=True)
    variance = jnp.mean(centred * centred, axis=-1, keepdims=True)
    return (centred * lax.rsqrt(variance + 1e-5)).astype(jnp.bfloat16)


def project(x, weight):
    return jnp.dot(x, weight, preferred_element_type=jnp.float32).astype(jnp.bfloat16)


def add_residual(state, update):
    return (state.astype(jnp.float32) + update).astype(jnp.bfloat16)


def gated_rows(projected, head_bias, key_ok, heads, head_dim):
    length = projected.shape[0]
    split_proj = projected.reshape(length, 4, heads, head_dim).astype(jnp.float32)
    scores = jnp.einsum('ihd,jhd->hij', split_proj[:, 0], split_proj[:, 1]) * head_dim ** -0.5
    if head_bias is not None:
        scores = scores + head_bias.astype(jnp.float32)
    scores = jnp.where(key_ok[None, None, :], scores, -1e9)
    attn_prob = jax.nn.softmax(scores, axis=-1).astype(jnp.bfloat16).astype(jnp.float32)
    mixed = jnp.einsum('hij,jhd->ihd', attn_prob, split_proj[:, 2])
    gated = (mixed * jax.nn.sigmoid(split_proj[:, 3])).astype(jnp.bfloat16)
    return gated.reshape(length, heads * head_dim)


def draw_masks(mask_key):
    seq_key, res_key = jax.random.split(mask_key)
    seq_idx = jnp.arange(NUM_SEQ)[:, None]
    res_idx = jnp.arange(NUM_RES)
    msa_draw = jax.random.randint(seq_key, (NUM_SEQ, NUM_RES), 0, 4)
    msa_mask = ((msa_draw != 0) | (seq_idx == 0) | (res_idx[None, :] == 0)).astype(jnp.int32)
    res_draw = jax.random.randint(res_key, (NUM_RES,), 0, 4)
    res_mask = ((res_draw != 0) | (res_idx == 0)).astype(jnp.int32)
    return msa_mask, res_mask


def dense(weight_key, rows, cols, gain):
    draw = jax.random.normal(weight_key, (rows, cols), jnp.float32)
    return (draw * (gain * rows ** -0.5)).astype(jnp.bfloat16)


def attn_in(weight_key, rows, heads, head_dim):
    draw = jax.random.normal(weight_key, (rows, 4, heads * head_dim), jnp.float32)
    boost = jnp.array([1.5, 1.5, 1.0, 1.0], jnp.float32)[None, :, None]
    return (draw * boost * rows ** -0.5).reshape(rows, 4 * heads * head_dim).astype(jnp.bfloat16)


def setup_inputs(seed: int = 0, part: int = 0) -> dict:
    part_keys = jax.random.split(jax.random.fold_in(jax.random.key(seed), part), 4)
    weight_keys = jax.random.split(jax.random.key(seed + 1), 13)
    profile = jax.random.normal(part_keys[0], (1, NUM_RES, C_M), jnp.float32)
    noise = jax.random.normal(part_keys[1], (NUM_SEQ, NUM_RES, C_M), jnp.float32)
    pair = jax.random.normal(part_keys[2], (NUM_RES, NUM_RES, C_Z), jnp.float32)
    msa_mask, res_mask = draw_masks(part_keys[3])
    return {
        'm': (profile + noise).astype(jnp.bfloat16),
        'z': pair.astype(jnp.bfloat16),
        'msa_mask': msa_mask,
        'res_mask': res_mask,
        'w_row_in': attn_in(weight_keys[0], C_M, HEADS_M, HEAD_M),
        'w_row_bias': dense(weight_keys[1], C_Z, HEADS_M, 1.5),
        'w_row_out': dense(weight_keys[2], HEADS_M * HEAD_M, C_M, 1.0),
        'w_col_in': attn_in(weight_keys[3], C_M, HEADS_M, HEAD_M),
        'w_col_out': dense(weight_keys[4], HEADS_M * HEAD_M, C_M, 1.0),
        'w_opm_in': dense(weight_keys[5], C_M, 2 * OPM, 1.0),
        'w_opm_out': dense(weight_keys[6], OPM * OPM, C_Z, 1.0),
        'w_start_in': attn_in(weight_keys[7], C_Z, HEADS_T, HEAD_T),
        'w_start_bias': dense(weight_keys[8], C_Z, HEADS_T, 1.5),
        'w_start_out': dense(weight_keys[9], HEADS_T * HEAD_T, C_Z, 1.0),
        'w_end_in': attn_in(weight_keys[10], C_Z, HEADS_T, HEAD_T),
        'w_end_bias': dense(weight_keys[11], C_Z, HEADS_T, 1.5),
        'w_end_out': dense(weight_keys[12], HEADS_T * HEAD_T, C_Z, 1.0),
    }


def reference(m, z, msa_mask, res_mask, w_row_in, w_row_bias, w_row_out, w_col_in, w_col_out,
              w_opm_in, w_opm_out, w_start_in, w_start_bias, w_start_out, w_end_in, w_end_bias, w_end_out):
    msa_ok = msa_mask != 0
    res_ok = res_mask != 0

    row_bias = jnp.transpose(project(layer_norm(z), w_row_bias), (2, 0, 1))
    row_proj = project(layer_norm(m), w_row_in)

    def row_step(step_in):
        return gated_rows(step_in[0], row_bias, step_in[1], HEADS_M, HEAD_M)

    row_gated = lax.map(row_step, (row_proj, msa_ok))
    m = add_residual(m, jnp.dot(row_gated, w_row_out, preferred_element_type=jnp.float32))

    col_proj = jnp.swapaxes(project(layer_norm(m), w_col_in), 0, 1)

    def col_step(step_in):
        return gated_rows(step_in[0], None, step_in[1], HEADS_M, HEAD_M)

    col_gated = jnp.swapaxes(lax.map(col_step, (col_proj, msa_ok.T)), 0, 1)
    m = add_residual(m, jnp.dot(col_gated, w_col_out, preferred_element_type=jnp.float32))

    outer_proj = project(layer_norm(m), w_opm_in)
    mask_w = msa_mask.astype(jnp.bfloat16)
    left = outer_proj[:, :, :OPM] * mask_w[:, :, None]
    right = (outer_proj[:, :, OPM:] * mask_w[:, :, None]).astype(jnp.float32)
    pair_norm = jnp.dot(mask_w.T, mask_w, preferred_element_type=jnp.float32)

    def outer_step(step_in):
        outer = jnp.einsum('sa,sjc->jac', step_in[0].astype(jnp.float32), right).astype(jnp.bfloat16)
        mapped = jnp.dot(outer.reshape(NUM_RES, OPM * OPM), w_opm_out, preferred_element_type=jnp.float32)
        return mapped / (1e-3 + step_in[1][:, None])

    z = add_residual(z, lax.map(outer_step, (jnp.swapaxes(left, 0, 1), pair_norm)))

    start_norm = layer_norm(z)
    start_proj = project(start_norm, w_start_in)
    start_bias = jnp.transpose(project(start_norm, w_start_bias), (2, 0, 1))

    def start_step(row_in):
        return gated_rows(row_in, start_bias, res_ok, HEADS_T, HEAD_T)

    start_gated = lax.map(start_step, start_proj)
    z = add_residual(z, jnp.dot(start_gated, w_start_out, preferred_element_type=jnp.float32))

    end_norm = layer_norm(z)
    end_proj = jnp.swapaxes(project(end_norm, w_end_in), 0, 1)
    end_bias = jnp.transpose(project(end_norm, w_end_bias), (2, 1, 0))

    def end_step(col_in):
        return gated_rows(col_in, end_bias, res_ok, HEADS_T, HEAD_T)

    end_gated = jnp.swapaxes(lax.map(end_step, end_proj), 0, 1)
    z = add_residual(z, jnp.dot(end_gated, w_end_out, preferred_element_type=jnp.float32))
    return m, z
```

```python
import jax
import jax.numpy as jnp
from jax import lax
from jax.sharding import PartitionSpec as P


def layer_norm(x):
    values = x.astype(jnp.float32)
    centred = values - jnp.mean(values, axis=-1, keepdims=True)
    variance = jnp.mean(centred * centred, axis=-1, keepdims=True)
    return (centred * lax.rsqrt(variance + 1e-5)).astype(jnp.bfloat16)


def add_residual(state, update):
    return (state.astype(jnp.float32) + update).astype(jnp.bfloat16)


def gated_attention(x_norm, w_in, w_out, heads, head_bias, key_ok, along_first):
    width = x_norm.shape[-1]
    head_dim = w_out.shape[0] // heads
    w_heads = jnp.transpose(w_in.reshape(width, 4, heads, head_dim), (2, 0, 1, 3))
    w_back = w_out.reshape(heads, head_dim, w_out.shape[1])
    if along_first:
        forms = ('nbc,cfd->nbfd', 'ibd,jbd->bij', 'bij,jbd->ibd', 'hibd,hdc->ibc')
    else:
        forms = ('bnc,cfd->bnfd', 'bid,bjd->bij', 'bij,bjd->bid', 'hbid,hdc->bic')
    key_keep = key_ok[:, None, :]
    scale = head_dim ** -0.5

    def one_head(head_in):
        projected = jnp.einsum(forms[0], x_norm, head_in[0], preferred_element_type=jnp.float32).astype(jnp.bfloat16)
        scores = jnp.einsum(forms[1], projected[:, :, 0], projected[:, :, 1], preferred_element_type=jnp.float32) * scale
        if len(head_in) > 1:
            scores = scores + head_in[1].astype(jnp.float32)[None]
        scores = jnp.where(key_keep, scores, -1e9)
        attn_prob = jax.nn.softmax(scores, axis=-1).astype(jnp.bfloat16)
        mixed = jnp.einsum(forms[2], attn_prob, projected[:, :, 2], preferred_element_type=jnp.float32)
        return (mixed * jax.nn.sigmoid(projected[:, :, 3].astype(jnp.float32))).astype(jnp.bfloat16)

    head_in = (w_heads,) if head_bias is None else (w_heads, head_bias)
    gated = lax.map(one_head, head_in)
    return jnp.einsum(forms[3], gated, w_back, preferred_element_type=jnp.float32)


def gather_rows(block, group, size):
    spread = jnp.broadcast_to(block[None], (size,) + block.shape)
    spread = lax.all_to_all(spread, group, 0, 0, tiled=True)
    return jnp.moveaxis(spread[:, :, 0], 0, 1)


def solution(mesh):
    dap_size = mesh.shape['dap']
    group = ('chip', 'dap')
    group_size = mesh.shape['chip'] * dap_size
    rows = P(('data', 'chip', 'dap'))
    in_specs = (rows, rows, P('data'), P('data')) + (P(),) * 13

    def per_device(m_blk, z_blk, value_a8, res_mask, w_row_in, w_row_bias, w_row_out, w_col_in, w_col_out,
                   w_opm_in, w_opm_out, w_start_in, w_start_bias, w_start_out, w_end_in, w_end_bias, w_end_out):
        group_idx = lax.axis_index('chip') * dap_size + lax.axis_index('dap')
        seq_loc = m_blk.shape[0]
        res_loc = z_blk.shape[0]
        heads_m = w_row_bias.shape[1]
        heads_t = w_start_bias.shape[1]
        opm = w_opm_in.shape[1] // 2
        value_a6 = value_a8 != 0
        res_ok = (res_mask != 0)[None, :]

        row_bias = jnp.einsum('ijc,ch->hij', layer_norm(z_blk), w_row_bias, preferred_element_type=jnp.float32).astype(jnp.bfloat16)
        row_bias = gather_rows(row_bias, group, group_size)
        seq_ok = lax.dynamic_slice_in_dim(value_a6, group_idx * seq_loc, seq_loc, axis=0)
        m_blk = add_residual(m_blk, gated_attention(layer_norm(m_blk), w_row_in, w_row_out, heads_m, row_bias, seq_ok, False))

        m_cols = lax.all_to_all(m_blk, group, 1, 0, tiled=True)
        col_mask = lax.dynamic_slice_in_dim(value_a8, group_idx * res_loc, res_loc, axis=1)
        m_cols = add_residual(m_cols, gated_attention(layer_norm(m_cols), w_col_in, w_col_out, heads_m, None, (col_mask != 0).T, True))

        outer_proj = jnp.dot(layer_norm(m_cols), w_opm_in, preferred_element_type=jnp.float32).astype(jnp.bfloat16)
        col_w = col_mask.astype(jnp.bfloat16)
        left = outer_proj[:, :, :opm] * col_w[:, :, None]
        right = lax.all_gather(outer_proj[:, :, opm:] * col_w[:, :, None], group, axis=1, tiled=True)
        pair_norm = jnp.einsum('si,sj->ij', col_w, value_a8.astype(jnp.bfloat16), preferred_element_type=jnp.float32)
        outer = jnp.einsum('sia,sjc->ijac', left, right, preferred_element_type=jnp.float32).astype(jnp.bfloat16)
        outer = outer.reshape(res_loc, outer.shape[1], opm * opm)
        z_blk = add_residual(z_blk, jnp.dot(outer, w_opm_out, preferred_element_type=jnp.float32) / (1e-3 + pair_norm[:, :, None]))

        start_norm = layer_norm(z_blk)
        start_bias = jnp.einsum('jkc,ch->hjk', start_norm, w_start_bias, preferred_element_type=jnp.float32).astype(jnp.bfloat16)
        start_bias = gather_rows(start_bias, group, group_size)
        z_blk = add_residual(z_blk, gated_attention(start_norm, w_start_in, w_start_out, heads_t, start_bias, res_ok, False))

        z_cols = lax.all_to_all(z_blk, group, 1, 0, tiled=True)
        end_norm = layer_norm(z_cols)
        end_bias = jnp.einsum('kjc,ch->hjk', end_norm, w_end_bias, preferred_element_type=jnp.float32).astype(jnp.bfloat16)
        end_bias = gather_rows(end_bias, group, group_size)
        z_cols = add_residual(z_cols, gated_attention(end_norm, w_end_in, w_end_out, heads_t, end_bias, res_ok, True))

        z_out = lax.all_to_all(z_cols, group, 0, 1, tiled=True)
        m_out = lax.all_to_all(m_cols, group, 0, 1, tiled=True)
        return m_out, z_out

    return jax.shard_map(per_device, mesh=mesh, in_specs=in_specs, out_specs=(rows, rows), check_vma=False)
```

```python
import functools

import jax
import jax.numpy as jnp
import numpy as np
from jax import lax
from jax.experimental import pallas as pl
from jax.experimental.pallas import tpu as pltpu
from jax.sharding import PartitionSpec as P

LOG2E = 1.4426950408889634
f32, bf16 = jnp.float32, jnp.bfloat16


def split3(value):
    parts = []
    rest = np.float64(value)
    for _ in range(3):
        part = np.float64(np.asarray(rest, dtype=jnp.bfloat16))
        parts.append(float(part))
        rest = rest - part
    return parts


def norm_rows(x):
    values = x.astype(f32)
    centred = values - jnp.mean(values, axis=-1, keepdims=True)
    variance = jnp.mean(centred * centred, axis=-1, keepdims=True)
    return (centred * lax.rsqrt(variance + 1e-5)).astype(bf16)


def dot_t(w, x):
    return lax.dot_general(w, x, (((0,), (1,)), ((), ())), preferred_element_type=f32)


def col_kernel(x_ref, mrow_ref, win_ref, wout_ref, wopm_ref, y_ref, ac_ref,
               kaug, qaug, vt, sig, gat, s0, s1, pr, wt, wka):
    seq, width = x_ref.shape
    heads, hd = vt.shape[0], vt.shape[1]
    fold = heads * hd
    bq = s0.shape[1]
    nq = seq // bq
    kc = 256
    nk = seq // kc
    c = hd ** -0.5 * LOG2E
    masked = split3(-1e9 * LOG2E)

    bp = 512
    lane = lax.broadcasted_iota(jnp.int32, (bp, 128), 1)
    row = lax.broadcasted_iota(jnp.int32, (128 - 3 * hd, bp), 0)
    fill = jnp.where(row == 0, masked[0], jnp.where(row == 1, masked[1], jnp.where(row == 2, masked[2], 0.0))).astype(bf16)
    flag = ((lane >= 3 * hd) & (lane < 3 * hd + 3)).astype(f32)
    flag2 = jnp.concatenate([flag, flag], axis=1)

    wt[...] = jnp.transpose(win_ref[...])
    for h in range(heads):
        wk = win_ref[:, fold + h * hd:fold + (h + 1) * hd]
        wka[:, h * 128:(h + 1) * 128] = jnp.concatenate([wk, wk, wk, jnp.zeros_like(wk)], axis=1)

    def project(b, carry):
        rows = pl.ds(pl.multiple_of(b * bp, bp), bp)
        xn = norm_rows(x_ref[rows, :])
        keep = jnp.transpose(jnp.broadcast_to(mrow_ref[:, rows], (128, bp)).astype(f32)) != 0
        keep2 = jnp.concatenate([keep, keep], axis=1)
        for h in range(0, heads, 2):
            k = jnp.dot(xn, wka[:, h * 128:(h + 2) * 128], preferred_element_type=f32)
            k = jnp.where(keep2, k, flag2).astype(bf16)
            kaug[h, rows, :] = k[:, :128]
            kaug[h + 1, rows, :] = k[:, 128:]

        def tdot(w):
            return lax.dot_general(w, xn, (((1,), (1,)), ((), ())), preferred_element_type=f32)

        qt = tdot(wt[:fold, :]).astype(bf16).astype(f32) * c
        hi = qt.astype(bf16)
        rest = qt - hi.astype(f32)
        mid = rest.astype(bf16)
        low = (rest - mid.astype(f32)).astype(bf16)
        vv = tdot(wt[2 * fold:3 * fold, :]).astype(bf16)
        gg = tdot(wt[3 * fold:, :]).astype(bf16).astype(f32)
        gg = 1.0 / (1.0 + jnp.exp(-gg))
        for h in range(heads):
            part = slice(h * hd, (h + 1) * hd)
            qaug[h, 0:hd, rows] = hi[part]
            qaug[h, hd:2 * hd, rows] = mid[part]
            qaug[h, 2 * hd:3 * hd, rows] = low[part]
            qaug[h, 3 * hd:, rows] = fill
            vt[h, :, rows] = vv[part]
            sig[h, :, rows] = gg[part]
        return carry

    lax.fori_loop(0, seq // bp, project, 0)

    def scores(h, q, k0):
        return jnp.dot(kaug[h, k0:k0 + kc, :], q, preferred_element_type=f32)

    def fold8(s):
        return s.reshape(kc // 8, 8, bq)

    def step(t, cur, nxt, m):
        qb, h = t // heads, t % heads
        tn = jnp.minimum(t + 1, nq * heads - 1)
        qbn, hn = tn // heads, tn % heads
        q = qaug[hn, :, pl.ds(pl.multiple_of(qbn * bq, bq), bq)]
        top = jnp.max(m, axis=0, keepdims=True)
        mn = None
        total = jnp.zeros((8, bq), f32)
        mixed = jnp.zeros((hd, bq), f32)
        for i in range(nk):
            s = scores(hn, q, i * kc)
            nxt[i * kc:(i + 1) * kc, :] = s
            sm = jnp.max(fold8(s), axis=0)
            mn = sm if mn is None else jnp.maximum(mn, sm)
            e = jnp.exp2(cur[i * kc:(i + 1) * kc, :] - top)
            total = total + jnp.sum(fold8(e), axis=0)
            mixed = mixed + jnp.dot(vt[h, :, i * kc:(i + 1) * kc], e.astype(bf16), preferred_element_type=f32)
        cols = pl.ds(pl.multiple_of(qb * bq, bq), bq)
        mixed = mixed / jnp.sum(total, axis=0, keepdims=True)
        gat[pl.ds(pl.multiple_of(h * hd, hd), hd), cols] = (mixed * sig[h, :, cols]).astype(bf16)
        return mn

    m = None
    q = qaug[0, :, 0:bq]
    for i in range(nk):
        s = scores(0, q, i * kc)
        s0[i * kc:(i + 1) * kc, :] = s
        sm = jnp.max(fold8(s), axis=0)
        m = sm if m is None else jnp.maximum(m, sm)

    def pair(u, m):
        m = step(2 * u, s0, s1, m)
        return step(2 * u + 1, s1, s0, m)

    lax.fori_loop(0, nq * heads // 2, pair, m)

    def finish(b, carry):
        rows = pl.ds(pl.multiple_of(b * bp, bp), bp)
        up = lax.dot_general(gat[:, rows], wout_ref[...], (((0,), (0,)), ((), ())), preferred_element_type=f32)
        y = (x_ref[rows, :].astype(f32) + up).astype(bf16)
        y_ref[rows, :] = y
        ac = lax.dot_general(jnp.transpose(wopm_ref[...]), norm_rows(y), (((1,), (1,)), ((), ())), preferred_element_type=f32).astype(bf16)
        ac_ref[:, rows] = (ac.astype(f32) * mrow_ref[:, rows].astype(f32)).astype(bf16)
        return carry

    lax.fori_loop(0, seq // bp, finish, 0)


def col_attention(x, mask, w_in, w_out, w_opm, heads, bq=512):
    seq, width = x.shape
    hd = w_out.shape[0] // heads
    vm = pl.BlockSpec(memory_space=pltpu.VMEM)
    return pl.pallas_call(
        col_kernel,
        out_shape=(jax.ShapeDtypeStruct((seq, width), bf16), jax.ShapeDtypeStruct((w_opm.shape[1], seq), bf16)),
        in_specs=[vm] * 5,
        out_specs=(vm, vm),
        scratch_shapes=[
            pltpu.VMEM((heads, seq, 128), bf16),
            pltpu.VMEM((heads, 128, seq), bf16),
            pltpu.VMEM((heads, hd, seq), bf16),
            pltpu.VMEM((heads, hd, seq), f32),
            pltpu.VMEM((heads * hd, seq), bf16),
            pltpu.VMEM((seq, bq), f32),
            pltpu.VMEM((seq, bq), f32),
            pltpu.VMEM((seq, bq), bf16),
            pltpu.VMEM(w_in.shape[::-1], bf16),
            pltpu.VMEM((width, heads * 128), bf16),
        ],
        compiler_params=pltpu.CompilerParams(vmem_limit_bytes=60 << 20),
        name="col_attention",
    )(x, mask[None, :], w_in, w_out, w_opm)


NT = (((1,), (1,)), ((), ()))
TN = (((0,), (0,)), ((), ()))
NEG = -1e9 * LOG2E


def mm(a, b, dims=(((1,), (0,)), ((), ()))):
    return lax.dot_general(a, b, dims, preferred_element_type=f32)


def attend_kernel(flip, per_row_mask, x_ref, b_ref, mask_ref, win_ref, wout_ref, y_ref,
                  kk, qt, vt, sig, gat, bias, wt, qd0, qd1):
    tokens, width = x_ref.shape
    size = bias.shape[0]
    seqs = tokens // size
    heads = bias.shape[1] // size
    fold = gat.shape[0]
    hd = fold // heads
    c = hd ** -0.5 * LOG2E
    bp = min(512, tokens)

    wt[...] = jnp.transpose(win_ref[...])
    qd0[...] = jnp.zeros_like(qd0)
    qd1[...] = jnp.zeros_like(qd1)
    for h in range(heads):
        block = b_ref[pl.ds(h, size, stride=heads), :] * LOG2E
        bias[:, h * size:(h + 1) * size] = jnp.transpose(block) if flip else block

    def project(b, carry):
        rows = pl.ds(pl.multiple_of(b * bp, bp), bp)
        xn = norm_rows(x_ref[rows, :])
        kk[rows, :] = mm(xn, win_ref[:, fold:2 * fold]).astype(bf16)
        qt[:, rows] = mm(wt[:fold, :], xn, NT).astype(bf16)
        vt[:, rows] = mm(wt[2 * fold:3 * fold, :], xn, NT).astype(bf16)
        gg = mm(wt[3 * fold:, :], xn, NT).astype(bf16).astype(f32)
        sig[:, rows] = 1.0 / (1.0 + jnp.exp(-gg))
        return carry

    if tokens == bp:
        project(0, 0)
    else:
        lax.fori_loop(0, tokens // bp, project, 0)

    def one(s, qd):
        cols = pl.ds(pl.multiple_of(s * size, size), size)
        for h in range(heads):
            qd[h * hd:(h + 1) * hd, h * size:(h + 1) * size] = qt[h * hd:(h + 1) * hd, cols]
        mrow = mask_ref[pl.ds(s if per_row_mask else 0, 1), :]
        keep = jnp.transpose(jnp.broadcast_to(mrow.astype(f32), (size, size))) != 0
        for h in range(0, heads, 2):
            two = slice(h * size, (h + 2) * size)
            t = mm(kk[cols, :], qd[:, two]) * c + bias[:, two]
            t = jnp.where(jnp.concatenate([keep, keep], axis=1), t, NEG)
            e = jnp.exp2(t - jnp.max(t, axis=0, keepdims=True))
            total = jnp.sum(e, axis=0, keepdims=True)
            mixed = mm(vt[h * hd:(h + 2) * hd, cols], e.astype(bf16)) / total
            gat[h * hd:(h + 1) * hd, cols] = (mixed[:hd, :size] * sig[h * hd:(h + 1) * hd, cols]).astype(bf16)
            gat[(h + 1) * hd:(h + 2) * hd, cols] = (mixed[hd:, size:] * sig[(h + 1) * hd:(h + 2) * hd, cols]).astype(bf16)

    if seqs == 1:
        one(0, qd0)
    else:
        def pair(u, carry):
            one(2 * u, qd0)
            one(2 * u + 1, qd1)
            return carry
        lax.fori_loop(0, seqs // 2, pair, 0)

    def finish(b, carry):
        rows = pl.ds(pl.multiple_of(b * bp, bp), bp)
        up = mm(gat[:, rows], wout_ref[...], TN)
        y_ref[rows, :] = (x_ref[rows, :].astype(f32) + up).astype(bf16)
        return carry

    if tokens == bp:
        finish(0, 0)
    else:
        lax.fori_loop(0, tokens // bp, finish, 0)


def attend(x, bias, mask, w_in, w_out, flip, per_row_mask, name):
    tokens, width = x.shape
    size = bias.shape[2]
    heads = bias.shape[1]
    fold = w_out.shape[0]
    vm = pl.BlockSpec(memory_space=pltpu.VMEM)
    return pl.pallas_call(
        functools.partial(attend_kernel, flip, per_row_mask),
        out_shape=jax.ShapeDtypeStruct((tokens, width), bf16),
        in_specs=[vm] * 5,
        out_specs=vm,
        scratch_shapes=[
            pltpu.VMEM((tokens, fold), bf16),
            pltpu.VMEM((fold, tokens), bf16),
            pltpu.VMEM((fold, tokens), bf16),
            pltpu.VMEM((fold, tokens), f32),
            pltpu.VMEM((fold, tokens), bf16),
            pltpu.VMEM((size, heads * size), f32),
            pltpu.VMEM(w_in.shape[::-1], bf16),
            pltpu.VMEM((fold, heads * size), bf16),
            pltpu.VMEM((fold, heads * size), bf16),
        ],
        compiler_params=pltpu.CompilerParams(vmem_limit_bytes=40 << 20),
        name=name,
    )(x, bias.reshape(size * heads, size), mask, w_in, w_out)


def gather_slots(block, group, size):
    spread = jnp.broadcast_to(block[None], (size,) + block.shape)
    return lax.all_to_all(spread, group, 0, 0, tiled=True)


def head_bias(x_norm, weight):
    return jnp.einsum('jc,ch->hj', x_norm, weight, preferred_element_type=f32).astype(bf16)


def solution(mesh):
    dap_size = mesh.shape['dap']
    group = ('chip', 'dap')
    group_size = mesh.shape['chip'] * dap_size
    rows = P(('data', 'chip', 'dap'))
    in_specs = (rows, rows, P('data'), P('data')) + (P(),) * 13

    def per_device(m_blk, z_blk, msa_mask, res_mask, w_row_in, w_row_bias, w_row_out, w_col_in, w_col_out,
                   w_opm_in, w_opm_out, w_start_in, w_start_bias, w_start_out, w_end_in, w_end_bias, w_end_out):
        me = lax.axis_index('chip') * dap_size + lax.axis_index('dap')
        seqs, res, width = m_blk.shape
        total = seqs * group_size
        heads_m = w_row_bias.shape[1]
        opm = w_opm_in.shape[1] // 2
        res_row = res_mask[None, :]

        row_bias = gather_slots(head_bias(norm_rows(z_blk[0]), w_row_bias), group, group_size).astype(f32)
        seq_mask = lax.dynamic_slice_in_dim(msa_mask, me * seqs, seqs, axis=0)
        m_blk = attend(m_blk.reshape(seqs * res, width), row_bias, seq_mask, w_row_in, w_row_out, True, True, 'row_attention')

        m_cols = lax.all_to_all(m_blk.reshape(seqs, res, width), group, 1, 0, tiled=True)
        col_mask = lax.dynamic_slice_in_dim(msa_mask, me, 1, axis=1)[:, 0]
        m_cols, pieces = col_attention(m_cols.reshape(total, width), col_mask, w_col_in, w_col_out, w_opm_in, heads_m)

        left = pieces[:opm]
        right = lax.all_gather(pieces[opm:], group, axis=0, tiled=True)
        weight = msa_mask.astype(bf16)
        pair_norm = jnp.einsum('s,sj->j', col_mask.astype(bf16), weight, preferred_element_type=f32)
        outer = lax.dot_general(right, left, NT, preferred_element_type=f32).astype(bf16)
        outer = jnp.swapaxes(outer.reshape(res, opm, opm), 1, 2).reshape(res, opm * opm)
        update = jnp.dot(outer, w_opm_out, preferred_element_type=f32) / (1e-3 + pair_norm[:, None])
        z_row = (z_blk[0].astype(f32) + update).astype(bf16)

        start_bias = gather_slots(head_bias(norm_rows(z_row), w_start_bias), group, group_size).astype(f32)
        z_row = attend(z_row, start_bias, res_row, w_start_in, w_start_out, True, False, 'start_attention')

        z_col = lax.all_to_all(z_row[None], group, 1, 0, tiled=True)[:, 0]
        end_bias = gather_slots(head_bias(norm_rows(z_col), w_end_bias), group, group_size).astype(f32)
        z_col = attend(z_col, end_bias, res_row, w_end_in, w_end_out, True, False, 'end_attention')

        z_out = lax.all_to_all(z_col[:, None], group, 0, 1, tiled=True)
        m_out = lax.all_to_all(m_cols[:, None], group, 0, 1, tiled=True)
        return m_out, z_out

    return jax.shard_map(per_device, mesh=mesh, in_specs=in_specs, out_specs=(rows, rows), check_vma=False)
```

```python
import functools

import jax
import jax.numpy as jnp
import numpy as np
from jax import lax
from jax.experimental import pallas as pl
from jax.experimental.pallas import tpu as pltpu
from jax.sharding import PartitionSpec as P

LOG2E = 1.4426950408889634
f32, bf16 = jnp.float32, jnp.bfloat16


def split3(value):
    parts = []
    rest = np.float64(value)
    for _ in range(3):
        part = np.float64(np.asarray(rest, dtype=jnp.bfloat16))
        parts.append(float(part))
        rest = rest - part
    return parts


def norm_rows(x):
    values = x.astype(f32)
    centred = values - jnp.mean(values, axis=-1, keepdims=True)
    variance = jnp.mean(centred * centred, axis=-1, keepdims=True)
    return (centred * lax.rsqrt(variance + 1e-5)).astype(bf16)


def dot_t(w, x):
    return lax.dot_general(w, x, (((0,), (1,)), ((), ())), preferred_element_type=f32)


def col_kernel(x_ref, mrow_ref, win_ref, wout_ref, wopm_ref, y_ref, ac_ref,
               kaug, qaug, vt, sig, gat, s0, s1, pr, wt, wka):
    seq, width = x_ref.shape
    heads, hd = vt.shape[0], vt.shape[1]
    fold = heads * hd
    bq = s0.shape[1]
    nq = seq // bq
    kc = 256
    nk = seq // kc
    c = hd ** -0.5 * LOG2E
    masked = split3(-1e9 * LOG2E)

    bp = 512
    lane = lax.broadcasted_iota(jnp.int32, (bp, 128), 1)
    row = lax.broadcasted_iota(jnp.int32, (128 - 3 * hd, bp), 0)
    fill = jnp.where(row == 0, masked[0], jnp.where(row == 1, masked[1], jnp.where(row == 2, masked[2], 0.0))).astype(bf16)
    flag = ((lane >= 3 * hd) & (lane < 3 * hd + 3)).astype(f32)
    flag2 = jnp.concatenate([flag, flag], axis=1)

    wt[...] = jnp.transpose(win_ref[...])
    for h in range(heads):
        wk = win_ref[:, fold + h * hd:fold + (h + 1) * hd]
        wka[:, h * 128:(h + 1) * 128] = jnp.concatenate([wk, wk, wk, jnp.zeros_like(wk)], axis=1)

    def project(b, carry):
        rows = pl.ds(pl.multiple_of(b * bp, bp), bp)
        xn = norm_rows(x_ref[rows, :])
        keep = jnp.transpose(jnp.broadcast_to(mrow_ref[:, rows], (128, bp)).astype(f32)) != 0
        keep2 = jnp.concatenate([keep, keep], axis=1)
        for h in range(0, heads, 2):
            k = jnp.dot(xn, wka[:, h * 128:(h + 2) * 128], preferred_element_type=f32)
            k = jnp.where(keep2, k, flag2).astype(bf16)
            kaug[h, rows, :] = k[:, :128]
            kaug[h + 1, rows, :] = k[:, 128:]

        def tdot(w):
            return lax.dot_general(w, xn, (((1,), (1,)), ((), ())), preferred_element_type=f32)

        qt = tdot(wt[:fold, :]).astype(bf16).astype(f32) * c
        hi = qt.astype(bf16)
        rest = qt - hi.astype(f32)
        mid = rest.astype(bf16)
        low = (rest - mid.astype(f32)).astype(bf16)
        vv = tdot(wt[2 * fold:3 * fold, :]).astype(bf16)
        gg = tdot(wt[3 * fold:, :]).astype(bf16).astype(f32)
        gg = 1.0 / (1.0 + jnp.exp(-gg))
        for h in range(heads):
            part = slice(h * hd, (h + 1) * hd)
            qaug[h, 0:hd, rows] = hi[part]
            qaug[h, hd:2 * hd, rows] = mid[part]
            qaug[h, 2 * hd:3 * hd, rows] = low[part]
            qaug[h, 3 * hd:, rows] = fill
            vt[h, :, rows] = vv[part]
            sig[h, :, rows] = gg[part]
        return carry

    lax.fori_loop(0, seq // bp, project, 0)

    def scores(h, q, k0):
        return jnp.dot(kaug[h, k0:k0 + kc, :], q, preferred_element_type=f32)

    def fold8(s):
        return s.reshape(kc // 8, 8, bq)

    def step(t, cur, nxt, m):
        qb, h = t // heads, t % heads
        tn = jnp.minimum(t + 1, nq * heads - 1)
        qbn, hn = tn // heads, tn % heads
        q = qaug[hn, :, pl.ds(pl.multiple_of(qbn * bq, bq), bq)]
        top = jnp.max(m, axis=0, keepdims=True)
        mn = None
        total = jnp.zeros((8, bq), f32)
        mixed = jnp.zeros((hd, bq), f32)
        for i in range(nk):
            s = scores(hn, q, i * kc)
            nxt[i * kc:(i + 1) * kc, :] = s
            sm = jnp.max(fold8(s), axis=0)
            mn = sm if mn is None else jnp.maximum(mn, sm)
            e = jnp.exp2(cur[i * kc:(i + 1) * kc, :] - top)
            total = total + jnp.sum(fold8(e), axis=0)
            mixed = mixed + jnp.dot(vt[h, :, i * kc:(i + 1) * kc], e.astype(bf16), preferred_element_type=f32)
        cols = pl.ds(pl.multiple_of(qb * bq, bq), bq)
        mixed = mixed / jnp.sum(total, axis=0, keepdims=True)
        gat[pl.ds(pl.multiple_of(h * hd, hd), hd), cols] = (mixed * sig[h, :, cols]).astype(bf16)
        return mn

    m = None
    q = qaug[0, :, 0:bq]
    for i in range(nk):
        s = scores(0, q, i * kc)
        s0[i * kc:(i + 1) * kc, :] = s
        sm = jnp.max(fold8(s), axis=0)
        m = sm if m is None else jnp.maximum(m, sm)

    def pair(u, m):
        m = step(2 * u, s0, s1, m)
        return step(2 * u + 1, s1, s0, m)

    lax.fori_loop(0, nq * heads // 2, pair, m)

    def finish(b, carry):
        rows = pl.ds(pl.multiple_of(b * bp, bp), bp)
        up = lax.dot_general(gat[:, rows], wout_ref[...], (((0,), (0,)), ((), ())), preferred_element_type=f32)
        y = (x_ref[rows, :].astype(f32) + up).astype(bf16)
        y_ref[rows, :] = y
        ac = lax.dot_general(jnp.transpose(wopm_ref[...]), norm_rows(y), (((1,), (1,)), ((), ())), preferred_element_type=f32).astype(bf16)
        ac_ref[:, rows] = (ac.astype(f32) * mrow_ref[:, rows].astype(f32)).astype(bf16)
        return carry

    lax.fori_loop(0, seq // bp, finish, 0)


def col_attention(x, mask, w_in, w_out, w_opm, heads, bq=512):
    seq, width = x.shape
    hd = w_out.shape[0] // heads
    vm = pl.BlockSpec(memory_space=pltpu.VMEM)
    return pl.pallas_call(
        col_kernel,
        out_shape=(jax.ShapeDtypeStruct((seq, width), bf16), jax.ShapeDtypeStruct((w_opm.shape[1], seq), bf16)),
        in_specs=[vm] * 5,
        out_specs=(vm, vm),
        scratch_shapes=[
            pltpu.VMEM((heads, seq, 128), bf16),
            pltpu.VMEM((heads, 128, seq), bf16),
            pltpu.VMEM((heads, hd, seq), bf16),
            pltpu.VMEM((heads, hd, seq), f32),
            pltpu.VMEM((heads * hd, seq), bf16),
            pltpu.VMEM((seq, bq), f32),
            pltpu.VMEM((seq, bq), f32),
            pltpu.VMEM((seq, bq), bf16),
            pltpu.VMEM(w_in.shape[::-1], bf16),
            pltpu.VMEM((width, heads * 128), bf16),
        ],
        compiler_params=pltpu.CompilerParams(vmem_limit_bytes=60 << 20),
        name="col_attention",
    )(x, mask[None, :], w_in, w_out, w_opm)


NT = (((1,), (1,)), ((), ()))
TN = (((0,), (0,)), ((), ()))
NEG = -1e9 * LOG2E


def mm(a, b, dims=(((1,), (0,)), ((), ()))):
    return lax.dot_general(a, b, dims, preferred_element_type=f32)


def attend_kernel(flip, per_row_mask, x_ref, b_ref, mask_ref, win_ref, wout_ref, y_ref,
                  kk, qt, vt, sig, gat, bias, wt, qd0, qd1):
    tokens, width = x_ref.shape
    size = bias.shape[0]
    seqs = tokens // size
    heads = bias.shape[1] // size
    fold = gat.shape[0]
    hd = fold // heads
    c = hd ** -0.5 * LOG2E
    bp = min(512, tokens)

    wt[...] = jnp.transpose(win_ref[...])
    qd0[...] = jnp.zeros_like(qd0)
    qd1[...] = jnp.zeros_like(qd1)
    for h in range(heads):
        block = b_ref[pl.ds(h, size, stride=heads), :] * LOG2E
        bias[:, h * size:(h + 1) * size] = jnp.transpose(block) if flip else block

    def project(b, carry):
        rows = pl.ds(pl.multiple_of(b * bp, bp), bp)
        xn = norm_rows(x_ref[rows, :])
        kk[rows, :] = mm(xn, win_ref[:, fold:2 * fold]).astype(bf16)
        qt[:, rows] = mm(wt[:fold, :], xn, NT).astype(bf16)
        vt[:, rows] = mm(wt[2 * fold:3 * fold, :], xn, NT).astype(bf16)
        gg = mm(wt[3 * fold:, :], xn, NT).astype(bf16).astype(f32)
        sig[:, rows] = 1.0 / (1.0 + jnp.exp(-gg))
        return carry

    if tokens == bp:
        project(0, 0)
    else:
        lax.fori_loop(0, tokens // bp, project, 0)

    def one(s, qd):
        cols = pl.ds(pl.multiple_of(s * size, size), size)
        for h in range(heads):
            qd[h * hd:(h + 1) * hd, h * size:(h + 1) * size] = qt[h * hd:(h + 1) * hd, cols]
        mrow = mask_ref[pl.ds(s if per_row_mask else 0, 1), :]
        keep = jnp.transpose(jnp.broadcast_to(mrow.astype(f32), (size, size))) != 0
        for h in range(0, heads, 2):
            two = slice(h * size, (h + 2) * size)
            t = mm(kk[cols, :], qd[:, two]) * c + bias[:, two]
            t = jnp.where(jnp.concatenate([keep, keep], axis=1), t, NEG)
            e = jnp.exp2(t - jnp.max(t, axis=0, keepdims=True))
            total = jnp.sum(e, axis=0, keepdims=True)
            mixed = mm(vt[h * hd:(h + 2) * hd, cols], e.astype(bf16)) / total
            gat[h * hd:(h + 1) * hd, cols] = (mixed[:hd, :size] * sig[h * hd:(h + 1) * hd, cols]).astype(bf16)
            gat[(h + 1) * hd:(h + 2) * hd, cols] = (mixed[hd:, size:] * sig[(h + 1) * hd:(h + 2) * hd, cols]).astype(bf16)

    if seqs == 1:
        one(0, qd0)
    else:
        def pair(u, carry):
            one(2 * u, qd0)
            one(2 * u + 1, qd1)
            return carry
        lax.fori_loop(0, seqs // 2, pair, 0)

    def finish(b, carry):
        rows = pl.ds(pl.multiple_of(b * bp, bp), bp)
        up = mm(gat[:, rows], wout_ref[...], TN)
        y_ref[rows, :] = (x_ref[rows, :].astype(f32) + up).astype(bf16)
        return carry

    if tokens == bp:
        finish(0, 0)
    else:
        lax.fori_loop(0, tokens // bp, finish, 0)


def attend(x, bias, mask, w_in, w_out, flip, per_row_mask, name):
    tokens, width = x.shape
    size = bias.shape[2]
    heads = bias.shape[1]
    fold = w_out.shape[0]
    vm = pl.BlockSpec(memory_space=pltpu.VMEM)
    return pl.pallas_call(
        functools.partial(attend_kernel, flip, per_row_mask),
        out_shape=jax.ShapeDtypeStruct((tokens, width), bf16),
        in_specs=[vm] * 5,
        out_specs=vm,
        scratch_shapes=[
            pltpu.VMEM((tokens, fold), bf16),
            pltpu.VMEM((fold, tokens), bf16),
            pltpu.VMEM((fold, tokens), bf16),
            pltpu.VMEM((fold, tokens), f32),
            pltpu.VMEM((fold, tokens), bf16),
            pltpu.VMEM((size, heads * size), f32),
            pltpu.VMEM(w_in.shape[::-1], bf16),
            pltpu.VMEM((fold, heads * size), bf16),
            pltpu.VMEM((fold, heads * size), bf16),
        ],
        compiler_params=pltpu.CompilerParams(vmem_limit_bytes=40 << 20),
        name=name,
    )(x, bias.reshape(size * heads, size), mask, w_in, w_out)


NN = (((1,), (0,)), ((), ()))
MESH = pl.DeviceIdType.MESH
INNER = 8
SLOT = 8


def place(t, dap):
    return (0, t // dap, t % dap)


def pair_project(x, win_ref, fold):
    xn = norm_rows(x)
    k = mm(xn, win_ref[:, fold:2 * fold]).astype(bf16)
    qt = dot_t(win_ref[:, :fold], xn).astype(bf16)
    vt = dot_t(win_ref[:, 2 * fold:3 * fold], xn).astype(bf16)
    gg = dot_t(win_ref[:, 3 * fold:], xn).astype(bf16).astype(f32)
    return k, qt, vt, 1.0 / (1.0 + jnp.exp(-gg))


def pair_attend(x, parts, biases, keep, wout_ref):
    k, qt, vt, sig = parts
    heads = len(biases)
    hd = vt.shape[0] // heads
    c = hd ** -0.5 * LOG2E
    gated = []
    for h in range(heads):
        part = slice(h * hd, (h + 1) * hd)
        t = mm(k[:, part], qt[part]) * c + biases[h] * LOG2E
        t = jnp.where(keep, t, NEG)
        e = jnp.exp2(t - jnp.max(t, axis=0, keepdims=True))
        mixed = mm(vt[part], e.astype(bf16)) / jnp.sum(e, axis=0, keepdims=True)
        gated.append((mixed * sig[part]).astype(bf16))
    up = mm(jnp.concatenate(gated, axis=0), wout_ref[...], TN)
    return (x.astype(f32) + up).astype(bf16)


def pair_kernel(group, dap, ac_ref, mcol_ref, z_ref, norm_ref, mask_ref, wopm_ref, ws_in, ws_bias, ws_out,
                we_in, we_bias, we_out, mout, zout,
                abuf, cbuf, oscr, uscr, usend, ubuf, zrow, bsend, bbuf, bscr, esend, ebuf, zsend, zfin, send, recv):
    me = lax.axis_index('chip') * dap + lax.axis_index('dap')
    hi, lo = me // INNER, me % INNER
    outer_n = group // INNER
    opm = ac_ref.shape[0] // 2
    heads = ws_bias.shape[1]
    fold = ws_out.shape[0]
    size = z_ref.shape[0]
    piece = mcol_ref.shape[0] // group

    barrier = pltpu.get_barrier_semaphore()

    def greet(o, carry):
        pl.semaphore_signal(barrier, inc=1, device_id=place((me + o) % group, dap), device_id_type=MESH)
        return carry

    lax.fori_loop(1, group, greet, 0)

    def remote(src, dst, i, t):
        return pltpu.make_async_remote_copy(src_ref=src, dst_ref=dst, send_sem=send.at[i], recv_sem=recv.at[i],
                                            device_id=place(t, dap), device_id_type=MESH)

    def settle(buf, i, n):
        done = remote(buf.at[pl.ds(0, n)], buf.at[pl.ds(0, n)], i, me)
        done.wait_send()
        done.wait_recv()

    abuf[lo] = ac_ref[:opm, :]
    cbuf[hi] = ac_ref[opm:, :]
    keep = jnp.transpose(jnp.broadcast_to(mask_ref[...].astype(f32), (size, size))) != 0
    pl.semaphore_wait(barrier, group - 1)

    def share_a(o, carry):
        remote(ac_ref.at[pl.ds(0, opm)], abuf.at[lo], 0, hi * INNER + (lo + o) % INNER).start()
        return carry

    def share_c(o, carry):
        remote(ac_ref.at[pl.ds(opm, opm)], cbuf.at[hi], 1, (hi + o) % outer_n * INNER + lo).start()
        return carry

    def share_m(o, carry):
        t = (me + o) % group
        remote(mcol_ref.at[pl.ds(pl.multiple_of(t * piece, piece), piece)], mout.at[me], 2, t).start()
        return carry

    lax.fori_loop(1, outer_n, share_c, 0)
    lax.fori_loop(1, INNER, share_a, 0)
    settle(abuf, 0, INNER - 1)
    settle(cbuf, 1, outer_n - 1)
    mout[me] = mcol_ref[pl.ds(pl.multiple_of(me * piece, piece), piece), :]
    lax.fori_loop(1, group, share_m, 0)

    per = 128 // opm
    outer = mm(abuf[...].reshape(INNER * opm, -1), cbuf[...].reshape(outer_n * opm, -1), NT)
    for g in range(outer_n // per):
        oscr[g] = outer[:, g * 128:(g + 1) * 128]
    lane = lax.broadcasted_iota(jnp.int32, (opm // per * INNER, 128), 1) // opm
    tiles = []
    for g in range(outer_n // per):
        slabs = [jnp.concatenate([oscr[g, pl.ds(b * per + r, INNER, stride=opm), :] for b in range(opm // per)], axis=0)
                 for r in range(per)]
        turned = [[slabs[r] if s == 0 else pltpu.roll(slabs[r], s * opm, 1) for s in range(per)] for r in range(per)]
        for q in range(per):
            pick = turned[0][(0 - q) % per]
            for r in range(1, per):
                pick = jnp.where(lane == r, turned[r][(r - q) % per], pick)
            tiles.append(pick)
    up = None
    for b in range(opm // per):
        block = jnp.concatenate([t[b * INNER:(b + 1) * INNER] for t in tiles], axis=0).astype(bf16)
        term = mm(block, wopm_ref[b * 128:(b + 1) * 128, :])
        up = term if up is None else up + term
    uscr[...] = up
    for x in range(INNER):
        usend[x] = uscr[pl.ds(x, outer_n, stride=INNER), :]
    ubuf[lo] = usend[lo]

    def share_u(o, carry):
        x = (lo + o) % INNER
        remote(usend.at[x], ubuf.at[lo], 3, hi * INNER + x).start()
        return carry

    lax.fori_loop(1, INNER, share_u, 0)
    settle(ubuf, 3, INNER - 1)
    for x in range(INNER):
        zrow[pl.ds(x, outer_n, stride=INNER), :] = ubuf[x]
    z1 = (z_ref[...].astype(f32) + zrow[...] / (1e-3 + norm_ref[...])).astype(bf16)

    def bias_rows(z, weight):
        rows = dot_t(weight[...], norm_rows(z)).astype(bf16)
        return jnp.concatenate([rows, jnp.zeros((SLOT - heads, size), bf16)], axis=0)

    bsend[...] = bias_rows(z1, ws_bias)
    bbuf[me] = bsend[...]

    def share_b(o, carry):
        remote(bsend, bbuf.at[me], 4, (me + o) % group).start()
        return carry

    lax.fori_loop(1, group, share_b, 0)
    parts = pair_project(z1, ws_in, fold)
    settle(bbuf, 4, group - 1)
    bscr[...] = bbuf[...].astype(f32).reshape(group * SLOT, size)
    biases = [jnp.transpose(bscr[pl.ds(h, size, stride=SLOT), :]) for h in range(heads)]
    z2 = pair_attend(z1, parts, biases, keep, ws_out)

    end_rows = bias_rows(z2, we_bias).astype(f32)
    for h in range(heads):
        bscr[pl.ds(h, size, stride=SLOT), :] = jnp.broadcast_to(end_rows[h:h + 1], (size, size))
    bscr[pl.ds(heads, size, stride=SLOT), :] = z2.astype(f32)
    esend[...] = bscr[...].astype(bf16).reshape(group, SLOT, size)
    ebuf[me] = esend[me]

    def share_e(o, carry):
        t = (me + o) % group
        remote(esend.at[t], ebuf.at[me], 5, t).start()
        return carry

    lax.fori_loop(1, group, share_e, 0)
    settle(ebuf, 5, group - 1)
    bscr[...] = ebuf[...].astype(f32).reshape(group * SLOT, size)
    zc = bscr[pl.ds(heads, size, stride=SLOT), :].astype(bf16)
    biases = [bscr[pl.ds(h, size, stride=SLOT), :] for h in range(heads)]
    z3 = pair_attend(zc, pair_project(zc, we_in, fold), biases, keep, we_out)

    zsend[...] = z3.astype(f32)
    zfin[pl.ds(me, 1), :] = zsend[pl.ds(me, 1), :]

    def share_z(o, carry):
        t = (me + o) % group
        remote(zsend.at[pl.ds(t, 1)], zfin.at[pl.ds(me, 1)], 6, t).start()
        return carry

    lax.fori_loop(1, group, share_z, 0)
    settle(zfin, 6, group - 1)
    zout[...] = zfin[...].astype(bf16)
    settle(mout, 2, group - 1)


def pair_update(ac, mcols, z, norm, mask, weights, group, dap):
    vm = pl.BlockSpec(memory_space=pltpu.VMEM)
    seq = ac.shape[1]
    opm = ac.shape[0] // 2
    size, width = z.shape
    outer_n = group // INNER
    piece = mcols.shape[0] // group
    return pl.pallas_call(
        functools.partial(pair_kernel, group, dap),
        out_shape=(jax.ShapeDtypeStruct((group, piece, mcols.shape[1]), bf16), jax.ShapeDtypeStruct((size, width), bf16)),
        in_specs=[vm] * 12,
        out_specs=(vm, vm),
        scratch_shapes=[
            pltpu.VMEM((INNER, opm, seq), bf16),
            pltpu.VMEM((outer_n, opm, seq), bf16),
            pltpu.VMEM((outer_n * opm // 128, INNER * opm, 128), f32),
            pltpu.VMEM((size, width), f32),
            pltpu.VMEM((INNER, outer_n, width), f32),
            pltpu.VMEM((INNER, outer_n, width), f32),
            pltpu.VMEM((size, width), f32),
            pltpu.VMEM((SLOT, size), bf16),
            pltpu.VMEM((group, SLOT, size), bf16),
            pltpu.VMEM((group * SLOT, size), f32),
            pltpu.VMEM((group, SLOT, size), bf16),
            pltpu.VMEM((group, SLOT, size), bf16),
            pltpu.VMEM((size, width), f32),
            pltpu.VMEM((size, width), f32),
            pltpu.SemaphoreType.DMA((7,)),
            pltpu.SemaphoreType.DMA((7,)),
        ],
        compiler_params=pltpu.CompilerParams(collective_id=1, has_side_effects=True, vmem_limit_bytes=40 << 20),
        name='pair_update',
    )(ac, mcols, z, norm, mask, *weights)


def gather_slots(block, group, size):
    spread = jnp.broadcast_to(block[None], (size,) + block.shape)
    return lax.all_to_all(spread, group, 0, 0, tiled=True)


def head_bias(x_norm, weight):
    return jnp.einsum('jc,ch->hj', x_norm, weight, preferred_element_type=f32).astype(bf16)


def solution(mesh):
    dap_size = mesh.shape['dap']
    group = ('chip', 'dap')
    group_size = mesh.shape['chip'] * dap_size
    rows = P(('data', 'chip', 'dap'))
    in_specs = (rows, rows, P('data'), P('data')) + (P(),) * 13

    def per_device(m_blk, z_blk, msa_mask, res_mask, w_row_in, w_row_bias, w_row_out, w_col_in, w_col_out,
                   w_opm_in, w_opm_out, w_start_in, w_start_bias, w_start_out, w_end_in, w_end_bias, w_end_out):
        me = lax.axis_index('chip') * dap_size + lax.axis_index('dap')
        seqs, res, width = m_blk.shape
        total = seqs * group_size
        heads_m = w_row_bias.shape[1]
        res_row = res_mask[None, :]

        row_bias = gather_slots(head_bias(norm_rows(z_blk[0]), w_row_bias), group, group_size).astype(f32)
        seq_mask = lax.dynamic_slice_in_dim(msa_mask, me * seqs, seqs, axis=0)
        m_blk = attend(m_blk.reshape(seqs * res, width), row_bias, seq_mask, w_row_in, w_row_out, True, True, 'row_attention')

        m_cols = lax.all_to_all(m_blk.reshape(seqs, res, width), group, 1, 0, tiled=True)
        col_mask = lax.dynamic_slice_in_dim(msa_mask, me, 1, axis=1)[:, 0]
        m_cols, pieces = col_attention(m_cols.reshape(total, width), col_mask, w_col_in, w_col_out, w_opm_in, heads_m)

        weight = msa_mask.astype(bf16)
        pair_norm = jnp.einsum('s,sj->j', col_mask.astype(bf16), weight, preferred_element_type=f32)
        pair_norm = jnp.broadcast_to(pair_norm[:, None], (res, z_blk.shape[2]))
        weights = (w_opm_out, w_start_in, w_start_bias, w_start_out, w_end_in, w_end_bias, w_end_out)
        m_slots, z_out = pair_update(pieces, m_cols, z_blk[0], pair_norm, res_row, weights, group_size, dap_size)
        m_out, z_out = jnp.swapaxes(m_slots, 0, 1), z_out[None]
        return m_out, z_out

    return jax.shard_map(per_device, mesh=mesh, in_specs=in_specs, out_specs=(rows, rows), check_vma=False)
```

```python
import functools

import jax
import jax.numpy as jnp
import numpy as np
from jax import lax
from jax.experimental import pallas as pl
from jax.experimental.pallas import tpu as pltpu
from jax.sharding import PartitionSpec as P

LOG2E = 1.4426950408889634
f32, bf16 = jnp.float32, jnp.bfloat16


def split3(value):
    parts = []
    rest = np.float64(value)
    for _ in range(3):
        part = np.float64(np.asarray(rest, dtype=jnp.bfloat16))
        parts.append(float(part))
        rest = rest - part
    return parts


def norm_rows(x):
    values = x.astype(f32)
    centred = values - jnp.mean(values, axis=-1, keepdims=True)
    variance = jnp.mean(centred * centred, axis=-1, keepdims=True)
    return (centred * lax.rsqrt(variance + 1e-5)).astype(bf16)


def dot_t(w, x):
    return lax.dot_general(w, x, (((0,), (1,)), ((), ())), preferred_element_type=f32)


NT = (((1,), (1,)), ((), ()))
TN = (((0,), (0,)), ((), ()))
NEG = -1e9 * LOG2E


def mm(a, b, dims=(((1,), (0,)), ((), ()))):
    return lax.dot_general(a, b, dims, preferred_element_type=f32)


def attend_kernel(flip, per_row_mask, x_ref, b_ref, mask_ref, win_ref, wout_ref, y_ref,
                  kk, qt, vt, sig, gat, bias, wt, qd0, qd1):
    tokens, width = x_ref.shape
    size = bias.shape[0]
    seqs = tokens // size
    heads = bias.shape[1] // size
    fold = gat.shape[0]
    hd = fold // heads
    c = hd ** -0.5 * LOG2E
    bp = min(512, tokens)

    wt[...] = jnp.transpose(win_ref[...])
    qd0[...] = jnp.zeros_like(qd0)
    qd1[...] = jnp.zeros_like(qd1)
    for h in range(heads):
        block = b_ref[pl.ds(h, size, stride=heads), :] * LOG2E
        bias[:, h * size:(h + 1) * size] = jnp.transpose(block) if flip else block

    def project(b, carry):
        rows = pl.ds(pl.multiple_of(b * bp, bp), bp)
        xn = norm_rows(x_ref[rows, :])
        kk[rows, :] = mm(xn, win_ref[:, fold:2 * fold]).astype(bf16)
        qt[:, rows] = mm(wt[:fold, :], xn, NT).astype(bf16)
        vt[:, rows] = mm(wt[2 * fold:3 * fold, :], xn, NT).astype(bf16)
        gg = mm(wt[3 * fold:, :], xn, NT).astype(bf16).astype(f32)
        sig[:, rows] = 1.0 / (1.0 + jnp.exp(-gg))
        return carry

    if tokens == bp:
        project(0, 0)
    else:
        lax.fori_loop(0, tokens // bp, project, 0)

    def one(s, qd):
        cols = pl.ds(pl.multiple_of(s * size, size), size)
        for h in range(heads):
            qd[h * hd:(h + 1) * hd, h * size:(h + 1) * size] = qt[h * hd:(h + 1) * hd, cols]
        mrow = mask_ref[pl.ds(s if per_row_mask else 0, 1), :]
        keep = jnp.transpose(jnp.broadcast_to(mrow.astype(f32), (size, size))) != 0
        for h in range(0, heads, 2):
            two = slice(h * size, (h + 2) * size)
            t = mm(kk[cols, :], qd[:, two]) * c + bias[:, two]
            t = jnp.where(jnp.concatenate([keep, keep], axis=1), t, NEG)
            e = jnp.exp2(t - jnp.max(t, axis=0, keepdims=True))
            total = jnp.sum(e, axis=0, keepdims=True)
            mixed = mm(vt[h * hd:(h + 2) * hd, cols], e.astype(bf16)) / total
            gat[h * hd:(h + 1) * hd, cols] = (mixed[:hd, :size] * sig[h * hd:(h + 1) * hd, cols]).astype(bf16)
            gat[(h + 1) * hd:(h + 2) * hd, cols] = (mixed[hd:, size:] * sig[(h + 1) * hd:(h + 2) * hd, cols]).astype(bf16)

    if seqs == 1:
        one(0, qd0)
    else:
        def pair(u, carry):
            one(2 * u, qd0)
            one(2 * u + 1, qd1)
            return carry
        lax.fori_loop(0, seqs // 2, pair, 0)

    def finish(b, carry):
        rows = pl.ds(pl.multiple_of(b * bp, bp), bp)
        up = mm(gat[:, rows], wout_ref[...], TN)
        y_ref[rows, :] = (x_ref[rows, :].astype(f32) + up).astype(bf16)
        return carry

    if tokens == bp:
        finish(0, 0)
    else:
        lax.fori_loop(0, tokens // bp, finish, 0)


def attend(x, bias, mask, w_in, w_out, flip, per_row_mask, name):
    tokens, width = x.shape
    size = bias.shape[2]
    heads = bias.shape[1]
    fold = w_out.shape[0]
    vm = pl.BlockSpec(memory_space=pltpu.VMEM)
    return pl.pallas_call(
        functools.partial(attend_kernel, flip, per_row_mask),
        out_shape=jax.ShapeDtypeStruct((tokens, width), bf16),
        in_specs=[vm] * 5,
        out_specs=vm,
        scratch_shapes=[
            pltpu.VMEM((tokens, fold), bf16),
            pltpu.VMEM((fold, tokens), bf16),
            pltpu.VMEM((fold, tokens), bf16),
            pltpu.VMEM((fold, tokens), f32),
            pltpu.VMEM((fold, tokens), bf16),
            pltpu.VMEM((size, heads * size), f32),
            pltpu.VMEM(w_in.shape[::-1], bf16),
            pltpu.VMEM((fold, heads * size), bf16),
            pltpu.VMEM((fold, heads * size), bf16),
        ],
        compiler_params=pltpu.CompilerParams(vmem_limit_bytes=40 << 20),
        name=name,
    )(x, bias.reshape(size * heads, size), mask, w_in, w_out)


NN = (((1,), (0,)), ((), ()))
MESH = pl.DeviceIdType.MESH
INNER = 8
SLOT = 8


def place(t, dap):
    return (0, t // dap, t % dap)


def pair_project(x, win_ref, fold):
    xn = norm_rows(x)
    k = mm(xn, win_ref[:, fold:2 * fold]).astype(bf16)
    qt = dot_t(win_ref[:, :fold], xn).astype(bf16)
    vt = dot_t(win_ref[:, 2 * fold:3 * fold], xn).astype(bf16)
    gg = dot_t(win_ref[:, 3 * fold:], xn).astype(bf16).astype(f32)
    return k, qt, vt, 1.0 / (1.0 + jnp.exp(-gg))


def pair_attend(x, parts, biases, keep, wout_ref):
    k, qt, vt, sig = parts
    heads = len(biases)
    hd = vt.shape[0] // heads
    c = hd ** -0.5 * LOG2E
    gated = []
    for h in range(heads):
        part = slice(h * hd, (h + 1) * hd)
        t = mm(k[:, part], qt[part]) * c + biases[h] * LOG2E
        t = jnp.where(keep, t, NEG)
        e = jnp.exp2(t - jnp.max(t, axis=0, keepdims=True))
        mixed = mm(vt[part], e.astype(bf16)) / jnp.sum(e, axis=0, keepdims=True)
        gated.append((mixed * sig[part]).astype(bf16))
    up = mm(jnp.concatenate(gated, axis=0), wout_ref[...], TN)
    return (x.astype(f32) + up).astype(bf16)


def col_stage(x_ref, mrow_ref, win_ref, wout_ref, wopm_ref, emit,
              kaug, qaug, vt, sig, gat, s0, s1, wt, wka):
    seq, width = x_ref.shape
    heads, hd = vt.shape[0], vt.shape[1]
    fold = heads * hd
    bq = s0.shape[1]
    nq = seq // bq
    kc = 256
    nk = seq // kc
    c = hd ** -0.5 * LOG2E
    masked = split3(-1e9 * LOG2E)

    lane = lax.broadcasted_iota(jnp.int32, (bq, 128), 1)
    row = lax.broadcasted_iota(jnp.int32, (128 - 3 * hd, bq), 0)
    fill = jnp.where(row == 0, masked[0], jnp.where(row == 1, masked[1], jnp.where(row == 2, masked[2], 0.0))).astype(bf16)
    flag = ((lane >= 3 * hd) & (lane < 3 * hd + 3)).astype(f32)
    flag2 = jnp.concatenate([flag, flag], axis=1)

    wt[...] = jnp.transpose(win_ref[...])
    for h in range(heads):
        wk = win_ref[:, fold + h * hd:fold + (h + 1) * hd]
        wka[:, h * 128:(h + 1) * 128] = jnp.concatenate([wk, wk, wk, jnp.zeros_like(wk)], axis=1)
    wopm_t = jnp.transpose(wopm_ref[...])

    def project(b, carry):
        rows = pl.ds(pl.multiple_of(b * bq, bq), bq)
        xn = norm_rows(x_ref[rows, :])
        keep = jnp.transpose(jnp.broadcast_to(mrow_ref[:, rows], (128, bq)).astype(f32)) != 0
        keep2 = jnp.concatenate([keep, keep], axis=1)
        for h in range(0, heads, 2):
            k = mm(xn, wka[:, h * 128:(h + 2) * 128])
            k = jnp.where(keep2, k, flag2).astype(bf16)
            kaug[h, rows, :] = k[:, :128]
            kaug[h + 1, rows, :] = k[:, 128:]
        qt = mm(wt[:fold, :], xn, NT).astype(bf16).astype(f32) * c
        hi = qt.astype(bf16)
        rest = qt - hi.astype(f32)
        mid = rest.astype(bf16)
        low = (rest - mid.astype(f32)).astype(bf16)
        vv = mm(wt[2 * fold:3 * fold, :], xn, NT).astype(bf16)
        gg = mm(wt[3 * fold:, :], xn, NT).astype(bf16).astype(f32)
        gg = 1.0 / (1.0 + jnp.exp(-gg))
        for h in range(heads):
            part = slice(h * hd, (h + 1) * hd)
            qaug[h, 0:hd, rows] = hi[part]
            qaug[h, hd:2 * hd, rows] = mid[part]
            qaug[h, 2 * hd:3 * hd, rows] = low[part]
            qaug[h, 3 * hd:, rows] = fill
            vt[h, :, rows] = vv[part]
            sig[h, :, rows] = gg[part]
        return carry

    lax.fori_loop(0, nq, project, 0)

    def fold8(s):
        return s.reshape(kc // 8, 8, bq)

    def chunk_scores(h, q, i, buf, m):
        s = mm(kaug[h, i * kc:(i + 1) * kc, :], q)
        buf[i * kc:(i + 1) * kc, :] = s
        top = jnp.max(fold8(s), axis=0)
        return top if m is None else jnp.maximum(m, top)

    def step(qb, h, cur, nxt, m):
        t = jnp.minimum(qb * heads + h + 1, nq * heads - 1)
        hn = t % heads
        q = qaug[hn, :, pl.ds(pl.multiple_of(t // heads * bq, bq), bq)]
        top = jnp.max(m, axis=0, keepdims=True)
        mn = None
        total = jnp.zeros((8, bq), f32)
        mixed = jnp.zeros((hd, bq), f32)
        for i in range(nk):
            mn = chunk_scores(hn, q, i, nxt, mn)
            e = jnp.exp2(cur[i * kc:(i + 1) * kc, :] - top)
            total = total + jnp.sum(fold8(e), axis=0)
            mixed = mixed + mm(vt[h, :, i * kc:(i + 1) * kc], e.astype(bf16))
        cols = pl.ds(pl.multiple_of(qb * bq, bq), bq)
        mixed = mixed / jnp.sum(total, axis=0, keepdims=True)
        gat[pl.ds(pl.multiple_of(h * hd, hd), hd), :] = (mixed * sig[h, :, cols]).astype(bf16)
        return mn

    m = None
    for i in range(nk):
        m = chunk_scores(0, qaug[0, :, 0:bq], i, s0, m)

    def block(qb, m):
        def pair(u, m):
            m = step(qb, 2 * u, s0, s1, m)
            return step(qb, 2 * u + 1, s1, s0, m)

        m = lax.fori_loop(0, heads // 2, pair, m)
        rows = pl.ds(pl.multiple_of(qb * bq, bq), bq)
        y = (x_ref[rows, :].astype(f32) + mm(gat[...], wout_ref[...], TN)).astype(bf16)
        ac = mm(wopm_t, norm_rows(y), NT).astype(bf16)
        emit(qb, y, (ac.astype(f32) * mrow_ref[:, rows].astype(f32)).astype(bf16))
        return m

    lax.fori_loop(0, nq, block, m)


class Links:
    def __init__(self, group, dap, send, recv):
        self.group, self.dap, self.send, self.recv = group, dap, send, recv
        self.me = lax.axis_index('chip') * dap + lax.axis_index('dap')
        self.hi, self.lo = self.me // INNER, self.me % INNER
        self.outer_n = group // INNER

    def greet(self):
        barrier = pltpu.get_barrier_semaphore()

        def one(o, carry):
            pl.semaphore_signal(barrier, inc=1, device_id=place((self.me + o) % self.group, self.dap), device_id_type=MESH)
            return carry

        lax.fori_loop(1, self.group, one, 0)

    def ready(self):
        pl.semaphore_wait(pltpu.get_barrier_semaphore(), self.group - 1)

    def copy(self, src, dst, i, t):
        return pltpu.make_async_remote_copy(src_ref=src, dst_ref=dst, send_sem=self.send.at[i], recv_sem=self.recv.at[i],
                                            device_id=place(t, self.dap), device_id_type=MESH)

    def settle(self, part, i):
        done = self.copy(part, part, i, self.me)
        done.wait_send()
        done.wait_recv()

    def to_all(self, make, i):
        def one(o, carry):
            t = (self.me + o) % self.group
            src, dst = make(t)
            self.copy(src, dst, i, t).start()
            return carry

        lax.fori_loop(1, self.group, one, 0)

    def to_inner(self, make, i):
        def one(o, carry):
            x = (self.lo + o) % INNER
            src, dst = make(x)
            self.copy(src, dst, i, self.hi * INNER + x).start()
            return carry

        lax.fori_loop(1, INNER, one, 0)

    def to_outer(self, make, i):
        def one(o, carry):
            src, dst = make()
            self.copy(src, dst, i, (self.hi + o) % self.outer_n * INNER + self.lo).start()
            return carry

        lax.fori_loop(1, self.outer_n, one, 0)


def pair_stage(net, z_ref, norm_ref, mask_ref, wopm_ref, ws_in, ws_bias, ws_out, we_in, we_bias, we_out, zout,
               abuf, cbuf, oscr, uscr, usend, ubuf, zrow, bsend, bbuf, bscr, esend, ebuf, zsend, zfin):
    me, lo, group, outer_n = net.me, net.lo, net.group, net.outer_n
    blocks, opm = abuf.shape[0], abuf.shape[2]
    heads = ws_bias.shape[1]
    fold = ws_out.shape[0]
    size = z_ref.shape[0]
    keep = jnp.transpose(jnp.broadcast_to(mask_ref[...].astype(f32), (size, size))) != 0

    per = 128 // opm
    outer = None
    for q in range(blocks):
        term = mm(abuf[q].reshape(INNER * opm, -1), cbuf[q].reshape(outer_n * opm, -1), NT)
        outer = term if outer is None else outer + term
    for g in range(outer_n // per):
        oscr[g] = outer[:, g * 128:(g + 1) * 128]
    lane = lax.broadcasted_iota(jnp.int32, (opm // per * INNER, 128), 1) // opm
    tiles = []
    for g in range(outer_n // per):
        slabs = [jnp.concatenate([oscr[g, pl.ds(b * per + r, INNER, stride=opm), :] for b in range(opm // per)], axis=0)
                 for r in range(per)]
        turned = [[slabs[r] if s == 0 else pltpu.roll(slabs[r], s * opm, 1) for s in range(per)] for r in range(per)]
        for q in range(per):
            pick = turned[0][(0 - q) % per]
            for r in range(1, per):
                pick = jnp.where(lane == r, turned[r][(r - q) % per], pick)
            tiles.append(pick)
    up = None
    for b in range(opm // per):
        block = jnp.concatenate([t[b * INNER:(b + 1) * INNER] for t in tiles], axis=0).astype(bf16)
        term = mm(block, wopm_ref[b * 128:(b + 1) * 128, :])
        up = term if up is None else up + term
    uscr[...] = up
    for x in range(INNER):
        usend[x] = uscr[pl.ds(x, outer_n, stride=INNER), :]
    ubuf[lo] = usend[lo]
    net.to_inner(lambda x: (usend.at[x], ubuf.at[lo]), 3)
    net.settle(ubuf.at[pl.ds(0, INNER - 1)], 3)
    for x in range(INNER):
        zrow[pl.ds(x, outer_n, stride=INNER), :] = ubuf[x]
    z1 = (z_ref[...].astype(f32) + zrow[...] / (1e-3 + norm_ref[...])).astype(bf16)

    def bias_rows(z, weight):
        rows = dot_t(weight[...], norm_rows(z)).astype(bf16)
        return jnp.concatenate([rows, jnp.zeros((SLOT - heads, size), bf16)], axis=0)

    bsend[...] = bias_rows(z1, ws_bias)
    bbuf[me] = bsend[...]
    net.to_all(lambda t: (bsend, bbuf.at[me]), 4)
    parts = pair_project(z1, ws_in, fold)
    net.settle(bbuf.at[pl.ds(0, group - 1)], 4)
    bscr[...] = bbuf[...].astype(f32).reshape(group * SLOT, size)
    biases = [jnp.transpose(bscr[pl.ds(h, size, stride=SLOT), :]) for h in range(heads)]
    z2 = pair_attend(z1, parts, biases, keep, ws_out)

    end_rows = bias_rows(z2, we_bias).astype(f32)
    for h in range(heads):
        bscr[pl.ds(h, size, stride=SLOT), :] = jnp.broadcast_to(end_rows[h:h + 1], (size, size))
    bscr[pl.ds(heads, size, stride=SLOT), :] = z2.astype(f32)
    esend[...] = bscr[...].astype(bf16).reshape(group, SLOT, size)
    ebuf[me] = esend[me]
    net.to_all(lambda t: (esend.at[t], ebuf.at[me]), 5)
    net.settle(ebuf.at[pl.ds(0, group - 1)], 5)
    bscr[...] = ebuf[...].astype(f32).reshape(group * SLOT, size)
    zc = bscr[pl.ds(heads, size, stride=SLOT), :].astype(bf16)
    biases = [bscr[pl.ds(h, size, stride=SLOT), :] for h in range(heads)]
    z3 = pair_attend(zc, pair_project(zc, we_in, fold), biases, keep, we_out)

    zsend[...] = z3.astype(f32)
    zfin[pl.ds(me, 1), :] = zsend[pl.ds(me, 1), :]
    net.to_all(lambda t: (zsend.at[pl.ds(t, 1)], zfin.at[pl.ds(me, 1)]), 6)
    net.settle(zfin.at[pl.ds(0, group - 1)], 6)
    zout[...] = zfin[...].astype(bf16)


def tail_kernel(group, dap, x_ref, mrow_ref, wc_in, wc_out, wopm_in, z_ref, norm_ref, mask_ref, wopm_out,
                ws_in, ws_bias, ws_out, we_in, we_bias, we_out, mout, zout,
                kaug, qaug, vt, sig, gat, s0, s1, wt, wka, ycol, acs, abuf, cbuf,
                oscr, uscr, usend, ubuf, zrow, bsend, bbuf, bscr, esend, ebuf, zsend, zfin, send, recv):
    net = Links(group, dap, send, recv)
    me, lo, hi = net.me, net.lo, net.hi
    blocks, opm = abuf.shape[0], abuf.shape[2]
    bq = s0.shape[1]
    piece = mout.shape[1]
    per = bq // piece
    net.greet()

    def emit(qb, y, ac):
        ycol[pl.ds(pl.multiple_of(qb * bq, bq), bq), :] = y
        acs[qb] = ac
        abuf[qb, lo] = ac[:opm]
        cbuf[qb, hi] = ac[opm:]

        @pl.when(qb == 0)
        def _():
            net.ready()

        net.to_outer(lambda: (acs.at[qb, pl.ds(opm, opm)], cbuf.at[qb, hi]), 1)
        net.to_inner(lambda x: (acs.at[qb, pl.ds(0, opm)], abuf.at[qb, lo]), 0)

        def share_m(o, carry):
            t = qb * per + (me + o) % per

            @pl.when(t != me)
            def _():
                net.copy(ycol.at[pl.ds(pl.multiple_of(t * piece, piece), piece)], mout.at[me], 2, t).start()

            return carry

        lax.fori_loop(0, per, share_m, 0)

    col_stage(x_ref, mrow_ref, wc_in, wc_out, wopm_in, emit, kaug, qaug, vt, sig, gat, s0, s1, wt, wka)
    mout[me] = ycol[pl.ds(pl.multiple_of(me * piece, piece), piece), :]
    net.settle(cbuf.at[:, pl.ds(0, net.outer_n - 1)], 1)
    net.settle(abuf.at[:, pl.ds(0, INNER - 1)], 0)
    pair_stage(net, z_ref, norm_ref, mask_ref, wopm_out, ws_in, ws_bias, ws_out, we_in, we_bias, we_out, zout,
               abuf, cbuf, oscr, uscr, usend, ubuf, zrow, bsend, bbuf, bscr, esend, ebuf, zsend, zfin)
    net.settle(mout.at[pl.ds(0, group - 1)], 2)


def col_scratch(seq, width, heads, hd, bq):
    return [
        pltpu.VMEM((heads, seq, 128), bf16),
        pltpu.VMEM((heads, 128, seq), bf16),
        pltpu.VMEM((heads, hd, seq), bf16),
        pltpu.VMEM((heads, hd, seq), f32),
        pltpu.VMEM((heads * hd, bq), bf16),
        pltpu.VMEM((seq, bq), f32),
        pltpu.VMEM((seq, bq), f32),
        pltpu.VMEM((4 * heads * hd, width), bf16),
        pltpu.VMEM((width, heads * 128), bf16),
        pltpu.VMEM((seq, width), bf16),
    ]


def pair_scratch(seq, size, width, opm, group, bq):
    outer_n = group // INNER
    return [
        pltpu.VMEM((seq // bq, 2 * opm, bq), bf16),
        pltpu.VMEM((seq // bq, INNER, opm, bq), bf16),
        pltpu.VMEM((seq // bq, outer_n, opm, bq), bf16),
        pltpu.VMEM((outer_n * opm // 128, INNER * opm, 128), f32),
        pltpu.VMEM((size, width), f32),
        pltpu.VMEM((INNER, outer_n, width), f32),
        pltpu.VMEM((INNER, outer_n, width), f32),
        pltpu.VMEM((size, width), f32),
        pltpu.VMEM((SLOT, size), bf16),
        pltpu.VMEM((group, SLOT, size), bf16),
        pltpu.VMEM((group * SLOT, size), f32),
        pltpu.VMEM((group, SLOT, size), bf16),
        pltpu.VMEM((group, SLOT, size), bf16),
        pltpu.VMEM((size, width), f32),
        pltpu.VMEM((size, width), f32),
    ]


def tail_update(mcols, col_mask, col_weights, z, norm, mask, weights, heads, group, dap, bq=512):
    vm = pl.BlockSpec(memory_space=pltpu.VMEM)
    seq, m_width = mcols.shape
    wc_in, wc_out, wopm_in = col_weights
    opm = wopm_in.shape[1] // 2
    size, width = z.shape
    return pl.pallas_call(
        functools.partial(tail_kernel, group, dap),
        out_shape=(jax.ShapeDtypeStruct((group, seq // group, m_width), bf16), jax.ShapeDtypeStruct((size, width), bf16)),
        in_specs=[vm] * 15,
        out_specs=(vm, vm),
        scratch_shapes=col_scratch(seq, m_width, heads, wc_out.shape[0] // heads, bq)
        + pair_scratch(seq, size, width, opm, group, bq)
        + [pltpu.SemaphoreType.DMA((7,)), pltpu.SemaphoreType.DMA((7,))],
        compiler_params=pltpu.CompilerParams(collective_id=1, has_side_effects=True, vmem_limit_bytes=56 << 20),
        name='tail_update',
    )(mcols, col_mask[None, :], *col_weights, z, norm, mask, *weights)


def gather_slots(block, group, size):
    spread = jnp.broadcast_to(block[None], (size,) + block.shape)
    return lax.all_to_all(spread, group, 0, 0, tiled=True)


def head_bias(x_norm, weight):
    return jnp.einsum('jc,ch->hj', x_norm, weight, preferred_element_type=f32).astype(bf16)


def solution(mesh):
    dap_size = mesh.shape['dap']
    group = ('chip', 'dap')
    group_size = mesh.shape['chip'] * dap_size
    rows = P(('data', 'chip', 'dap'))
    in_specs = (rows, rows, P('data'), P('data')) + (P(),) * 13

    def per_device(m_blk, z_blk, msa_mask, res_mask, w_row_in, w_row_bias, w_row_out, w_col_in, w_col_out,
                   w_opm_in, w_opm_out, w_start_in, w_start_bias, w_start_out, w_end_in, w_end_bias, w_end_out):
        me = lax.axis_index('chip') * dap_size + lax.axis_index('dap')
        seqs, res, width = m_blk.shape
        total = seqs * group_size
        heads_m = w_row_bias.shape[1]
        res_row = res_mask[None, :]

        row_bias = gather_slots(head_bias(norm_rows(z_blk[0]), w_row_bias), group, group_size).astype(f32)
        seq_mask = lax.dynamic_slice_in_dim(msa_mask, me * seqs, seqs, axis=0)
        m_blk = attend(m_blk.reshape(seqs * res, width), row_bias, seq_mask, w_row_in, w_row_out, True, True, 'row_attention')

        m_cols = lax.all_to_all(m_blk.reshape(seqs, res, width), group, 1, 0, tiled=True)
        col_mask = lax.dynamic_slice_in_dim(msa_mask, me, 1, axis=1)[:, 0]
        weight = msa_mask.astype(bf16)
        pair_norm = jnp.einsum('s,sj->j', col_mask.astype(bf16), weight, preferred_element_type=f32)
        pair_norm = jnp.broadcast_to(pair_norm[:, None], (res, z_blk.shape[2]))
        weights = (w_opm_out, w_start_in, w_start_bias, w_start_out, w_end_in, w_end_bias, w_end_out)
        m_slots, z_out = tail_update(m_cols.reshape(total, width), col_mask, (w_col_in, w_col_out, w_opm_in), z_blk[0],
                                     pair_norm, res_row, weights, heads_m, group_size, dap_size)
        m_out, z_out = jnp.swapaxes(m_slots, 0, 1), z_out[None]
        return m_out, z_out

    return jax.shard_map(per_device, mesh=mesh, in_specs=in_specs, out_specs=(rows, rows), check_vma=False)
```

```python
import functools

import jax
import jax.numpy as jnp
import numpy as np
from jax import lax
from jax.experimental import pallas as pl
from jax.experimental.pallas import tpu as pltpu
from jax.sharding import PartitionSpec as P

LOG2E = 1.4426950408889634
f32, bf16 = jnp.float32, jnp.bfloat16


def split3(value):
    parts = []
    rest = np.float64(value)
    for _ in range(3):
        part = np.float64(np.asarray(rest, dtype=jnp.bfloat16))
        parts.append(float(part))
        rest = rest - part
    return parts


def norm_rows(x):
    values = x.astype(f32)
    centred = values - jnp.mean(values, axis=-1, keepdims=True)
    variance = jnp.mean(centred * centred, axis=-1, keepdims=True)
    return (centred * lax.rsqrt(variance + 1e-5)).astype(bf16)


def dot_t(w, x):
    return lax.dot_general(w, x, (((0,), (1,)), ((), ())), preferred_element_type=f32)


NT = (((1,), (1,)), ((), ()))
TN = (((0,), (0,)), ((), ()))
NEG = -1e9 * LOG2E


def mm(a, b, dims=(((1,), (0,)), ((), ()))):
    return lax.dot_general(a, b, dims, preferred_element_type=f32)


NN = (((1,), (0,)), ((), ()))
MESH = pl.DeviceIdType.MESH
INNER = 8
SLOT = 8


def place(t, dap):
    return (0, t // dap, t % dap)


def pair_project(x, win_ref, fold):
    xn = norm_rows(x)
    k = mm(xn, win_ref[:, fold:2 * fold]).astype(bf16)
    qt = dot_t(win_ref[:, :fold], xn).astype(bf16)
    vt = dot_t(win_ref[:, 2 * fold:3 * fold], xn).astype(bf16)
    gg = dot_t(win_ref[:, 3 * fold:], xn).astype(bf16).astype(f32)
    return k, qt, vt, 1.0 / (1.0 + jnp.exp(-gg))


def pair_attend(x, parts, biases, keep, wout_ref):
    k, qt, vt, sig = parts
    heads = len(biases)
    hd = vt.shape[0] // heads
    c = hd ** -0.5 * LOG2E
    gated = []
    for h in range(heads):
        part = slice(h * hd, (h + 1) * hd)
        t = mm(k[:, part], qt[part]) * c + biases[h] * LOG2E
        t = jnp.where(keep, t, NEG)
        e = jnp.exp2(t - jnp.max(t, axis=0, keepdims=True))
        mixed = mm(vt[part], e.astype(bf16)) / jnp.sum(e, axis=0, keepdims=True)
        gated.append((mixed * sig[part]).astype(bf16))
    up = mm(jnp.concatenate(gated, axis=0), wout_ref[...], TN)
    return (x.astype(f32) + up).astype(bf16)


def col_stage(load, seq, mrow_ref, win_ref, wout_ref, wopm_ref, emit,
              kaug, qaug, vt, sig, gat, s0, s1, wt, wka):
    heads, hd = vt.shape[0], vt.shape[1]
    fold = heads * hd
    bq = s0.shape[1]
    nq = seq // bq
    kc = 256
    nk = seq // kc
    c = hd ** -0.5 * LOG2E
    masked = split3(-1e9 * LOG2E)

    lane = lax.broadcasted_iota(jnp.int32, (bq, 128), 1)
    row = lax.broadcasted_iota(jnp.int32, (128 - 3 * hd, bq), 0)
    fill = jnp.where(row == 0, masked[0], jnp.where(row == 1, masked[1], jnp.where(row == 2, masked[2], 0.0))).astype(bf16)
    flag = ((lane >= 3 * hd) & (lane < 3 * hd + 3)).astype(f32)
    flag2 = jnp.concatenate([flag, flag], axis=1)

    wt[...] = jnp.transpose(win_ref[...])
    for h in range(heads):
        wk = win_ref[:, fold + h * hd:fold + (h + 1) * hd]
        wka[:, h * 128:(h + 1) * 128] = jnp.concatenate([wk, wk, wk, jnp.zeros_like(wk)], axis=1)

    def project(b, carry):
        rows = pl.ds(pl.multiple_of(b * bq, bq), bq)
        xn = norm_rows(load(b))
        keep = jnp.transpose(jnp.broadcast_to(mrow_ref[0:1, rows], (128, bq))) != 0
        keep2 = jnp.concatenate([keep, keep], axis=1)
        for h in range(0, heads, 2):
            k = mm(xn, wka[:, h * 128:(h + 2) * 128])
            k = jnp.where(keep2, k, flag2).astype(bf16)
            kaug[h, rows, :] = k[:, :128]
            kaug[h + 1, rows, :] = k[:, 128:]
        qt = mm(wt[:fold, :], xn, NT).astype(bf16).astype(f32) * c
        hi = qt.astype(bf16)
        rest = qt - hi.astype(f32)
        mid = rest.astype(bf16)
        low = (rest - mid.astype(f32)).astype(bf16)
        vv = mm(wt[2 * fold:3 * fold, :], xn, NT).astype(bf16)
        gg = mm(wt[3 * fold:, :], xn, NT).astype(bf16).astype(f32)
        gg = 1.0 / (1.0 + jnp.exp(-gg))
        for h in range(heads):
            part = slice(h * hd, (h + 1) * hd)
            qaug[h, 0:hd, rows] = hi[part]
            qaug[h, hd:2 * hd, rows] = mid[part]
            qaug[h, 2 * hd:3 * hd, rows] = low[part]
            qaug[h, 3 * hd:, rows] = fill
            vt[h, :, rows] = vv[part]
            sig[h, :, rows] = gg[part]
        return carry

    lax.fori_loop(0, nq, project, 0)

    def fold8(s):
        return s.reshape(kc // 8, 8, bq)

    def chunk_scores(h, q, i, buf, m):
        s = mm(kaug[h, i * kc:(i + 1) * kc, :], q)
        buf[i * kc:(i + 1) * kc, :] = s
        top = jnp.max(fold8(s), axis=0)
        return top if m is None else jnp.maximum(m, top)

    def step(qb, h, cur, nxt, m):
        t = jnp.minimum(qb * heads + h + 1, nq * heads - 1)
        hn = t % heads
        q = qaug[hn, :, pl.ds(pl.multiple_of(t // heads * bq, bq), bq)]
        top = jnp.max(m, axis=0, keepdims=True)
        mn = None
        total = jnp.zeros((8, bq), f32)
        mixed = jnp.zeros((hd, bq), f32)
        for i in range(nk):
            mn = chunk_scores(hn, q, i, nxt, mn)
            e = jnp.exp2(cur[i * kc:(i + 1) * kc, :] - top)
            total = total + jnp.sum(fold8(e), axis=0)
            mixed = mixed + mm(vt[h, :, i * kc:(i + 1) * kc], e.astype(bf16))
        cols = pl.ds(pl.multiple_of(qb * bq, bq), bq)
        mixed = mixed / jnp.sum(total, axis=0, keepdims=True)
        gat[pl.ds(pl.multiple_of(h * hd, hd), hd), :] = (mixed * sig[h, :, cols]).astype(bf16)
        return mn

    m = None
    for i in range(nk):
        m = chunk_scores(0, qaug[0, :, 0:bq], i, s0, m)

    def block(qb, m):
        def pair(u, m):
            m = step(qb, 2 * u, s0, s1, m)
            return step(qb, 2 * u + 1, s1, s0, m)

        m = lax.fori_loop(0, heads // 2, pair, m)
        rows = pl.ds(pl.multiple_of(qb * bq, bq), bq)
        y = (load(qb).astype(f32) + mm(gat[...], wout_ref[...], TN)).astype(bf16)
        ac = mm(wopm_ref[...], norm_rows(y), NT).astype(bf16)
        emit(qb, y, (ac.astype(f32) * mrow_ref[0:1, rows]).astype(bf16))
        return m

    lax.fori_loop(0, nq, block, m)


class Links:
    def __init__(self, group, dap, send, recv):
        self.group, self.dap, self.send, self.recv = group, dap, send, recv
        self.me = lax.axis_index('chip') * dap + lax.axis_index('dap')
        self.hi, self.lo = self.me // INNER, self.me % INNER
        self.outer_n = group // INNER

    def greet(self):
        barrier = pltpu.get_barrier_semaphore()

        def one(o, carry):
            pl.semaphore_signal(barrier, inc=1, device_id=place((self.me + o) % self.group, self.dap), device_id_type=MESH)
            return carry

        lax.fori_loop(1, self.group, one, 0)

    def ready(self):
        pl.semaphore_wait(pltpu.get_barrier_semaphore(), self.group - 1)

    def copy(self, src, dst, i, t):
        return pltpu.make_async_remote_copy(src_ref=src, dst_ref=dst, send_sem=self.send.at[i], recv_sem=self.recv.at[i],
                                            device_id=place(t, self.dap), device_id_type=MESH)

    def settle(self, part, i):
        done = self.copy(part, part, i, self.me)
        done.wait_send()
        done.wait_recv()

    def to_all(self, make, i):
        def one(o, carry):
            t = (self.me + o) % self.group
            src, dst = make(t)
            self.copy(src, dst, i, t).start()
            return carry

        lax.fori_loop(1, self.group, one, 0)

    def to_inner(self, make, i):
        def one(o, carry):
            x = (self.lo + o) % INNER
            src, dst = make(x)
            self.copy(src, dst, i, self.hi * INNER + x).start()
            return carry

        lax.fori_loop(1, INNER, one, 0)

    def to_outer(self, make, i):
        def one(o, carry):
            src, dst = make()
            self.copy(src, dst, i, (self.hi + o) % self.outer_n * INNER + self.lo).start()
            return carry

        lax.fori_loop(1, self.outer_n, one, 0)


def bias_rows(z, weight):
    rows = mm(weight[...], norm_rows(z), NT).astype(bf16)
    spare = SLOT - rows.shape[0]
    return jnp.concatenate([rows, jnp.zeros((spare, rows.shape[1]), bf16)], axis=0) if spare else rows


def pair_stage(net, z_ref, norm, mask_ref, wopm_ref, ws_in, ws_bias, ws_out, we_in, we_bias, we_out, zout,
               abuf, cbuf, oscr, uscr, usend, ubuf, zrow, bsend, bbuf, bscr, esend, ebuf, zsend, zfin):
    me, lo, group, outer_n = net.me, net.lo, net.group, net.outer_n
    blocks, opm = abuf.shape[0], abuf.shape[2]
    heads = ws_bias.shape[0]
    fold = ws_out.shape[0]
    size = z_ref.shape[0]
    keep = jnp.transpose(jnp.broadcast_to(mask_ref[...].astype(f32), (size, size))) != 0

    per = 128 // opm
    outer = None
    for q in range(blocks):
        term = mm(abuf[q].reshape(INNER * opm, -1), cbuf[q].reshape(outer_n * opm, -1), NT)
        outer = term if outer is None else outer + term
    for g in range(outer_n // per):
        oscr[g] = outer[:, g * 128:(g + 1) * 128]
    lane = lax.broadcasted_iota(jnp.int32, (opm // per * INNER, 128), 1) // opm
    tiles = []
    for g in range(outer_n // per):
        slabs = [jnp.concatenate([oscr[g, pl.ds(b * per + r, INNER, stride=opm), :] for b in range(opm // per)], axis=0)
                 for r in range(per)]
        turned = [[slabs[r] if s == 0 else pltpu.roll(slabs[r], s * opm, 1) for s in range(per)] for r in range(per)]
        for q in range(per):
            pick = turned[0][(0 - q) % per]
            for r in range(1, per):
                pick = jnp.where(lane == r, turned[r][(r - q) % per], pick)
            tiles.append(pick)
    up = None
    for b in range(opm // per):
        block = jnp.concatenate([t[b * INNER:(b + 1) * INNER] for t in tiles], axis=0).astype(bf16)
        term = mm(block, wopm_ref[b * 128:(b + 1) * 128, :])
        up = term if up is None else up + term
    uscr[...] = up
    for x in range(INNER):
        usend[x] = uscr[pl.ds(x, outer_n, stride=INNER), :]
    ubuf[lo] = usend[lo]
    net.to_inner(lambda x: (usend.at[x], ubuf.at[lo]), 3)
    net.settle(ubuf.at[pl.ds(0, INNER - 1)], 3)
    for x in range(INNER):
        zrow[pl.ds(x, outer_n, stride=INNER), :] = ubuf[x]
    z1 = (z_ref[...].astype(f32) + zrow[...] / (1e-3 + norm[...])).astype(bf16)

    bsend[...] = bias_rows(z1, ws_bias)
    bbuf[me] = bsend[...]
    net.to_all(lambda t: (bsend, bbuf.at[me]), 4)
    parts = pair_project(z1, ws_in, fold)
    net.settle(bbuf.at[pl.ds(0, group - 1)], 4)
    bscr[...] = bbuf[...].astype(f32).reshape(group * SLOT, size)
    biases = [jnp.transpose(bscr[pl.ds(h, size, stride=SLOT), :]) for h in range(heads)]
    z2 = pair_attend(z1, parts, biases, keep, ws_out)

    end_rows = bias_rows(z2, we_bias).astype(f32)
    for h in range(heads):
        bscr[pl.ds(h, size, stride=SLOT), :] = jnp.broadcast_to(end_rows[h:h + 1], (size, size))
    bscr[pl.ds(heads, size, stride=SLOT), :] = z2.astype(f32)
    esend[...] = bscr[...].astype(bf16).reshape(group, SLOT, size)
    ebuf[me] = esend[me]
    net.to_all(lambda t: (esend.at[t], ebuf.at[me]), 5)
    net.settle(ebuf.at[pl.ds(0, group - 1)], 5)
    bscr[...] = ebuf[...].astype(f32).reshape(group * SLOT, size)
    zc = bscr[pl.ds(heads, size, stride=SLOT), :].astype(bf16)
    biases = [bscr[pl.ds(h, size, stride=SLOT), :] for h in range(heads)]
    z3 = pair_attend(zc, pair_project(zc, we_in, fold), biases, keep, we_out)

    zsend[...] = z3.astype(f32)
    zfin[pl.ds(me, 1), :] = zsend[pl.ds(me, 1), :]
    net.to_all(lambda t: (zsend.at[pl.ds(t, 1)], zfin.at[pl.ds(me, 1)]), 6)
    net.settle(zfin.at[pl.ds(0, group - 1)], 6)
    zout[...] = zfin[...].astype(bf16)


def row_stage(net, x_ref, z_ref, mask_ref, wb_ref, win_ref, wout_ref, ship, side,
              kk, qt, vt, sig, gat, bias, wt, qd0, qd1, bsend, bbuf, bscr, ytr):
    tokens, width = x_ref.shape
    size = bias.shape[0]
    seqs = tokens // size
    heads = bias.shape[1] // size
    fold = gat.shape[0]
    hd = fold // heads
    c = hd ** -0.5 * LOG2E
    bp = 512
    me, group = net.me, net.group

    net.greet()
    bsend[...] = bias_rows(z_ref[...], wb_ref)
    bbuf[me] = bsend[...]
    wt[...] = jnp.transpose(win_ref[...])
    qd0[...] = jnp.zeros_like(qd0)
    qd1[...] = jnp.zeros_like(qd1)

    def project(b, carry):
        rows = pl.ds(pl.multiple_of(b * bp, bp), bp)
        xn = norm_rows(x_ref[rows, :])
        kk[rows, :] = mm(xn, win_ref[:, fold:2 * fold]).astype(bf16)
        qt[:, rows] = mm(wt[:fold, :], xn, NT).astype(bf16)
        vt[:, rows] = mm(wt[2 * fold:3 * fold, :], xn, NT).astype(bf16)
        gg = mm(wt[3 * fold:, :], xn, NT).astype(bf16).astype(f32)
        sig[:, rows] = 1.0 / (1.0 + jnp.exp(-gg))

        @pl.when(b == 1)
        def _():
            net.ready()
            net.to_all(lambda t: (bsend, bbuf.at[me]), 7)

        return carry

    lax.fori_loop(0, tokens // bp, project, 0)
    side()
    net.settle(bbuf.at[pl.ds(0, group - 1)], 7)
    bscr[...] = bbuf[...].astype(f32).reshape(group * SLOT, size)
    for h in range(heads):
        bias[:, h * size:(h + 1) * size] = jnp.transpose(bscr[pl.ds(h, size, stride=SLOT), :] * LOG2E)

    def one(s, qd):
        cols = pl.ds(pl.multiple_of(s * size, size), size)
        for h in range(heads):
            qd[h * hd:(h + 1) * hd, h * size:(h + 1) * size] = qt[h * hd:(h + 1) * hd, cols]
        mrow = mask_ref[pl.ds(me * seqs + s, 1), :]
        keep = jnp.transpose(jnp.broadcast_to(mrow.astype(f32), (size, size))) != 0
        keep2 = jnp.concatenate([keep, keep], axis=1)
        for h in range(0, heads, 2):
            two = slice(h * size, (h + 2) * size)
            t = mm(kk[cols, :], qd[:, two]) * c + bias[:, two]
            t = jnp.where(keep2, t, NEG)
            e = jnp.exp2(t - jnp.max(t, axis=0, keepdims=True))
            total = jnp.sum(e, axis=0, keepdims=True)
            mixed = mm(vt[h * hd:(h + 2) * hd, cols], e.astype(bf16)) / total
            gat[h * hd:(h + 1) * hd, cols] = (mixed[:hd, :size] * sig[h * hd:(h + 1) * hd, cols]).astype(bf16)
            gat[(h + 1) * hd:(h + 2) * hd, cols] = (mixed[hd:, size:] * sig[(h + 1) * hd:(h + 2) * hd, cols]).astype(bf16)

    def chunk(k, carry):
        def pair(u, carry):
            one(k * SLOT + 2 * u, qd0)
            one(k * SLOT + 2 * u + 1, qd1)
            return carry

        lax.fori_loop(0, SLOT // 2, pair, 0)
        for b in range(SLOT * size // bp):
            rows = pl.ds(pl.multiple_of((k * SLOT * size // bp + b) * bp, bp), bp)
            y = (x_ref[rows, :].astype(f32) + mm(gat[:, rows], wout_ref[...], TN)).astype(bf16).astype(f32)
            for i in range(bp // size):
                for half in range(width // 128):
                    ytr[half, pl.ds(b * (bp // size) + i, size, stride=SLOT), :] = (
                        y[i * size:(i + 1) * size, half * 128:(half + 1) * 128])
        ship(k, jnp.concatenate([ytr[half] for half in range(width // 128)], axis=1).astype(bf16))
        return carry

    lax.fori_loop(0, seqs // SLOT, chunk, 0)


def block_kernel(group, dap, m_ref, z_ref, mask_ref, res_ref, wr_in, wr_bias, wr_out, wc_in, wc_out, wopm_in, wopm_out,
                 ws_in, ws_bias, ws_out, we_in, we_bias, we_out, mout, zout,
                 kk, qt, rvt, rsig, rgat, bias, rwt, qd0, qd1, rsend, rbuf, rscr, ytr, msend, xbuf, mrow, norm,
                 kaug, qaug, vt, sig, gat, s0, s1, wt, wka, ycol, acs, abuf, cbuf,
                 oscr, uscr, usend, ubuf, zrow, bsend, bbuf, bscr, esend, ebuf, zsend, zfin, send, recv):
    net = Links(group, dap, send, recv)
    me, lo, hi = net.me, net.lo, net.hi
    opm = abuf.shape[2]
    seq, size = mask_ref.shape
    chunks = xbuf.shape[0]
    bq = s0.shape[1]
    per = bq // SLOT
    turns = group // per

    def side():
        flags = mask_ref[...].astype(bf16)
        pick = (lax.broadcasted_iota(jnp.int32, (size, size), 0) == me).astype(bf16)
        norm[...] = mm(flags, mm(flags, pick).astype(bf16), TN)
        row = (lax.broadcasted_iota(jnp.int32, (SLOT, size), 1) == me).astype(bf16)
        split = mask_ref[...].reshape(group, chunks, SLOT, size)
        for k in range(chunks):
            mrow[:, k * group * SLOT:(k + 1) * group * SLOT] = mm(
                row, split[:, k].astype(f32).reshape(group * SLOT, size).astype(bf16), NT)

    def ship(k, y):
        msend[k] = y.astype(f32).reshape(group, SLOT, -1).astype(bf16)
        xbuf[k, me] = msend[k, me]
        net.to_all(lambda t: (msend.at[k, t], xbuf.at[k, me]), 8)

    row_stage(net, m_ref, z_ref, mask_ref, wr_bias, wr_in, wr_out, ship, side,
              kk, qt, rvt, rsig, rgat, bias, rwt, qd0, qd1, rsend, rbuf, rscr, ytr)
    net.settle(xbuf.at[:, pl.ds(0, group - 1)], 8)

    def load(b):
        part = xbuf[b // turns, pl.ds(pl.multiple_of(b % turns * per, per), per)]
        return part.astype(f32).reshape(bq, -1)

    def emit(qb, y, ac):
        ycol[qb] = y.astype(f32).reshape(per, SLOT, -1).astype(bf16)
        acs[qb] = ac
        abuf[qb, lo] = ac[:opm]
        cbuf[qb, hi] = ac[opm:]
        net.to_outer(lambda: (acs.at[qb, pl.ds(opm, opm)], cbuf.at[qb, hi]), 1)
        net.to_inner(lambda x: (acs.at[qb, pl.ds(0, opm)], abuf.at[qb, lo]), 0)

        def share_m(o, carry):
            i = (me + o) % per
            t = qb % turns * per + i

            @pl.when(t != me)
            def _():
                net.copy(ycol.at[qb, i], mout.at[qb // turns, me], 2, t).start()

            return carry

        lax.fori_loop(0, per, share_m, 0)

    col_stage(load, seq, mrow, wc_in, wc_out, wopm_in, emit, kaug, qaug, vt, sig, gat, s0, s1, wt, wka)
    for k in range(chunks):
        mout[k, me] = ycol[k * turns + me // per, me % per]
    net.settle(cbuf.at[:, pl.ds(0, net.outer_n - 1)], 1)
    net.settle(abuf.at[:, pl.ds(0, INNER - 1)], 0)
    pair_stage(net, z_ref, norm, res_ref, wopm_out, ws_in, ws_bias, ws_out, we_in, we_bias, we_out, zout,
               abuf, cbuf, oscr, uscr, usend, ubuf, zrow, bsend, bbuf, bscr, esend, ebuf, zsend, zfin)
    net.settle(mout.at[:, pl.ds(0, group - 1)], 2)


def row_scratch(tokens, size, width, heads, fold, group):
    seqs = tokens // size
    return [
        pltpu.VMEM((tokens, fold), bf16),
        pltpu.VMEM((fold, tokens), bf16),
        pltpu.VMEM((fold, tokens), bf16),
        pltpu.VMEM((fold, tokens), f32),
        pltpu.VMEM((fold, tokens), bf16),
        pltpu.VMEM((size, heads * size), f32),
        pltpu.VMEM((4 * fold, width), bf16),
        pltpu.VMEM((fold, heads * size), bf16),
        pltpu.VMEM((fold, heads * size), bf16),
        pltpu.VMEM((SLOT, size), bf16),
        pltpu.VMEM((group, SLOT, size), bf16),
        pltpu.VMEM((group * SLOT, size), f32),
        pltpu.VMEM((width // 128, SLOT * size, 128), f32),
        pltpu.VMEM((seqs // SLOT, group, SLOT, width), bf16),
        pltpu.VMEM((seqs // SLOT, group, SLOT, width), bf16),
        pltpu.VMEM((SLOT, seqs * group), f32),
        pltpu.VMEM((size, size), f32),
    ]


def col_scratch(seq, width, heads, hd, bq):
    return [
        pltpu.VMEM((heads, seq, 128), bf16),
        pltpu.VMEM((heads, 128, seq), bf16),
        pltpu.VMEM((heads, hd, seq), bf16),
        pltpu.VMEM((heads, hd, seq), f32),
        pltpu.VMEM((heads * hd, bq), bf16),
        pltpu.VMEM((seq, bq), f32),
        pltpu.VMEM((seq, bq), f32),
        pltpu.VMEM((4 * heads * hd, width), bf16),
        pltpu.VMEM((width, heads * 128), bf16),
        pltpu.VMEM((seq // bq, bq // SLOT, SLOT, width), bf16),
    ]


def pair_scratch(seq, size, width, opm, group, bq):
    outer_n = group // INNER
    return [
        pltpu.VMEM((seq // bq, 2 * opm, bq), bf16),
        pltpu.VMEM((seq // bq, INNER, opm, bq), bf16),
        pltpu.VMEM((seq // bq, outer_n, opm, bq), bf16),
        pltpu.VMEM((outer_n * opm // 128, INNER * opm, 128), f32),
        pltpu.VMEM((size, width), f32),
        pltpu.VMEM((INNER, outer_n, width), f32),
        pltpu.VMEM((INNER, outer_n, width), f32),
        pltpu.VMEM((size, width), f32),
        pltpu.VMEM((SLOT, size), bf16),
        pltpu.VMEM((group, SLOT, size), bf16),
        pltpu.VMEM((group * SLOT, size), f32),
        pltpu.VMEM((group, SLOT, size), bf16),
        pltpu.VMEM((group, SLOT, size), bf16),
        pltpu.VMEM((size, width), f32),
        pltpu.VMEM((size, width), f32),
    ]


def block_update(m, z, msa_mask, res_mask, weights, heads, group, dap, bq=512):
    vm = pl.BlockSpec(memory_space=pltpu.VMEM)
    tokens, m_width = m.shape
    size, width = z.shape
    seqs = tokens // size
    seq = seqs * group
    fold = weights[2].shape[0]
    opm = weights[5].shape[0] // 2
    return pl.pallas_call(
        functools.partial(block_kernel, group, dap),
        out_shape=(jax.ShapeDtypeStruct((seqs // SLOT, group, SLOT, m_width), bf16), jax.ShapeDtypeStruct((size, width), bf16)),
        in_specs=[vm] * (4 + len(weights)),
        out_specs=(vm, vm),
        scratch_shapes=row_scratch(tokens, size, m_width, heads, fold, group)
        + col_scratch(seq, m_width, heads, fold // heads, bq)
        + pair_scratch(seq, size, width, opm, group, bq)
        + [pltpu.SemaphoreType.DMA((9,)), pltpu.SemaphoreType.DMA((9,))],
        compiler_params=pltpu.CompilerParams(collective_id=1, has_side_effects=True, vmem_limit_bytes=63 << 20),
        name='block_update',
    )(m, z, msa_mask, res_mask, *weights)


def solution(mesh):
    dap_size = mesh.shape['dap']
    group_size = mesh.shape['chip'] * dap_size
    rows = P(('data', 'chip', 'dap'))
    in_specs = (rows, rows, P('data'), P('data')) + (P(),) * 13

    def per_device(m_blk, z_blk, msa_mask, res_mask, w_row_in, w_row_bias, w_row_out, w_col_in, w_col_out,
                   w_opm_in, w_opm_out, w_start_in, w_start_bias, w_start_out, w_end_in, w_end_bias, w_end_out):
        seqs, res, width = m_blk.shape
        weights = (w_row_in, w_row_bias.T, w_row_out, w_col_in, w_col_out, w_opm_in.T, w_opm_out,
                   w_start_in, w_start_bias.T, w_start_out, w_end_in, w_end_bias.T, w_end_out)
        slots, z_out = block_update(m_blk.reshape(seqs * res, width), z_blk[0], msa_mask, res_mask[None, :], weights,
                                    w_row_bias.shape[1], group_size, dap_size)
        m_out = jnp.swapaxes(slots, 1, 2).reshape(seqs, res, width)
        return m_out, z_out[None]

    return jax.shard_map(per_device, mesh=mesh, in_specs=in_specs, out_specs=(rows, rows), check_vma=False)
```

```python
import functools

import jax
import jax.numpy as jnp
import numpy as np
from jax import lax
from jax.experimental import pallas as pl
from jax.experimental.pallas import tpu as pltpu
from jax.sharding import PartitionSpec as P

LOG2E = 1.4426950408889634
f32, bf16 = jnp.float32, jnp.bfloat16


def split3(value):
    parts = []
    rest = np.float64(value)
    for _ in range(3):
        part = np.float64(np.asarray(rest, dtype=jnp.bfloat16))
        parts.append(float(part))
        rest = rest - part
    return parts


def norm_rows(x):
    values = x.astype(f32)
    centred = values - jnp.mean(values, axis=-1, keepdims=True)
    variance = jnp.mean(centred * centred, axis=-1, keepdims=True)
    return (centred * lax.rsqrt(variance + 1e-5)).astype(bf16)


def dot_t(w, x):
    return lax.dot_general(w, x, (((0,), (1,)), ((), ())), preferred_element_type=f32)


NT = (((1,), (1,)), ((), ()))
TN = (((0,), (0,)), ((), ()))
NEG = -1e9 * LOG2E


def mm(a, b, dims=(((1,), (0,)), ((), ()))):
    return lax.dot_general(a, b, dims, preferred_element_type=f32)


NN = (((1,), (0,)), ((), ()))
MESH = pl.DeviceIdType.MESH
INNER = 8
SLOT = 8


def place(t, dap):
    return (0, lax.div(t, dap), lax.rem(t, dap))


def pair_project(x, win_ref, fold):
    xn = norm_rows(x)
    k = mm(xn, win_ref[:, fold:2 * fold]).astype(bf16)
    qt = dot_t(win_ref[:, :fold], xn).astype(bf16)
    vt = dot_t(win_ref[:, 2 * fold:3 * fold], xn).astype(bf16)
    gg = dot_t(win_ref[:, 3 * fold:], xn).astype(bf16).astype(f32)
    return k, qt, vt, 1.0 / (1.0 + jnp.exp(-gg))


def pair_attend(x, parts, biases, keep, wout_ref):
    k, qt, vt, sig = parts
    heads = len(biases)
    hd = vt.shape[0] // heads
    c = hd ** -0.5 * LOG2E
    gated = []
    for h in range(heads):
        part = slice(h * hd, (h + 1) * hd)
        t = mm(k[:, part], qt[part]) * c + biases[h] * LOG2E
        t = jnp.where(keep, t, NEG)
        e = jnp.exp2(t - jnp.max(t, axis=0, keepdims=True))
        mixed = mm(vt[part], e.astype(bf16)) / jnp.sum(e, axis=0, keepdims=True)
        gated.append((mixed * sig[part]).astype(bf16))
    up = mm(jnp.concatenate(gated, axis=0), wout_ref[...], TN)
    return (x.astype(f32) + up).astype(bf16)


def col_stage(arrive, load, seq, mrow_ref, win_ref, wout_ref, wopm_ref, emit,
              kaug, qaug, vt, sig, gat, s0, s1, wt, wka):
    heads, hd = vt.shape[0], vt.shape[1]
    fold = heads * hd
    bq = s0.shape[1]
    nq = seq // bq
    kc = 256
    nk = seq // kc
    c = hd ** -0.5 * LOG2E
    masked = split3(-1e9 * LOG2E)

    lane = lax.broadcasted_iota(jnp.int32, (bq, 128), 1)
    row = lax.broadcasted_iota(jnp.int32, (128 - 3 * hd, bq), 0)
    fill = jnp.where(row == 0, masked[0], jnp.where(row == 1, masked[1], jnp.where(row == 2, masked[2], 0.0))).astype(bf16)
    flag = ((lane >= 3 * hd) & (lane < 3 * hd + 3)).astype(f32)
    flag2 = jnp.concatenate([flag, flag], axis=1)

    wt[...] = jnp.transpose(win_ref[...])
    for h in range(heads):
        wk = win_ref[:, fold + h * hd:fold + (h + 1) * hd]
        wka[:, h * 128:(h + 1) * 128] = jnp.concatenate([wk, wk, wk, jnp.zeros_like(wk)], axis=1)

    def project(b, carry):
        rows = pl.ds(pl.multiple_of(b * bq, bq), bq)
        arrive(b)
        xn = norm_rows(load(b))
        keep = jnp.transpose(jnp.broadcast_to(mrow_ref[0:1, rows], (128, bq))) != 0
        keep2 = jnp.concatenate([keep, keep], axis=1)
        for h in range(0, heads, 2):
            k = mm(xn, wka[:, h * 128:(h + 2) * 128])
            k = jnp.where(keep2, k, flag2).astype(bf16)
            kaug[h, rows, :] = k[:, :128]
            kaug[h + 1, rows, :] = k[:, 128:]
        qt = mm(wt[:fold, :], xn, NT).astype(bf16).astype(f32) * c
        hi = qt.astype(bf16)
        rest = qt - hi.astype(f32)
        mid = rest.astype(bf16)
        low = (rest - mid.astype(f32)).astype(bf16)
        vv = mm(wt[2 * fold:3 * fold, :], xn, NT).astype(bf16)
        gg = mm(wt[3 * fold:, :], xn, NT).astype(bf16).astype(f32)
        gg = 1.0 / (1.0 + jnp.exp(-gg))
        for h in range(heads):
            part = slice(h * hd, (h + 1) * hd)
            qaug[h, 0:hd, rows] = hi[part]
            qaug[h, hd:2 * hd, rows] = mid[part]
            qaug[h, 2 * hd:3 * hd, rows] = low[part]
            qaug[h, 3 * hd:, rows] = fill
            vt[h, :, rows] = vv[part]
            sig[h, :, rows] = gg[part]
        return carry

    lax.fori_loop(0, nq, project, 0)

    def fold8(s):
        return s.reshape(kc // 8, 8, bq)

    def chunk_scores(h, q, i, buf, m):
        s = mm(kaug[h, i * kc:(i + 1) * kc, :], q)
        buf[i * kc:(i + 1) * kc, :] = s
        top = jnp.max(fold8(s), axis=0)
        return top if m is None else jnp.maximum(m, top)

    def step(qb, h, cur, nxt, m):
        t = jnp.minimum(qb * heads + h + 1, nq * heads - 1)
        hn = t % heads
        q = qaug[hn, :, pl.ds(pl.multiple_of(t // heads * bq, bq), bq)]
        top = jnp.max(m, axis=0, keepdims=True)
        mn = None
        total = jnp.zeros((8, bq), f32)
        mixed = jnp.zeros((hd, bq), f32)
        for i in range(nk):
            mn = chunk_scores(hn, q, i, nxt, mn)
            e = jnp.exp2(cur[i * kc:(i + 1) * kc, :] - top)
            total = total + jnp.sum(fold8(e), axis=0)
            mixed = mixed + mm(vt[h, :, i * kc:(i + 1) * kc], e.astype(bf16))
        cols = pl.ds(pl.multiple_of(qb * bq, bq), bq)
        mixed = mixed / jnp.sum(total, axis=0, keepdims=True)
        gat[pl.ds(pl.multiple_of(h * hd, hd), hd), :] = (mixed * sig[h, :, cols]).astype(bf16)
        return mn

    m = None
    for i in range(nk):
        m = chunk_scores(0, qaug[0, :, 0:bq], i, s0, m)

    def block(qb, m):
        def pair(u, m):
            m = step(qb, 2 * u, s0, s1, m)
            return step(qb, 2 * u + 1, s1, s0, m)

        m = lax.fori_loop(0, heads // 2, pair, m)
        rows = pl.ds(pl.multiple_of(qb * bq, bq), bq)
        y = (load(qb).astype(f32) + mm(gat[...], wout_ref[...], TN)).astype(bf16)
        ac = mm(wopm_ref[...], norm_rows(y), NT).astype(bf16)
        emit(qb, y, (ac.astype(f32) * mrow_ref[0:1, rows]).astype(bf16))
        return m

    lax.fori_loop(0, nq, block, m)


def each(start, stop, one, step=8):
    whole = (stop - start) // step

    def some(i, carry):
        for j in range(step):
            one(start + i * step + j)
        return carry

    lax.fori_loop(0, whole, some, 0)
    for o in range(start + whole * step, stop):
        one(o)


class Links:
    def __init__(self, group, dap, send, recv):
        self.group, self.dap, self.send, self.recv = group, dap, send, recv
        self.me = lax.axis_index('chip') * dap + lax.axis_index('dap')
        self.hi, self.lo = lax.div(self.me, INNER), lax.rem(self.me, INNER)
        self.outer_n = group // INNER

    def greet(self):
        barrier = pltpu.get_barrier_semaphore()

        def one(o):
            t = lax.rem(self.me + o, self.group)
            pl.semaphore_signal(barrier, inc=1, device_id=place(t, self.dap), device_id_type=MESH)

        each(1, self.group, one)

    def ready(self):
        pl.semaphore_wait(pltpu.get_barrier_semaphore(), self.group - 1)

    def copy(self, src, dst, i, t):
        return pltpu.make_async_remote_copy(src_ref=src, dst_ref=dst, send_sem=self.send.at[i], recv_sem=self.recv.at[i],
                                            device_id=place(t, self.dap), device_id_type=MESH)

    def settle(self, part, i):
        done = self.copy(part, part, i, self.me)
        done.wait_send()
        done.wait_recv()

    def to_all(self, make, i):
        def one(o):
            t = lax.rem(self.me + o, self.group)
            src, dst = make(t)
            self.copy(src, dst, i, t).start()

        each(1, self.group, one)

    def to_inner(self, make, i):
        for o in range(1, INNER):
            x = lax.rem(self.lo + o, INNER)
            src, dst = make(x)
            self.copy(src, dst, i, self.hi * INNER + x).start()

    def to_half(self, src, dst, i):
        half = self.outer_n // 2
        base = lax.div(self.hi, half) * half
        for o in range(1, half):
            y = base + lax.rem(lax.rem(self.hi, half) + o, half)
            self.copy(src, dst, i, y * INNER + self.lo).start()

    def to_partner(self, part, i):
        self.copy(part, part, i, lax.rem(self.me + self.group // 2, self.group)).start()


def bias_rows(z, weight):
    rows = mm(weight[...], norm_rows(z), NT).astype(bf16)
    spare = SLOT - rows.shape[0]
    return jnp.concatenate([rows, jnp.zeros((spare, rows.shape[1]), bf16)], axis=0) if spare else rows


def pair_stage(net, z_ref, norm, mask_ref, wopm_ref, ws_in, ws_bias, ws_out, we_in, we_bias, we_out, zout,
               abuf, cbuf, oscr, uscr, usend, ubuf, zrow, bsend, bbuf, bscr, esend, ebuf, zsend, zfin):
    me, lo, group, outer_n = net.me, net.lo, net.group, net.outer_n
    blocks, opm = abuf.shape[0], abuf.shape[2]
    heads = ws_bias.shape[0]
    fold = ws_out.shape[0]
    size = z_ref.shape[0]
    keep = jnp.transpose(jnp.broadcast_to(mask_ref[...].astype(f32), (size, size))) != 0

    per = 128 // opm
    outer = None
    for q in range(blocks):
        term = mm(abuf[q].reshape(INNER * opm, -1), cbuf[q].reshape(outer_n * opm, -1), NT)
        outer = term if outer is None else outer + term
    for g in range(outer_n // per):
        oscr[g] = outer[:, g * 128:(g + 1) * 128]
    lane = lax.broadcasted_iota(jnp.int32, (opm // per * INNER, 128), 1) // opm
    tiles = []
    for g in range(outer_n // per):
        slabs = [jnp.concatenate([oscr[g, pl.ds(b * per + r, INNER, stride=opm), :] for b in range(opm // per)], axis=0)
                 for r in range(per)]
        turned = [[slabs[r] if s == 0 else pltpu.roll(slabs[r], s * opm, 1) for s in range(per)] for r in range(per)]
        for q in range(per):
            pick = turned[0][(0 - q) % per]
            for r in range(1, per):
                pick = jnp.where(lane == r, turned[r][(r - q) % per], pick)
            tiles.append(pick)
    up = None
    for b in range(opm // per):
        block = jnp.concatenate([t[b * INNER:(b + 1) * INNER] for t in tiles], axis=0).astype(bf16)
        term = mm(block, wopm_ref[b * 128:(b + 1) * 128, :])
        up = term if up is None else up + term
    uscr[...] = up
    for x in range(INNER):
        usend[x] = uscr[pl.ds(x, outer_n, stride=INNER), :]
    ubuf[lo] = usend[lo]
    net.to_inner(lambda x: (usend.at[x], ubuf.at[lo]), 3)
    net.settle(ubuf.at[pl.ds(0, INNER - 1)], 3)
    for x in range(INNER):
        zrow[pl.ds(x, outer_n, stride=INNER), :] = ubuf[x]
    z1 = (z_ref[...].astype(f32) + zrow[...] / (1e-3 + norm[...])).astype(bf16)

    bsend[...] = bias_rows(z1, ws_bias)
    bbuf[me] = bsend[...]
    net.to_all(lambda t: (bsend, bbuf.at[me]), 4)
    parts = pair_project(z1, ws_in, fold)
    net.settle(bbuf.at[pl.ds(0, group - 1)], 4)
    bscr[...] = bbuf[...].astype(f32).reshape(group * SLOT, size)
    biases = [jnp.transpose(bscr[pl.ds(h, size, stride=SLOT), :]) for h in range(heads)]
    z2 = pair_attend(z1, parts, biases, keep, ws_out)

    end_rows = bias_rows(z2, we_bias).astype(f32)
    for h in range(heads):
        bscr[pl.ds(h, size, stride=SLOT), :] = jnp.broadcast_to(end_rows[h:h + 1], (size, size))
    bscr[pl.ds(heads, size, stride=SLOT), :] = z2.astype(f32)
    esend[...] = bscr[...].astype(bf16).reshape(group, SLOT, size)
    ebuf[me] = esend[me]
    net.to_all(lambda t: (esend.at[t], ebuf.at[me]), 5)
    net.settle(ebuf.at[pl.ds(0, group - 1)], 5)
    bscr[...] = ebuf[...].astype(f32).reshape(group * SLOT, size)
    zc = bscr[pl.ds(heads, size, stride=SLOT), :].astype(bf16)
    biases = [bscr[pl.ds(h, size, stride=SLOT), :] for h in range(heads)]
    z3 = pair_attend(zc, pair_project(zc, we_in, fold), biases, keep, we_out)

    zsend[...] = z3.astype(f32)
    zfin[pl.ds(me, 1), :] = zsend[pl.ds(me, 1), :]
    net.to_all(lambda t: (zsend.at[pl.ds(t, 1)], zfin.at[pl.ds(me, 1)]), 6)
    net.settle(zfin.at[pl.ds(0, group - 1)], 6)
    zout[...] = zfin[...].astype(bf16)


def row_stage(net, x_ref, z_ref, mask_ref, wb_ref, win_ref, wout_ref, ship, side,
              kk, qt, vt, sig, gat, bias, wt, qd0, qd1, bsend, bbuf, bscr, ytr):
    tokens, width = x_ref.shape
    size = bias.shape[0]
    seqs = tokens // size
    heads = bias.shape[1] // size
    fold = gat.shape[0]
    hd = fold // heads
    c = hd ** -0.5 * LOG2E
    bp = 512
    me, group = net.me, net.group

    net.greet()
    bsend[...] = bias_rows(z_ref[...], wb_ref)
    bbuf[me] = bsend[...]
    wt[...] = jnp.transpose(win_ref[...])
    qd0[...] = jnp.zeros_like(qd0)
    qd1[...] = jnp.zeros_like(qd1)

    def project(b, carry):
        rows = pl.ds(pl.multiple_of(b * bp, bp), bp)
        xn = norm_rows(x_ref[rows, :])
        kk[rows, :] = mm(xn, win_ref[:, fold:2 * fold]).astype(bf16)
        qt[:, rows] = mm(wt[:fold, :], xn, NT).astype(bf16)
        vt[:, rows] = mm(wt[2 * fold:3 * fold, :], xn, NT).astype(bf16)
        gg = mm(wt[3 * fold:, :], xn, NT).astype(bf16).astype(f32)
        sig[:, rows] = 1.0 / (1.0 + jnp.exp(-gg))

        @pl.when(b == 0)
        def _():
            net.ready()
            net.to_all(lambda t: (bsend, bbuf.at[me]), 7)

        return carry

    lax.fori_loop(0, tokens // bp, project, 0)
    side()
    net.settle(bbuf.at[pl.ds(0, group - 1)], 7)
    bscr[...] = bbuf[...].astype(f32).reshape(group * SLOT, size)
    for h in range(heads):
        bias[:, h * size:(h + 1) * size] = jnp.transpose(bscr[pl.ds(h, size, stride=SLOT), :] * LOG2E)

    def one(s, qd):
        cols = pl.ds(pl.multiple_of(s * size, size), size)
        for h in range(heads):
            qd[h * hd:(h + 1) * hd, h * size:(h + 1) * size] = qt[h * hd:(h + 1) * hd, cols]
        mrow = mask_ref[pl.ds(me * seqs + s, 1), :]
        keep = jnp.transpose(jnp.broadcast_to(mrow.astype(f32), (size, size))) != 0
        keep2 = jnp.concatenate([keep, keep], axis=1)
        for h in range(0, heads, 2):
            two = slice(h * size, (h + 2) * size)
            t = mm(kk[cols, :], qd[:, two]) * c + bias[:, two]
            t = jnp.where(keep2, t, NEG)
            e = jnp.exp2(t - jnp.max(t, axis=0, keepdims=True))
            total = jnp.sum(e, axis=0, keepdims=True)
            mixed = mm(vt[h * hd:(h + 2) * hd, cols], e.astype(bf16)) / total
            gat[h * hd:(h + 1) * hd, cols] = (mixed[:hd, :size] * sig[h * hd:(h + 1) * hd, cols]).astype(bf16)
            gat[(h + 1) * hd:(h + 2) * hd, cols] = (mixed[hd:, size:] * sig[(h + 1) * hd:(h + 2) * hd, cols]).astype(bf16)

    def chunk(k, carry):
        def pair(u, carry):
            one(k * SLOT + 2 * u, qd0)
            one(k * SLOT + 2 * u + 1, qd1)
            return carry

        lax.fori_loop(0, SLOT // 2, pair, 0)
        for b in range(SLOT * size // bp):
            rows = pl.ds(pl.multiple_of((k * SLOT * size // bp + b) * bp, bp), bp)
            y = (x_ref[rows, :].astype(f32) + mm(gat[:, rows], wout_ref[...], TN)).astype(bf16).astype(f32)
            for i in range(bp // size):
                for half in range(width // 128):
                    ytr[half, pl.ds(b * (bp // size) + i, size, stride=SLOT), :] = (
                        y[i * size:(i + 1) * size, half * 128:(half + 1) * 128])
        ship(k, jnp.concatenate([ytr[half] for half in range(width // 128)], axis=1).astype(bf16))
        return carry

    lax.fori_loop(0, seqs // SLOT, chunk, 0)


def block_kernel(group, dap, m_ref, z_ref, mask_ref, res_ref, wr_in, wr_bias, wr_out, wc_in, wc_out, wopm_in, wopm_out,
                 ws_in, ws_bias, ws_out, we_in, we_bias, we_out, mout, zout,
                 kk, qt, rvt, rsig, rgat, bias, rwt, qd0, qd1, rsend, rbuf, rscr, ytr, msend, xbuf, mrow, norm,
                 kaug, qaug, vt, sig, gat, s0, s1, wt, wka, ycol, acs, abuf, cbuf,
                 oscr, uscr, usend, ubuf, zrow, bsend, bbuf, bscr, esend, ebuf, zsend, zfin, send, recv):
    net = Links(group, dap, send, recv)
    me, lo, hi = net.me, net.lo, net.hi
    opm = abuf.shape[2]
    seq, size = mask_ref.shape
    chunks = xbuf.shape[0]
    bq = s0.shape[1]
    per = bq // SLOT
    turns = group // per

    def side():
        flags = mask_ref[...].astype(bf16)
        pick = (lax.broadcasted_iota(jnp.int32, (size, size), 0) == me).astype(bf16)
        norm[...] = mm(flags, mm(flags, pick).astype(bf16), TN)
        row = (lax.broadcasted_iota(jnp.int32, (SLOT, size), 1) == me).astype(bf16)
        split = mask_ref[...].reshape(group, chunks, SLOT, size)
        for k in range(chunks):
            mrow[:, k * group * SLOT:(k + 1) * group * SLOT] = mm(
                row, split[:, k].astype(f32).reshape(group * SLOT, size).astype(bf16), NT)

    def ship(k, y):
        msend[k] = y.astype(f32).reshape(group, SLOT, -1).astype(bf16)
        xbuf[k, me] = msend[k, me]
        net.to_all(lambda t: (msend.at[k, t], xbuf.at[k, me]), 8 + k)

    row_stage(net, m_ref, z_ref, mask_ref, wr_bias, wr_in, wr_out, ship, side,
              kk, qt, rvt, rsig, rgat, bias, rwt, qd0, qd1, rsend, rbuf, rscr, ytr)

    def arrive(b):
        @pl.when(lax.rem(b, turns) == 0)
        def _():
            k = lax.div(b, turns)
            net.settle(xbuf.at[k, pl.ds(0, group - 1)], 8 + k)

    def load(b):
        part = xbuf[b // turns, pl.ds(pl.multiple_of(b % turns * per, per), per)]
        return part.astype(f32).reshape(bq, -1)

    half = pl.ds(pl.multiple_of(lax.div(hi, net.outer_n // 2) * (net.outer_n // 2), net.outer_n // 2), net.outer_n // 2)

    def pass_on(qb):
        net.settle(cbuf.at[qb, pl.ds(0, net.outer_n // 2 - 1)], 10 + qb)
        net.to_partner(cbuf.at[qb, half], 1)

    def emit(qb, y, ac):
        ycol[qb] = y.astype(f32).reshape(per, SLOT, -1).astype(bf16)
        acs[qb] = ac
        abuf[qb, lo] = ac[:opm]
        cbuf[qb, hi] = ac[opm:]
        net.to_half(acs.at[qb, pl.ds(opm, opm)], cbuf.at[qb, hi], 10 + qb)
        net.to_inner(lambda x: (acs.at[qb, pl.ds(0, opm)], abuf.at[qb, lo]), 0)

        @pl.when(qb > 0)
        def _():
            pass_on(qb - 1)

        def share_m(o):
            i = lax.rem(me + o, per)
            t = lax.rem(qb, turns) * per + i

            @pl.when(t != me)
            def _():
                net.copy(ycol.at[qb, i], mout.at[lax.div(qb, turns), me], 2, t).start()

        each(0, per, share_m)

    col_stage(arrive, load, seq, mrow, wc_in, wc_out, wopm_in, emit, kaug, qaug, vt, sig, gat, s0, s1, wt, wka)
    for k in range(chunks):
        mout[k, me] = ycol[k * turns + lax.div(me, per), lax.rem(me, per)]
    pass_on(cbuf.shape[0] - 1)
    net.settle(cbuf.at[:, pl.ds(0, net.outer_n // 2)], 1)
    net.settle(abuf.at[:, pl.ds(0, INNER - 1)], 0)
    pair_stage(net, z_ref, norm, res_ref, wopm_out, ws_in, ws_bias, ws_out, we_in, we_bias, we_out, zout,
               abuf, cbuf, oscr, uscr, usend, ubuf, zrow, bsend, bbuf, bscr, esend, ebuf, zsend, zfin)
    net.settle(mout.at[:, pl.ds(0, group - 1)], 2)


def row_scratch(tokens, size, width, heads, fold, group):
    seqs = tokens // size
    return [
        pltpu.VMEM((tokens, fold), bf16),
        pltpu.VMEM((fold, tokens), bf16),
        pltpu.VMEM((fold, tokens), bf16),
        pltpu.VMEM((fold, tokens), f32),
        pltpu.VMEM((fold, tokens), bf16),
        pltpu.VMEM((size, heads * size), f32),
        pltpu.VMEM((4 * fold, width), bf16),
        pltpu.VMEM((fold, heads * size), bf16),
        pltpu.VMEM((fold, heads * size), bf16),
        pltpu.VMEM((SLOT, size), bf16),
        pltpu.VMEM((group, SLOT, size), bf16),
        pltpu.VMEM((group * SLOT, size), f32),
        pltpu.VMEM((width // 128, SLOT * size, 128), f32),
        pltpu.VMEM((seqs // SLOT, group, SLOT, width), bf16),
        pltpu.VMEM((seqs // SLOT, group, SLOT, width), bf16),
        pltpu.VMEM((SLOT, seqs * group), f32),
        pltpu.VMEM((size, size), f32),
    ]


def col_scratch(seq, width, heads, hd, bq):
    return [
        pltpu.VMEM((heads, seq, 128), bf16),
        pltpu.VMEM((heads, 128, seq), bf16),
        pltpu.VMEM((heads, hd, seq), bf16),
        pltpu.VMEM((heads, hd, seq), f32),
        pltpu.VMEM((heads * hd, bq), bf16),
        pltpu.VMEM((seq, bq), f32),
        pltpu.VMEM((seq, bq), f32),
        pltpu.VMEM((4 * heads * hd, width), bf16),
        pltpu.VMEM((width, heads * 128), bf16),
        pltpu.VMEM((seq // bq, bq // SLOT, SLOT, width), bf16),
    ]


def pair_scratch(seq, size, width, opm, group, bq):
    outer_n = group // INNER
    return [
        pltpu.VMEM((seq // bq, 2 * opm, bq), bf16),
        pltpu.VMEM((seq // bq, INNER, opm, bq), bf16),
        pltpu.VMEM((seq // bq, outer_n, opm, bq), bf16),
        pltpu.VMEM((outer_n * opm // 128, INNER * opm, 128), f32),
        pltpu.VMEM((size, width), f32),
        pltpu.VMEM((INNER, outer_n, width), f32),
        pltpu.VMEM((INNER, outer_n, width), f32),
        pltpu.VMEM((size, width), f32),
        pltpu.VMEM((SLOT, size), bf16),
        pltpu.VMEM((group, SLOT, size), bf16),
        pltpu.VMEM((group * SLOT, size), f32),
        pltpu.VMEM((group, SLOT, size), bf16),
        pltpu.VMEM((group, SLOT, size), bf16),
        pltpu.VMEM((size, width), f32),
        pltpu.VMEM((size, width), f32),
    ]


def block_update(m, z, msa_mask, res_mask, weights, heads, group, dap, bq=512):
    vm = pl.BlockSpec(memory_space=pltpu.VMEM)
    tokens, m_width = m.shape
    size, width = z.shape
    seqs = tokens // size
    seq = seqs * group
    fold = weights[2].shape[0]
    opm = weights[5].shape[0] // 2
    return pl.pallas_call(
        functools.partial(block_kernel, group, dap),
        out_shape=(jax.ShapeDtypeStruct((seqs // SLOT, group, SLOT, m_width), bf16), jax.ShapeDtypeStruct((size, width), bf16)),
        in_specs=[vm] * (4 + len(weights)),
        out_specs=(vm, vm),
        scratch_shapes=row_scratch(tokens, size, m_width, heads, fold, group)
        + col_scratch(seq, m_width, heads, fold // heads, bq)
        + pair_scratch(seq, size, width, opm, group, bq)
        + [pltpu.SemaphoreType.DMA((14,)), pltpu.SemaphoreType.DMA((14,))],
        compiler_params=pltpu.CompilerParams(collective_id=1, has_side_effects=True, vmem_limit_bytes=63 << 20),
        name='block_update',
    )(m, z, msa_mask, res_mask, *weights)


def solution(mesh):
    dap_size = mesh.shape['dap']
    group_size = mesh.shape['chip'] * dap_size
    rows = P(('data', 'chip', 'dap'))
    in_specs = (rows, rows, P('data'), P('data')) + (P(),) * 13

    def per_device(m_blk, z_blk, msa_mask, res_mask, w_row_in, w_row_bias, w_row_out, w_col_in, w_col_out,
                   w_opm_in, w_opm_out, w_start_in, w_start_bias, w_start_out, w_end_in, w_end_bias, w_end_out):
        seqs, res, width = m_blk.shape
        weights = (w_row_in, w_row_bias.T, w_row_out, w_col_in, w_col_out, w_opm_in.T, w_opm_out,
                   w_start_in, w_start_bias.T, w_start_out, w_end_in, w_end_bias.T, w_end_out)
        slots, z_out = block_update(m_blk.reshape(seqs * res, width), z_blk[0], msa_mask, res_mask[None, :], weights,
                                    w_row_bias.shape[1], group_size, dap_size)
        m_out = jnp.swapaxes(slots, 1, 2).reshape(seqs, res, width)
        return m_out, z_out[None]

    return jax.shard_map(per_device, mesh=mesh, in_specs=in_specs, out_specs=(rows, rows), check_vma=False)
```

```python
import functools

import jax
import jax.numpy as jnp
import numpy as np
from jax import lax
from jax.experimental import pallas as pl
from jax.experimental.pallas import tpu as pltpu
from jax.sharding import PartitionSpec as P

LOG2E = 1.4426950408889634
f32, bf16 = jnp.float32, jnp.bfloat16


def split3(value):
    parts = []
    rest = np.float64(value)
    for _ in range(3):
        part = np.float64(np.asarray(rest, dtype=jnp.bfloat16))
        parts.append(float(part))
        rest = rest - part
    return parts


def norm_rows(x):
    values = x.astype(f32)
    centred = values - jnp.mean(values, axis=-1, keepdims=True)
    variance = jnp.mean(centred * centred, axis=-1, keepdims=True)
    return (centred * lax.rsqrt(variance + 1e-5)).astype(bf16)


def dot_t(w, x):
    return lax.dot_general(w, x, (((0,), (1,)), ((), ())), preferred_element_type=f32)


NT = (((1,), (1,)), ((), ()))
TN = (((0,), (0,)), ((), ()))
NEG = -1e9 * LOG2E


def mm(a, b, dims=(((1,), (0,)), ((), ()))):
    return lax.dot_general(a, b, dims, preferred_element_type=f32)


NN = (((1,), (0,)), ((), ()))
MESH = pl.DeviceIdType.MESH
INNER = 8
SLOT = 8


def place(t, dap):
    return (0, lax.div(t, dap), lax.rem(t, dap))


def pair_project(x, win_ref, fold):
    xn = norm_rows(x)
    k = mm(xn, win_ref[:, fold:2 * fold]).astype(bf16)
    qt = dot_t(win_ref[:, :fold], xn).astype(bf16)
    vt = dot_t(win_ref[:, 2 * fold:3 * fold], xn).astype(bf16)
    gg = dot_t(win_ref[:, 3 * fold:], xn).astype(bf16).astype(f32)
    return k, qt, vt, 1.0 / (1.0 + jnp.exp(-gg))


def pair_attend(x, parts, biases, keep, wout_ref):
    k, qt, vt, sig = parts
    heads = len(biases)
    hd = vt.shape[0] // heads
    c = hd ** -0.5 * LOG2E
    gated = []
    for h in range(heads):
        part = slice(h * hd, (h + 1) * hd)
        t = mm(k[:, part], qt[part]) * c + biases[h] * LOG2E
        t = jnp.where(keep, t, NEG)
        e = jnp.exp2(t - jnp.max(t, axis=0, keepdims=True))
        mixed = mm(vt[part], e.astype(bf16)) / jnp.sum(e, axis=0, keepdims=True)
        gated.append((mixed * sig[part]).astype(bf16))
    up = mm(jnp.concatenate(gated, axis=0), wout_ref[...], TN)
    return (x.astype(f32) + up).astype(bf16)


def col_stage(arrive, load, seq, mrow_ref, win_ref, wout_ref, wopm_ref, emit,
              kaug, qaug, vt, sig, gat, s0, s1, wt, wka):
    heads, hd = vt.shape[0], vt.shape[1]
    fold = heads * hd
    bq = s0.shape[1]
    nq = seq // bq
    kc = 256
    nk = seq // kc
    c = hd ** -0.5 * LOG2E
    masked = split3(-1e9 * LOG2E)

    lane = lax.broadcasted_iota(jnp.int32, (bq, 128), 1)
    row = lax.broadcasted_iota(jnp.int32, (128 - 3 * hd, bq), 0)
    fill = jnp.where(row == 0, masked[0], jnp.where(row == 1, masked[1], jnp.where(row == 2, masked[2], 0.0))).astype(bf16)
    flag = ((lane >= 3 * hd) & (lane < 3 * hd + 3)).astype(f32)
    flag2 = jnp.concatenate([flag, flag], axis=1)

    wt[...] = jnp.transpose(win_ref[...])
    for h in range(heads):
        wk = win_ref[:, fold + h * hd:fold + (h + 1) * hd]
        wka[:, h * 128:(h + 1) * 128] = jnp.concatenate([wk, wk, wk, jnp.zeros_like(wk)], axis=1)

    def project(b, carry):
        rows = pl.ds(pl.multiple_of(b * bq, bq), bq)
        arrive(b)
        xn = norm_rows(load(b))
        keep = jnp.transpose(jnp.broadcast_to(mrow_ref[0:1, rows], (128, bq))) != 0
        keep2 = jnp.concatenate([keep, keep], axis=1)
        for h in range(0, heads, 2):
            k = mm(xn, wka[:, h * 128:(h + 2) * 128])
            k = jnp.where(keep2, k, flag2).astype(bf16)
            kaug[h, rows, :] = k[:, :128]
            kaug[h + 1, rows, :] = k[:, 128:]
        qt = mm(wt[:fold, :], xn, NT).astype(bf16).astype(f32) * c
        hi = qt.astype(bf16)
        rest = qt - hi.astype(f32)
        mid = rest.astype(bf16)
        low = (rest - mid.astype(f32)).astype(bf16)
        vv = mm(wt[2 * fold:3 * fold, :], xn, NT).astype(bf16)
        gg = mm(wt[3 * fold:, :], xn, NT).astype(bf16).astype(f32)
        gg = 1.0 / (1.0 + jnp.exp(-gg))
        for h in range(heads):
            part = slice(h * hd, (h + 1) * hd)
            qaug[h, 0:hd, rows] = hi[part]
            qaug[h, hd:2 * hd, rows] = mid[part]
            qaug[h, 2 * hd:3 * hd, rows] = low[part]
            qaug[h, 3 * hd:, rows] = fill
            vt[h, :, rows] = vv[part]
            sig[h, :, rows] = gg[part]
        return carry

    lax.fori_loop(0, nq, project, 0)

    def fold8(s):
        return s.reshape(kc // 8, 8, bq)

    def chunk_scores(h, q, i, buf, m):
        s = mm(kaug[h, i * kc:(i + 1) * kc, :], q)
        buf[i * kc:(i + 1) * kc, :] = s
        top = jnp.max(fold8(s), axis=0)
        return top if m is None else jnp.maximum(m, top)

    def step(qb, h, cur, nxt, m):
        t = jnp.minimum(qb * heads + h + 1, nq * heads - 1)
        hn = t % heads
        q = qaug[hn, :, pl.ds(pl.multiple_of(t // heads * bq, bq), bq)]
        top = jnp.max(m, axis=0, keepdims=True)
        mn = None
        total = jnp.zeros((8, bq), f32)
        mixed = jnp.zeros((hd, bq), f32)
        held = None
        for i in range(nk):
            mn = chunk_scores(hn, q, i, nxt, mn)
            if held is not None:
                mixed = mixed + mm(vt[h, :, (i - 1) * kc:i * kc], held)
            e = jnp.exp2(cur[i * kc:(i + 1) * kc, :] - top)
            total = total + jnp.sum(fold8(e), axis=0)
            held = e.astype(bf16)
        mixed = mixed + mm(vt[h, :, (nk - 1) * kc:], held)
        cols = pl.ds(pl.multiple_of(qb * bq, bq), bq)
        mixed = mixed / jnp.sum(total, axis=0, keepdims=True)
        gat[pl.ds(pl.multiple_of(h * hd, hd), hd), :] = (mixed * sig[h, :, cols]).astype(bf16)
        return mn

    m = None
    for i in range(nk):
        m = chunk_scores(0, qaug[0, :, 0:bq], i, s0, m)

    def block(qb, m):
        def pair(u, m):
            m = step(qb, 2 * u, s0, s1, m)
            return step(qb, 2 * u + 1, s1, s0, m)

        m = lax.fori_loop(0, heads // 2, pair, m)
        rows = pl.ds(pl.multiple_of(qb * bq, bq), bq)
        y = (load(qb).astype(f32) + mm(gat[...], wout_ref[...], TN)).astype(bf16)
        ac = mm(wopm_ref[...], norm_rows(y), NT).astype(bf16)
        emit(qb, y, (ac.astype(f32) * mrow_ref[0:1, rows]).astype(bf16))
        return m

    lax.fori_loop(0, nq, block, m)


def each(start, stop, one, step=8):
    whole = (stop - start) // step

    def some(i, carry):
        for j in range(step):
            one(start + i * step + j)
        return carry

    lax.fori_loop(0, whole, some, 0)
    for o in range(start + whole * step, stop):
        one(o)


class Links:
    def __init__(self, group, dap, send, recv):
        self.group, self.dap, self.send, self.recv = group, dap, send, recv
        self.me = lax.axis_index('chip') * dap + lax.axis_index('dap')
        self.hi, self.lo = lax.div(self.me, INNER), lax.rem(self.me, INNER)
        self.outer_n = group // INNER

    def greet(self):
        barrier = pltpu.get_barrier_semaphore()

        def one(o):
            t = lax.rem(self.me + o, self.group)
            pl.semaphore_signal(barrier, inc=1, device_id=place(t, self.dap), device_id_type=MESH)

        each(1, self.group, one)

    def ready(self):
        pl.semaphore_wait(pltpu.get_barrier_semaphore(), self.group - 1)

    def copy(self, src, dst, i, t):
        return pltpu.make_async_remote_copy(src_ref=src, dst_ref=dst, send_sem=self.send.at[i], recv_sem=self.recv.at[i],
                                            device_id=place(t, self.dap), device_id_type=MESH)

    def settle(self, part, i):
        done = self.copy(part, part, i, self.me)
        done.wait_send()
        done.wait_recv()

    def to_all(self, make, i):
        def one(o):
            t = lax.rem(self.me + o, self.group)
            src, dst = make(t)
            self.copy(src, dst, i, t).start()

        each(1, self.group, one)

    def to_inner(self, make, i):
        for o in range(1, INNER):
            x = lax.rem(self.lo + o, INNER)
            src, dst = make(x)
            self.copy(src, dst, i, self.hi * INNER + x).start()

    def to_half(self, src, dst, i):
        half = self.outer_n // 2
        base = lax.div(self.hi, half) * half
        for o in range(1, half):
            y = base + lax.rem(lax.rem(self.hi, half) + o, half)
            self.copy(src, dst, i, y * INNER + self.lo).start()

    def to_partner(self, part, i):
        self.copy(part, part, i, lax.rem(self.me + self.group // 2, self.group)).start()


def bias_rows(z, weight):
    rows = mm(weight[...], norm_rows(z), NT).astype(bf16)
    spare = SLOT - rows.shape[0]
    return jnp.concatenate([rows, jnp.zeros((spare, rows.shape[1]), bf16)], axis=0) if spare else rows


def pair_stage(net, z_ref, norm, mask_ref, wopm_ref, ws_in, ws_bias, ws_out, we_in, we_bias, we_out, zout,
               abuf, cbuf, oscr, uscr, usend, ubuf, zrow, bsend, bbuf, bscr, esend, ebuf, zsend, zfin):
    me, lo, group, outer_n = net.me, net.lo, net.group, net.outer_n
    blocks, opm = abuf.shape[0], abuf.shape[2]
    heads = ws_bias.shape[0]
    fold = ws_out.shape[0]
    size = z_ref.shape[0]
    keep = jnp.transpose(jnp.broadcast_to(mask_ref[...].astype(f32), (size, size))) != 0

    per = 128 // opm
    outer = None
    for q in range(blocks):
        term = mm(abuf[q].reshape(INNER * opm, -1), cbuf[q].reshape(outer_n * opm, -1), NT)
        outer = term if outer is None else outer + term
    for g in range(outer_n // per):
        oscr[g] = outer[:, g * 128:(g + 1) * 128]
    lane = lax.broadcasted_iota(jnp.int32, (opm // per * INNER, 128), 1) // opm
    tiles = []
    for g in range(outer_n // per):
        slabs = [jnp.concatenate([oscr[g, pl.ds(b * per + r, INNER, stride=opm), :] for b in range(opm // per)], axis=0)
                 for r in range(per)]
        turned = [[slabs[r] if s == 0 else pltpu.roll(slabs[r], s * opm, 1) for s in range(per)] for r in range(per)]
        for q in range(per):
            pick = turned[0][(0 - q) % per]
            for r in range(1, per):
                pick = jnp.where(lane == r, turned[r][(r - q) % per], pick)
            tiles.append(pick)
    up = None
    for b in range(opm // per):
        block = jnp.concatenate([t[b * INNER:(b + 1) * INNER] for t in tiles], axis=0).astype(bf16)
        term = mm(block, wopm_ref[b * 128:(b + 1) * 128, :])
        up = term if up is None else up + term
    uscr[...] = up
    for x in range(INNER):
        usend[x] = uscr[pl.ds(x, outer_n, stride=INNER), :]
    ubuf[lo] = usend[lo]
    net.to_inner(lambda x: (usend.at[x], ubuf.at[lo]), 3)
    net.settle(ubuf.at[pl.ds(0, INNER - 1)], 3)
    for x in range(INNER):
        zrow[pl.ds(x, outer_n, stride=INNER), :] = ubuf[x]
    z1 = (z_ref[...].astype(f32) + zrow[...] / (1e-3 + norm[...])).astype(bf16)

    bsend[...] = bias_rows(z1, ws_bias)
    bbuf[me] = bsend[...]
    net.to_all(lambda t: (bsend, bbuf.at[me]), 4)
    parts = pair_project(z1, ws_in, fold)
    net.settle(bbuf.at[pl.ds(0, group - 1)], 4)
    bscr[...] = bbuf[...].astype(f32).reshape(group * SLOT, size)
    biases = [jnp.transpose(bscr[pl.ds(h, size, stride=SLOT), :]) for h in range(heads)]
    z2 = pair_attend(z1, parts, biases, keep, ws_out)

    end_rows = bias_rows(z2, we_bias).astype(f32)
    for h in range(heads):
        bscr[pl.ds(h, size, stride=SLOT), :] = jnp.broadcast_to(end_rows[h:h + 1], (size, size))
    bscr[pl.ds(heads, size, stride=SLOT), :] = z2.astype(f32)
    esend[...] = bscr[...].astype(bf16).reshape(group, SLOT, size)
    ebuf[me] = esend[me]
    net.to_all(lambda t: (esend.at[t], ebuf.at[me]), 5)
    net.settle(ebuf.at[pl.ds(0, group - 1)], 5)
    bscr[...] = ebuf[...].astype(f32).reshape(group * SLOT, size)
    zc = bscr[pl.ds(heads, size, stride=SLOT), :].astype(bf16)
    biases = [bscr[pl.ds(h, size, stride=SLOT), :] for h in range(heads)]
    z3 = pair_attend(zc, pair_project(zc, we_in, fold), biases, keep, we_out)

    zsend[...] = z3.astype(f32)
    zfin[pl.ds(me, 1), :] = zsend[pl.ds(me, 1), :]
    net.to_all(lambda t: (zsend.at[pl.ds(t, 1)], zfin.at[pl.ds(me, 1)]), 6)
    net.settle(zfin.at[pl.ds(0, group - 1)], 6)
    zout[...] = zfin[...].astype(bf16)


def row_stage(net, x_ref, z_ref, mask_ref, wb_ref, win_ref, wout_ref, ship, side, stash,
              kk, qt, vt, sig, gat, bias, wt, qd0, qd1, bsend, bbuf, bscr, ytr):
    tokens, width = x_ref.shape
    size = bias.shape[0]
    seqs = tokens // size
    heads = bias.shape[1] // size
    fold = gat.shape[0]
    hd = fold // heads
    c = hd ** -0.5 * LOG2E
    bp = 512
    me, group = net.me, net.group

    net.greet()
    bsend[...] = bias_rows(z_ref[...], wb_ref)
    bbuf[me] = bsend[...]
    wt[...] = jnp.transpose(win_ref[...])
    qd0[...] = jnp.zeros_like(qd0)
    qd1[...] = jnp.zeros_like(qd1)

    def project(b, carry):
        rows = pl.ds(pl.multiple_of(b * bp, bp), bp)
        xn = norm_rows(x_ref[rows, :])
        kk[rows, :] = mm(xn, win_ref[:, fold:2 * fold]).astype(bf16)
        qt[:, rows] = mm(wt[:fold, :], xn, NT).astype(bf16)
        vt[:, rows] = mm(wt[2 * fold:3 * fold, :], xn, NT).astype(bf16)
        gg = mm(wt[3 * fold:, :], xn, NT).astype(bf16).astype(f32)
        sig[:, rows] = 1.0 / (1.0 + jnp.exp(-gg))

        @pl.when(b == 0)
        def _():
            net.ready()
            net.to_all(lambda t: (bsend, bbuf.at[me]), 7)

        return carry

    lax.fori_loop(0, tokens // bp, project, 0)
    slab = heads // 2

    def prescore(s, u, buf, qd):
        cols = pl.ds(pl.multiple_of(s * size, size), size)
        for h in range(heads):
            qd[h * hd:(h + 1) * hd, h * size:(h + 1) * size] = qt[h * hd:(h + 1) * hd, cols]
        for g in range(2):
            out = pl.ds(pl.multiple_of((2 * u + g) * size, size), size)
            buf[out, :] = mm(kk[cols, :], qd[:, g * slab * size:(g + 1) * slab * size]) * c

    for k, buf in enumerate(stash):
        def ahead(u, carry):
            prescore(k * SLOT + 2 * u, 2 * u, buf, qd0)
            prescore(k * SLOT + 2 * u + 1, 2 * u + 1, buf, qd1)
            return carry

        lax.fori_loop(0, SLOT // 2, ahead, 0)
    side()
    net.settle(bbuf.at[pl.ds(0, group - 1)], 7)
    bscr[...] = bbuf[...].astype(f32).reshape(group * SLOT, size)
    for h in range(heads):
        bias[:, h * size:(h + 1) * size] = jnp.transpose(bscr[pl.ds(h, size, stride=SLOT), :] * LOG2E)

    def one(s, u, buf):
        cols = pl.ds(pl.multiple_of(s * size, size), size)
        mrow = mask_ref[pl.ds(me * seqs + s, 1), :]
        keep = jnp.transpose(jnp.broadcast_to(mrow.astype(f32), (size, size))) != 0
        keep2 = jnp.concatenate([keep, keep], axis=1)
        for h in range(0, heads, 2):
            two = slice(h * size, (h + 2) * size)
            rows = pl.ds(pl.multiple_of((2 * u + h // slab) * size, size), size)
            t = buf[rows, h % slab * size:(h % slab + 2) * size] + bias[:, two]
            t = jnp.where(keep2, t, NEG)
            e = jnp.exp2(t - jnp.max(t, axis=0, keepdims=True))
            total = jnp.sum(e, axis=0, keepdims=True)
            mixed = mm(vt[h * hd:(h + 2) * hd, cols], e.astype(bf16)) / total
            gat[h * hd:(h + 1) * hd, cols] = (mixed[:hd, :size] * sig[h * hd:(h + 1) * hd, cols]).astype(bf16)
            gat[(h + 1) * hd:(h + 2) * hd, cols] = (mixed[hd:, size:] * sig[(h + 1) * hd:(h + 2) * hd, cols]).astype(bf16)

    for k, buf in enumerate(stash):
        def several(u, carry):
            for j in range(4):
                one(k * SLOT + 4 * u + j, 4 * u + j, buf)
            return carry

        lax.fori_loop(0, SLOT // 4, several, 0)
        for b in range(SLOT * size // bp):
            rows = slice((k * SLOT * size // bp + b) * bp, (k * SLOT * size // bp + b + 1) * bp)
            y = (x_ref[rows, :].astype(f32) + mm(gat[:, rows], wout_ref[...], TN)).astype(bf16).astype(f32)
            for i in range(bp // size):
                for half in range(width // 128):
                    ytr[half, pl.ds(b * (bp // size) + i, size, stride=SLOT), :] = (
                        y[i * size:(i + 1) * size, half * 128:(half + 1) * 128])
        ship(k, jnp.concatenate([ytr[half] for half in range(width // 128)], axis=1).astype(bf16))


def block_kernel(group, dap, m_ref, z_ref, mask_ref, res_ref, wr_in, wr_bias, wr_out, wc_in, wc_out, wopm_in, wopm_out,
                 ws_in, ws_bias, ws_out, we_in, we_bias, we_out, mout, zout,
                 kk, qt, rvt, rsig, rgat, bias, rwt, qd0, qd1, rsend, rbuf, rscr, ytr, msend, xbuf, mrow, norm,
                 kaug, qaug, vt, sig, gat, s0, s1, wt, wka, ycol, acs, abuf, cbuf,
                 oscr, uscr, usend, ubuf, zrow, bsend, bbuf, bscr, esend, ebuf, zsend, zfin, send, recv):
    net = Links(group, dap, send, recv)
    me, lo, hi = net.me, net.lo, net.hi
    opm = abuf.shape[2]
    seq, size = mask_ref.shape
    chunks = xbuf.shape[0]
    bq = s0.shape[1]
    per = bq // SLOT
    turns = group // per

    def side():
        flags = mask_ref[...].astype(bf16)
        pick = (lax.broadcasted_iota(jnp.int32, (size, size), 0) == me).astype(bf16)
        norm[...] = mm(flags, mm(flags, pick).astype(bf16), TN)
        row = (lax.broadcasted_iota(jnp.int32, (SLOT, size), 1) == me).astype(bf16)
        split = mask_ref[...].reshape(group, chunks, SLOT, size)
        for k in range(chunks):
            mrow[:, k * group * SLOT:(k + 1) * group * SLOT] = mm(
                row, split[:, k].astype(f32).reshape(group * SLOT, size).astype(bf16), NT)

    def ship(k, y):
        msend[k] = y.astype(f32).reshape(group, SLOT, -1).astype(bf16)
        xbuf[k, me] = msend[k, me]
        net.to_all(lambda t: (msend.at[k, t], xbuf.at[k, me]), 8 + k)

    row_stage(net, m_ref, z_ref, mask_ref, wr_bias, wr_in, wr_out, ship, side, (s0, s1),
              kk, qt, rvt, rsig, rgat, bias, rwt, qd0, qd1, rsend, rbuf, rscr, ytr)

    def arrive(b):
        @pl.when(lax.rem(b, turns) == 0)
        def _():
            k = lax.div(b, turns)
            net.settle(xbuf.at[k, pl.ds(0, group - 1)], 8 + k)

    def load(b):
        part = xbuf[b // turns, pl.ds(pl.multiple_of(b % turns * per, per), per)]
        return part.astype(f32).reshape(bq, -1)

    half = pl.ds(pl.multiple_of(lax.div(hi, net.outer_n // 2) * (net.outer_n // 2), net.outer_n // 2), net.outer_n // 2)

    def pass_on(qb):
        net.settle(cbuf.at[qb, pl.ds(0, net.outer_n // 2 - 1)], 10 + qb)
        net.to_partner(cbuf.at[qb, half], 1)

    def emit(qb, y, ac):
        ycol[qb] = y.astype(f32).reshape(per, SLOT, -1).astype(bf16)
        acs[qb] = ac
        abuf[qb, lo] = ac[:opm]
        cbuf[qb, hi] = ac[opm:]
        net.to_half(acs.at[qb, pl.ds(opm, opm)], cbuf.at[qb, hi], 10 + qb)
        net.to_inner(lambda x: (acs.at[qb, pl.ds(0, opm)], abuf.at[qb, lo]), 0)

        @pl.when(qb > 0)
        def _():
            pass_on(qb - 1)

        def share_m(o):
            i = lax.rem(me + o, per)
            t = lax.rem(qb, turns) * per + i

            @pl.when(t != me)
            def _():
                net.copy(ycol.at[qb, i], mout.at[lax.div(qb, turns), me], 2, t).start()

        each(0, per, share_m)

    col_stage(arrive, load, seq, mrow, wc_in, wc_out, wopm_in, emit, kaug, qaug, vt, sig, gat, s0, s1, wt, wka)
    for k in range(chunks):
        mout[k, me] = ycol[k * turns + lax.div(me, per), lax.rem(me, per)]
    pass_on(cbuf.shape[0] - 1)
    net.settle(cbuf.at[:, pl.ds(0, net.outer_n // 2)], 1)
    net.settle(abuf.at[:, pl.ds(0, INNER - 1)], 0)
    pair_stage(net, z_ref, norm, res_ref, wopm_out, ws_in, ws_bias, ws_out, we_in, we_bias, we_out, zout,
               abuf, cbuf, oscr, uscr, usend, ubuf, zrow, bsend, bbuf, bscr, esend, ebuf, zsend, zfin)
    net.settle(mout.at[:, pl.ds(0, group - 1)], 2)


def row_scratch(tokens, size, width, heads, fold, group):
    seqs = tokens // size
    return [
        pltpu.VMEM((tokens, fold), bf16),
        pltpu.VMEM((fold, tokens), bf16),
        pltpu.VMEM((fold, tokens), bf16),
        pltpu.VMEM((fold, tokens), f32),
        pltpu.VMEM((fold, tokens), bf16),
        pltpu.VMEM((size, heads * size), f32),
        pltpu.VMEM((4 * fold, width), bf16),
        pltpu.VMEM((fold, heads * size), bf16),
        pltpu.VMEM((fold, heads * size), bf16),
        pltpu.VMEM((SLOT, size), bf16),
        pltpu.VMEM((group, SLOT, size), bf16),
        pltpu.VMEM((group * SLOT, size), f32),
        pltpu.VMEM((width // 128, SLOT * size, 128), f32),
        pltpu.VMEM((seqs // SLOT, group, SLOT, width), bf16),
        pltpu.VMEM((seqs // SLOT, group, SLOT, width), bf16),
        pltpu.VMEM((SLOT, seqs * group), f32),
        pltpu.VMEM((size, size), f32),
    ]


def col_scratch(seq, width, heads, hd, bq):
    return [
        pltpu.VMEM((heads, seq, 128), bf16),
        pltpu.VMEM((heads, 128, seq), bf16),
        pltpu.VMEM((heads, hd, seq), bf16),
        pltpu.VMEM((heads, hd, seq), f32),
        pltpu.VMEM((heads * hd, bq), bf16),
        pltpu.VMEM((seq, bq), f32),
        pltpu.VMEM((seq, bq), f32),
        pltpu.VMEM((4 * heads * hd, width), bf16),
        pltpu.VMEM((width, heads * 128), bf16),
        pltpu.VMEM((seq // bq, bq // SLOT, SLOT, width), bf16),
    ]


def pair_scratch(seq, size, width, opm, group, bq):
    outer_n = group // INNER
    return [
        pltpu.VMEM((seq // bq, 2 * opm, bq), bf16),
        pltpu.VMEM((seq // bq, INNER, opm, bq), bf16),
        pltpu.VMEM((seq // bq, outer_n, opm, bq), bf16),
        pltpu.VMEM((outer_n * opm // 128, INNER * opm, 128), f32),
        pltpu.VMEM((size, width), f32),
        pltpu.VMEM((INNER, outer_n, width), f32),
        pltpu.VMEM((INNER, outer_n, width), f32),
        pltpu.VMEM((size, width), f32),
        pltpu.VMEM((SLOT, size), bf16),
        pltpu.VMEM((group, SLOT, size), bf16),
        pltpu.VMEM((group * SLOT, size), f32),
        pltpu.VMEM((group, SLOT, size), bf16),
        pltpu.VMEM((group, SLOT, size), bf16),
        pltpu.VMEM((size, width), f32),
        pltpu.VMEM((size, width), f32),
    ]


def block_update(m, z, msa_mask, res_mask, weights, heads, group, dap, bq=512):
    vm = pl.BlockSpec(memory_space=pltpu.VMEM)
    tokens, m_width = m.shape
    size, width = z.shape
    seqs = tokens // size
    seq = seqs * group
    fold = weights[2].shape[0]
    opm = weights[5].shape[0] // 2
    return pl.pallas_call(
        functools.partial(block_kernel, group, dap),
        out_shape=(jax.ShapeDtypeStruct((seqs // SLOT, group, SLOT, m_width), bf16), jax.ShapeDtypeStruct((size, width), bf16)),
        in_specs=[vm] * (4 + len(weights)),
        out_specs=(vm, vm),
        scratch_shapes=row_scratch(tokens, size, m_width, heads, fold, group)
        + col_scratch(seq, m_width, heads, fold // heads, bq)
        + pair_scratch(seq, size, width, opm, group, bq)
        + [pltpu.SemaphoreType.DMA((14,)), pltpu.SemaphoreType.DMA((14,))],
        compiler_params=pltpu.CompilerParams(collective_id=1, has_side_effects=True, vmem_limit_bytes=63 << 20),
        name='block_update',
    )(m, z, msa_mask, res_mask, *weights)


def solution(mesh):
    dap_size = mesh.shape['dap']
    group_size = mesh.shape['chip'] * dap_size
    rows = P(('data', 'chip', 'dap'))
    in_specs = (rows, rows, P('data'), P('data')) + (P(),) * 13

    def per_device(m_blk, z_blk, msa_mask, res_mask, w_row_in, w_row_bias, w_row_out, w_col_in, w_col_out,
                   w_opm_in, w_opm_out, w_start_in, w_start_bias, w_start_out, w_end_in, w_end_bias, w_end_out):
        seqs, res, width = m_blk.shape
        weights = (w_row_in, w_row_bias.T, w_row_out, w_col_in, w_col_out, w_opm_in.T, w_opm_out,
                   w_start_in, w_start_bias.T, w_start_out, w_end_in, w_end_bias.T, w_end_out)
        slots, z_out = block_update(m_blk.reshape(seqs * res, width), z_blk[0], msa_mask, res_mask[None, :], weights,
                                    w_row_bias.shape[1], group_size, dap_size)
        m_out = jnp.swapaxes(slots, 1, 2).reshape(seqs, res, width)
        return m_out, z_out[None]

    return jax.shard_map(per_device, mesh=mesh, in_specs=in_specs, out_specs=(rows, rows), check_vma=False)
```

```python
import functools

import jax
import jax.numpy as jnp
import numpy as np
from jax import lax
from jax.experimental import pallas as pl
from jax.experimental.pallas import tpu as pltpu
from jax.sharding import PartitionSpec as P

LOG2E = 1.4426950408889634
f32, bf16 = jnp.float32, jnp.bfloat16


def split3(value):
    parts = []
    rest = np.float64(value)
    for _ in range(3):
        part = np.float64(np.asarray(rest, dtype=jnp.bfloat16))
        parts.append(float(part))
        rest = rest - part
    return parts


def norm_rows(x):
    values = x.astype(f32)
    centred = values - jnp.mean(values, axis=-1, keepdims=True)
    variance = jnp.mean(centred * centred, axis=-1, keepdims=True)
    return (centred * lax.rsqrt(variance + 1e-5)).astype(bf16)


def dot_t(w, x):
    return lax.dot_general(w, x, (((0,), (1,)), ((), ())), preferred_element_type=f32)


NT = (((1,), (1,)), ((), ()))
TN = (((0,), (0,)), ((), ()))
NEG = -1e9 * LOG2E


def mm(a, b, dims=(((1,), (0,)), ((), ()))):
    return lax.dot_general(a, b, dims, preferred_element_type=f32)


NN = (((1,), (0,)), ((), ()))
MESH = pl.DeviceIdType.MESH
INNER = 8
SLOT = 8


def place(t, dap):
    return (0, lax.div(t, dap), lax.rem(t, dap))


def pair_project(x, win_ref, fold):
    xn = norm_rows(x)
    k = mm(xn, win_ref[:, fold:2 * fold]).astype(bf16)
    qt = dot_t(win_ref[:, :fold], xn).astype(bf16)
    vt = dot_t(win_ref[:, 2 * fold:3 * fold], xn).astype(bf16)
    gg = dot_t(win_ref[:, 3 * fold:], xn).astype(bf16).astype(f32)
    return k, qt, vt, 1.0 / (1.0 + jnp.exp(-gg))


def pair_attend(x, parts, biases, keep, wout_ref):
    k, qt, vt, sig = parts
    heads = len(biases)
    hd = vt.shape[0] // heads
    c = hd ** -0.5 * LOG2E
    gated = []
    for h in range(heads):
        part = slice(h * hd, (h + 1) * hd)
        t = mm(k[:, part], qt[part]) * c + biases[h] * LOG2E
        t = jnp.where(keep, t, NEG)
        e = jnp.exp2(t - jnp.max(t, axis=0, keepdims=True))
        mixed = mm(vt[part], e.astype(bf16)) / jnp.sum(e, axis=0, keepdims=True)
        gated.append((mixed * sig[part]).astype(bf16))
    up = mm(jnp.concatenate(gated, axis=0), wout_ref[...], TN)
    return (x.astype(f32) + up).astype(bf16)


def col_stage(arrive, load, seq, mrow_ref, win_ref, wout_ref, wopm_ref, emit,
              kaug, qaug, vt, sig, gat, s0, s1, wt, wka):
    heads, hd = vt.shape[0], vt.shape[1]
    fold = heads * hd
    bq = s0.shape[1]
    nq = seq // bq
    kc = 256
    nk = seq // kc
    c = hd ** -0.5 * LOG2E
    masked = split3(-1e9 * LOG2E)

    lane = lax.broadcasted_iota(jnp.int32, (bq, 128), 1)
    row = lax.broadcasted_iota(jnp.int32, (128 - 3 * hd, bq), 0)
    fill = jnp.where(row == 0, masked[0], jnp.where(row == 1, masked[1], jnp.where(row == 2, masked[2], 0.0))).astype(bf16)
    flag = ((lane >= 3 * hd) & (lane < 3 * hd + 3)).astype(f32)
    flag2 = jnp.concatenate([flag, flag], axis=1)

    wt[...] = jnp.transpose(win_ref[...])
    for h in range(heads):
        wk = win_ref[:, fold + h * hd:fold + (h + 1) * hd]
        wka[:, h * 128:(h + 1) * 128] = jnp.concatenate([wk, wk, wk, jnp.zeros_like(wk)], axis=1)

    def project(b, carry):
        rows = pl.ds(pl.multiple_of(b * bq, bq), bq)
        arrive(b)
        xn = norm_rows(load(b))
        keep = jnp.transpose(jnp.broadcast_to(mrow_ref[0:1, rows], (128, bq))) != 0
        keep2 = jnp.concatenate([keep, keep], axis=1)
        for h in range(0, heads, 2):
            k = mm(xn, wka[:, h * 128:(h + 2) * 128])
            k = jnp.where(keep2, k, flag2).astype(bf16)
            kaug[h, rows, :] = k[:, :128]
            kaug[h + 1, rows, :] = k[:, 128:]
        qt = mm(wt[:fold, :], xn, NT).astype(bf16).astype(f32) * c
        hi = qt.astype(bf16)
        rest = qt - hi.astype(f32)
        mid = rest.astype(bf16)
        low = (rest - mid.astype(f32)).astype(bf16)
        vv = mm(wt[2 * fold:3 * fold, :], xn, NT).astype(bf16)
        gg = mm(wt[3 * fold:, :], xn, NT).astype(bf16).astype(f32)
        gg = 1.0 / (1.0 + jnp.exp(-gg))
        for h in range(heads):
            part = slice(h * hd, (h + 1) * hd)
            qaug[h, 0:hd, rows] = hi[part]
            qaug[h, hd:2 * hd, rows] = mid[part]
            qaug[h, 2 * hd:3 * hd, rows] = low[part]
            qaug[h, 3 * hd:, rows] = fill
            vt[h, :, rows] = vv[part]
            sig[h, :, rows] = gg[part]
        return carry

    lax.fori_loop(0, nq, project, 0)

    def fold8(s):
        return s.reshape(kc // 8, 8, bq)

    def chunk_scores(h, q, i, buf, m):
        s = mm(kaug[h, i * kc:(i + 1) * kc, :], q)
        buf[i * kc:(i + 1) * kc, :] = s
        top = jnp.max(fold8(s), axis=0)
        return top if m is None else jnp.maximum(m, top)

    def step(qb, h, cur, nxt, m):
        t = jnp.minimum(qb * heads + h + 1, nq * heads - 1)
        hn = t % heads
        q = qaug[hn, :, pl.ds(pl.multiple_of(t // heads * bq, bq), bq)]
        top = jnp.max(m, axis=0, keepdims=True)
        mn = None
        total = jnp.zeros((8, bq), f32)
        mixed = jnp.zeros((hd, bq), f32)
        held = None
        for i in range(nk):
            mn = chunk_scores(hn, q, i, nxt, mn)
            if held is not None:
                mixed = mixed + mm(vt[h, :, (i - 1) * kc:i * kc], held)
            e = jnp.exp2(cur[i * kc:(i + 1) * kc, :] - top)
            total = total + jnp.sum(fold8(e), axis=0)
            held = e.astype(bf16)
        mixed = mixed + mm(vt[h, :, (nk - 1) * kc:], held)
        cols = pl.ds(pl.multiple_of(qb * bq, bq), bq)
        mixed = mixed / jnp.sum(total, axis=0, keepdims=True)
        gat[pl.ds(pl.multiple_of(h * hd, hd), hd), :] = (mixed * sig[h, :, cols]).astype(bf16)
        return mn

    m = None
    for i in range(nk):
        m = chunk_scores(0, qaug[0, :, 0:bq], i, s0, m)

    def block(qb, m):
        def pair(u, m):
            m = step(qb, 2 * u, s0, s1, m)
            return step(qb, 2 * u + 1, s1, s0, m)

        m = lax.fori_loop(0, heads // 2, pair, m)
        rows = pl.ds(pl.multiple_of(qb * bq, bq), bq)
        y = (load(qb).astype(f32) + mm(gat[...], wout_ref[...], TN)).astype(bf16)
        ac = mm(wopm_ref[...], norm_rows(y), NT).astype(bf16)
        emit(qb, y, (ac.astype(f32) * mrow_ref[0:1, rows]).astype(bf16))
        return m

    lax.fori_loop(0, nq, block, m)


def each(start, stop, one, step=8):
    whole = (stop - start) // step

    def some(i, carry):
        for j in range(step):
            one(start + i * step + j)
        return carry

    lax.fori_loop(0, whole, some, 0)
    for o in range(start + whole * step, stop):
        one(o)


class Links:
    def __init__(self, group, dap, send, recv):
        self.group, self.dap, self.send, self.recv = group, dap, send, recv
        self.me = lax.axis_index('chip') * dap + lax.axis_index('dap')
        self.hi, self.lo = lax.div(self.me, INNER), lax.rem(self.me, INNER)
        self.outer_n = group // INNER

    def greet(self):
        barrier = pltpu.get_barrier_semaphore()

        def one(o):
            t = lax.rem(self.me + o, self.group)
            pl.semaphore_signal(barrier, inc=1, device_id=place(t, self.dap), device_id_type=MESH)

        each(1, self.group, one)

    def ready(self):
        pl.semaphore_wait(pltpu.get_barrier_semaphore(), self.group - 1)

    def copy(self, src, dst, i, t):
        return pltpu.make_async_remote_copy(src_ref=src, dst_ref=dst, send_sem=self.send.at[i], recv_sem=self.recv.at[i],
                                            device_id=place(t, self.dap), device_id_type=MESH)

    def settle(self, part, i):
        done = self.copy(part, part, i, self.me)
        done.wait_send()
        done.wait_recv()

    def to_all(self, make, i):
        def one(o):
            t = lax.rem(self.me + o, self.group)
            src, dst = make(t)
            self.copy(src, dst, i, t).start()

        each(1, self.group, one)

    def to_inner(self, make, i):
        for o in range(1, INNER):
            x = lax.rem(self.lo + o, INNER)
            src, dst = make(x)
            self.copy(src, dst, i, self.hi * INNER + x).start()

    def to_half(self, src, dst, i):
        half = self.outer_n // 2
        base = lax.div(self.hi, half) * half
        for o in range(1, half):
            y = base + lax.rem(lax.rem(self.hi, half) + o, half)
            self.copy(src, dst, i, y * INNER + self.lo).start()

    def to_partner(self, part, i):
        self.copy(part, part, i, lax.rem(self.me + self.group // 2, self.group)).start()


def bias_rows(z, weight):
    rows = mm(weight[...], norm_rows(z), NT).astype(bf16)
    spare = SLOT - rows.shape[0]
    return jnp.concatenate([rows, jnp.zeros((spare, rows.shape[1]), bf16)], axis=0) if spare else rows


def untile(block):
    size = block.shape[0]
    out = jnp.transpose(block)
    row = lax.broadcasted_iota(jnp.int32, (size, size), 0)
    lane = lax.broadcasted_iota(jnp.int32, (size, size), 1)
    step = INNER // 2
    while step:
        low, high = lax.rem(lax.div(row, step), 2), lax.rem(lax.div(lane, step), 2)
        down = pltpu.roll(pltpu.roll(out, size - step, 0), step, 1)
        back = pltpu.roll(pltpu.roll(out, step, 0), size - step, 1)
        out = jnp.where(low == high, out, jnp.where(low < high, down, back))
        step //= 2
    return out


def pair_stage(net, z_ref, norm, tnorm, ztbuf, mask_ref, wopm_ref, ws_in, ws_bias, ws_out, we_in, we_bias, we_out, zout,
               abuf, cbuf, oscr, uscr, usend, ubuf, zrow, bsend, bbuf, bscr, esend, ebuf, zsend, zfin):
    me, lo, group, outer_n = net.me, net.lo, net.group, net.outer_n
    blocks, opm = abuf.shape[0], abuf.shape[2]
    heads = ws_bias.shape[0]
    fold = ws_out.shape[0]
    size = z_ref.shape[0]
    keep = jnp.transpose(jnp.broadcast_to(mask_ref[...].astype(f32), (size, size))) != 0

    per = 128 // opm
    outer = None
    for q in range(blocks):
        term = mm(abuf[q].reshape(INNER * opm, -1), cbuf[q].reshape(outer_n * opm, -1), NT)
        outer = term if outer is None else outer + term
    for g in range(outer_n // per):
        oscr[g] = outer[:, g * 128:(g + 1) * 128]
    lane = lax.broadcasted_iota(jnp.int32, (opm // per * INNER, 128), 1) // opm
    tiles = []
    for g in range(outer_n // per):
        slabs = [jnp.concatenate([oscr[g, pl.ds(b * per + r, INNER, stride=opm), :] for b in range(opm // per)], axis=0)
                 for r in range(per)]
        turned = [[slabs[r] if s == 0 else pltpu.roll(slabs[r], s * opm, 1) for s in range(per)] for r in range(per)]
        for q in range(per):
            pick = turned[0][(0 - q) % per]
            for r in range(1, per):
                pick = jnp.where(lane == r, turned[r][(r - q) % per], pick)
            tiles.append(pick)
    up = None
    for b in range(opm // per):
        block = jnp.concatenate([t[b * INNER:(b + 1) * INNER] for t in tiles], axis=0).astype(bf16)
        term = mm(block, wopm_ref[b * 128:(b + 1) * 128, :])
        up = term if up is None else up + term
    uscr[...] = up
    for x in range(INNER):
        usend[x] = uscr[pl.ds(x, outer_n, stride=INNER), :]
    ubuf[lo] = usend[lo]
    net.to_inner(lambda x: (usend.at[x], ubuf.at[lo]), 3)
    net.settle(ztbuf.at[pl.ds(0, INNER - 1)], 14)
    for x in range(INNER):
        zrow[pl.ds(x, outer_n, stride=INNER), :] = ztbuf[x]
    tile = (zrow[...] + up / (1e-3 + tnorm[...])).astype(bf16)
    bsend[...] = bias_rows(tile, ws_bias)
    bbuf[me] = bsend[...]
    net.to_all(lambda t: (bsend, bbuf.at[me]), 4)
    net.settle(ubuf.at[pl.ds(0, INNER - 1)], 3)
    for x in range(INNER):
        zrow[pl.ds(x, outer_n, stride=INNER), :] = ubuf[x]
    z1 = (z_ref[...].astype(f32) + zrow[...] / (1e-3 + norm[...])).astype(bf16)

    parts = pair_project(z1, ws_in, fold)
    net.settle(bbuf.at[pl.ds(0, group - 1)], 4)
    bscr[...] = bbuf[...].astype(f32).reshape(group * SLOT, size)
    biases = [untile(bscr[pl.ds(h, size, stride=SLOT), :]) for h in range(heads)]
    z2 = pair_attend(z1, parts, biases, keep, ws_out)

    end_rows = bias_rows(z2, we_bias).astype(f32)
    for h in range(heads):
        bscr[pl.ds(h, size, stride=SLOT), :] = jnp.broadcast_to(end_rows[h:h + 1], (size, size))
    bscr[pl.ds(heads, size, stride=SLOT), :] = z2.astype(f32)
    esend[...] = bscr[...].astype(bf16).reshape(group, SLOT, size)
    ebuf[me] = esend[me]
    net.to_all(lambda t: (esend.at[t], ebuf.at[me]), 5)
    net.settle(ebuf.at[pl.ds(0, group - 1)], 5)
    bscr[...] = ebuf[...].astype(f32).reshape(group * SLOT, size)
    zc = bscr[pl.ds(heads, size, stride=SLOT), :].astype(bf16)
    biases = [bscr[pl.ds(h, size, stride=SLOT), :] for h in range(heads)]
    z3 = pair_attend(zc, pair_project(zc, we_in, fold), biases, keep, we_out)

    zsend[...] = z3.astype(f32)
    zfin[pl.ds(me, 1), :] = zsend[pl.ds(me, 1), :]
    net.to_all(lambda t: (zsend.at[pl.ds(t, 1)], zfin.at[pl.ds(me, 1)]), 6)
    net.settle(zfin.at[pl.ds(0, group - 1)], 6)
    zout[...] = zfin[...].astype(bf16)


def row_stage(net, x_ref, z_ref, mask_ref, wb_ref, win_ref, wout_ref, ship, side, stash,
              kk, qt, vt, sig, gat, bias, wt, qd0, qd1, bsend, bbuf, bscr, ytr):
    tokens, width = x_ref.shape
    size = bias.shape[0]
    seqs = tokens // size
    heads = bias.shape[1] // size
    fold = gat.shape[0]
    hd = fold // heads
    c = hd ** -0.5 * LOG2E
    bp = 512
    me, group = net.me, net.group

    net.greet()
    bsend[...] = bias_rows(z_ref[...], wb_ref)
    bbuf[me] = bsend[...]
    wt[...] = jnp.transpose(win_ref[...])
    qd0[...] = jnp.zeros_like(qd0)
    qd1[...] = jnp.zeros_like(qd1)

    def project(b, carry):
        rows = pl.ds(pl.multiple_of(b * bp, bp), bp)
        xn = norm_rows(x_ref[rows, :])
        kk[rows, :] = mm(xn, win_ref[:, fold:2 * fold]).astype(bf16)
        qt[:, rows] = mm(wt[:fold, :], xn, NT).astype(bf16)
        vt[:, rows] = mm(wt[2 * fold:3 * fold, :], xn, NT).astype(bf16)
        gg = mm(wt[3 * fold:, :], xn, NT).astype(bf16).astype(f32)
        sig[:, rows] = 1.0 / (1.0 + jnp.exp(-gg))

        @pl.when(b == 0)
        def _():
            net.ready()
            net.to_all(lambda t: (bsend, bbuf.at[me]), 7)

        return carry

    lax.fori_loop(0, tokens // bp, project, 0)
    slab = heads // 2

    def prescore(s, u, buf, qd):
        cols = pl.ds(pl.multiple_of(s * size, size), size)
        for h in range(heads):
            qd[h * hd:(h + 1) * hd, h * size:(h + 1) * size] = qt[h * hd:(h + 1) * hd, cols]
        for g in range(2):
            out = pl.ds(pl.multiple_of((2 * u + g) * size, size), size)
            buf[out, :] = mm(kk[cols, :], qd[:, g * slab * size:(g + 1) * slab * size]) * c

    for k, buf in enumerate(stash):
        def ahead(u, carry):
            prescore(k * SLOT + 2 * u, 2 * u, buf, qd0)
            prescore(k * SLOT + 2 * u + 1, 2 * u + 1, buf, qd1)
            return carry

        lax.fori_loop(0, SLOT // 2, ahead, 0)
    side()
    net.settle(bbuf.at[pl.ds(0, group - 1)], 7)
    bscr[...] = bbuf[...].astype(f32).reshape(group * SLOT, size)
    for h in range(heads):
        bias[:, h * size:(h + 1) * size] = jnp.transpose(bscr[pl.ds(h, size, stride=SLOT), :] * LOG2E)

    def one(s, u, buf):
        cols = pl.ds(pl.multiple_of(s * size, size), size)
        mrow = mask_ref[pl.ds(me * seqs + s, 1), :]
        keep = jnp.transpose(jnp.broadcast_to(mrow.astype(f32), (size, size))) != 0
        keep2 = jnp.concatenate([keep, keep], axis=1)
        for h in range(0, heads, 2):
            two = slice(h * size, (h + 2) * size)
            rows = pl.ds(pl.multiple_of((2 * u + h // slab) * size, size), size)
            t = buf[rows, h % slab * size:(h % slab + 2) * size] + bias[:, two]
            t = jnp.where(keep2, t, NEG)
            e = jnp.exp2(t - jnp.max(t, axis=0, keepdims=True))
            total = jnp.sum(e, axis=0, keepdims=True)
            mixed = mm(vt[h * hd:(h + 2) * hd, cols], e.astype(bf16)) / total
            gat[h * hd:(h + 1) * hd, cols] = (mixed[:hd, :size] * sig[h * hd:(h + 1) * hd, cols]).astype(bf16)
            gat[(h + 1) * hd:(h + 2) * hd, cols] = (mixed[hd:, size:] * sig[(h + 1) * hd:(h + 2) * hd, cols]).astype(bf16)

    for k, buf in enumerate(stash):
        def several(u, carry):
            for j in range(4):
                one(k * SLOT + 4 * u + j, 4 * u + j, buf)
            return carry

        lax.fori_loop(0, SLOT // 4, several, 0)
        for b in range(SLOT * size // bp):
            rows = slice((k * SLOT * size // bp + b) * bp, (k * SLOT * size // bp + b + 1) * bp)
            y = (x_ref[rows, :].astype(f32) + mm(gat[:, rows], wout_ref[...], TN)).astype(bf16).astype(f32)
            for i in range(bp // size):
                for half in range(width // 128):
                    ytr[half, pl.ds(b * (bp // size) + i, size, stride=SLOT), :] = (
                        y[i * size:(i + 1) * size, half * 128:(half + 1) * 128])
        ship(k, jnp.concatenate([ytr[half] for half in range(width // 128)], axis=1).astype(bf16))


def block_kernel(group, dap, m_ref, z_ref, mask_ref, res_ref, wr_in, wr_bias, wr_out, wc_in, wc_out, wopm_in, wopm_out,
                 ws_in, ws_bias, ws_out, we_in, we_bias, we_out, mout, zout,
                 kk, qt, rvt, rsig, rgat, bias, rwt, qd0, qd1, rsend, rbuf, rscr, ytr, msend, xbuf, mrow, norm, tnorm, zst, ztbuf,
                 kaug, qaug, vt, sig, gat, s0, s1, wt, wka, ycol, acs, abuf, cbuf,
                 oscr, uscr, usend, ubuf, zrow, bsend, bbuf, bscr, esend, ebuf, zsend, zfin, send, recv):
    net = Links(group, dap, send, recv)
    me, lo, hi = net.me, net.lo, net.hi
    opm = abuf.shape[2]
    seq, size = mask_ref.shape
    chunks = xbuf.shape[0]
    bq = s0.shape[1]
    per = bq // SLOT
    turns = group // per

    def side():
        zrow[...] = z_ref[...].astype(f32)
        for x in range(INNER):
            zst[x] = zrow[pl.ds(x, group // INNER, stride=INNER), :]
        ztbuf[lo] = zst[lo]
        net.to_inner(lambda x: (zst.at[x], ztbuf.at[lo]), 14)
        flags = mask_ref[...].astype(bf16)
        source = lax.broadcasted_iota(jnp.int32, (size, size), 0)
        pair = lax.broadcasted_iota(jnp.int32, (size, size), 1)
        rows_i = mm(flags, (source == hi * INNER + lax.rem(pair, INNER)).astype(bf16))
        rows_j = mm(flags, (source == lax.div(pair, INNER) * INNER + lo).astype(bf16))
        tnorm[...] = jnp.transpose(jnp.broadcast_to(jnp.sum(rows_i * rows_j, axis=0, keepdims=True), (size, size)))
        pick = (lax.broadcasted_iota(jnp.int32, (size, size), 0) == me).astype(bf16)
        norm[...] = mm(flags, mm(flags, pick).astype(bf16), TN)
        row = (lax.broadcasted_iota(jnp.int32, (SLOT, size), 1) == me).astype(bf16)
        split = mask_ref[...].reshape(group, chunks, SLOT, size)
        for k in range(chunks):
            mrow[:, k * group * SLOT:(k + 1) * group * SLOT] = mm(
                row, split[:, k].astype(f32).reshape(group * SLOT, size).astype(bf16), NT)

    def ship(k, y):
        msend[k] = y.astype(f32).reshape(group, SLOT, -1).astype(bf16)
        xbuf[k, me] = msend[k, me]
        net.to_all(lambda t: (msend.at[k, t], xbuf.at[k, me]), 8 + k)

    row_stage(net, m_ref, z_ref, mask_ref, wr_bias, wr_in, wr_out, ship, side, (s0, s1),
              kk, qt, rvt, rsig, rgat, bias, rwt, qd0, qd1, rsend, rbuf, rscr, ytr)

    def arrive(b):
        @pl.when(lax.rem(b, turns) == 0)
        def _():
            k = lax.div(b, turns)
            net.settle(xbuf.at[k, pl.ds(0, group - 1)], 8 + k)

    def load(b):
        part = xbuf[b // turns, pl.ds(pl.multiple_of(b % turns * per, per), per)]
        return part.astype(f32).reshape(bq, -1)

    half = pl.ds(pl.multiple_of(lax.div(hi, net.outer_n // 2) * (net.outer_n // 2), net.outer_n // 2), net.outer_n // 2)

    def pass_on(qb):
        net.settle(cbuf.at[qb, pl.ds(0, net.outer_n // 2 - 1)], 10 + qb)
        net.to_partner(cbuf.at[qb, half], 1)

    def emit(qb, y, ac):
        ycol[qb] = y.astype(f32).reshape(per, SLOT, -1).astype(bf16)
        acs[qb] = ac
        abuf[qb, lo] = ac[:opm]
        cbuf[qb, hi] = ac[opm:]
        net.to_half(acs.at[qb, pl.ds(opm, opm)], cbuf.at[qb, hi], 10 + qb)
        net.to_inner(lambda x: (acs.at[qb, pl.ds(0, opm)], abuf.at[qb, lo]), 0)

        @pl.when(qb > 0)
        def _():
            pass_on(qb - 1)

        def share_m(o):
            i = lax.rem(me + o, per)
            t = lax.rem(qb, turns) * per + i

            @pl.when(t != me)
            def _():
                net.copy(ycol.at[qb, i], mout.at[lax.div(qb, turns), me], 2, t).start()

        each(0, per, share_m)

    col_stage(arrive, load, seq, mrow, wc_in, wc_out, wopm_in, emit, kaug, qaug, vt, sig, gat, s0, s1, wt, wka)
    for k in range(chunks):
        mout[k, me] = ycol[k * turns + lax.div(me, per), lax.rem(me, per)]
    pass_on(cbuf.shape[0] - 1)
    net.settle(cbuf.at[:, pl.ds(0, net.outer_n // 2)], 1)
    net.settle(abuf.at[:, pl.ds(0, INNER - 1)], 0)
    pair_stage(net, z_ref, norm, tnorm, ztbuf, res_ref, wopm_out, ws_in, ws_bias, ws_out, we_in, we_bias, we_out, zout,
               abuf, cbuf, oscr, uscr, usend, ubuf, zrow, bsend, bbuf, bscr, esend, ebuf, zsend, zfin)
    net.settle(mout.at[:, pl.ds(0, group - 1)], 2)


def row_scratch(tokens, size, width, z_width, heads, fold, group):
    seqs = tokens // size
    return [
        pltpu.VMEM((tokens, fold), bf16),
        pltpu.VMEM((fold, tokens), bf16),
        pltpu.VMEM((fold, tokens), bf16),
        pltpu.VMEM((fold, tokens), f32),
        pltpu.VMEM((fold, tokens), bf16),
        pltpu.VMEM((size, heads * size), f32),
        pltpu.VMEM((4 * fold, width), bf16),
        pltpu.VMEM((fold, heads * size), bf16),
        pltpu.VMEM((fold, heads * size), bf16),
        pltpu.VMEM((SLOT, size), bf16),
        pltpu.VMEM((group, SLOT, size), bf16),
        pltpu.VMEM((group * SLOT, size), f32),
        pltpu.VMEM((width // 128, SLOT * size, 128), f32),
        pltpu.VMEM((seqs // SLOT, group, SLOT, width), bf16),
        pltpu.VMEM((seqs // SLOT, group, SLOT, width), bf16),
        pltpu.VMEM((SLOT, seqs * group), f32),
        pltpu.VMEM((size, size), f32),
        pltpu.VMEM((size, size), f32),
        pltpu.VMEM((INNER, group // INNER, z_width), f32),
        pltpu.VMEM((INNER, group // INNER, z_width), f32),
    ]


def col_scratch(seq, width, heads, hd, bq):
    return [
        pltpu.VMEM((heads, seq, 128), bf16),
        pltpu.VMEM((heads, 128, seq), bf16),
        pltpu.VMEM((heads, hd, seq), bf16),
        pltpu.VMEM((heads, hd, seq), f32),
        pltpu.VMEM((heads * hd, bq), bf16),
        pltpu.VMEM((seq, bq), f32),
        pltpu.VMEM((seq, bq), f32),
        pltpu.VMEM((4 * heads * hd, width), bf16),
        pltpu.VMEM((width, heads * 128), bf16),
        pltpu.VMEM((seq // bq, bq // SLOT, SLOT, width), bf16),
    ]


def pair_scratch(seq, size, width, opm, group, bq):
    outer_n = group // INNER
    return [
        pltpu.VMEM((seq // bq, 2 * opm, bq), bf16),
        pltpu.VMEM((seq // bq, INNER, opm, bq), bf16),
        pltpu.VMEM((seq // bq, outer_n, opm, bq), bf16),
        pltpu.VMEM((outer_n * opm // 128, INNER * opm, 128), f32),
        pltpu.VMEM((size, width), f32),
        pltpu.VMEM((INNER, outer_n, width), f32),
        pltpu.VMEM((INNER, outer_n, width), f32),
        pltpu.VMEM((size, width), f32),
        pltpu.VMEM((SLOT, size), bf16),
        pltpu.VMEM((group, SLOT, size), bf16),
        pltpu.VMEM((group * SLOT, size), f32),
        pltpu.VMEM((group, SLOT, size), bf16),
        pltpu.VMEM((group, SLOT, size), bf16),
        pltpu.VMEM((size, width), f32),
        pltpu.VMEM((size, width), f32),
    ]


def block_update(m, z, msa_mask, res_mask, weights, heads, group, dap, bq=512):
    vm = pl.BlockSpec(memory_space=pltpu.VMEM)
    tokens, m_width = m.shape
    size, width = z.shape
    seqs = tokens // size
    seq = seqs * group
    fold = weights[2].shape[0]
    opm = weights[5].shape[0] // 2
    return pl.pallas_call(
        functools.partial(block_kernel, group, dap),
        out_shape=(jax.ShapeDtypeStruct((seqs // SLOT, group, SLOT, m_width), bf16), jax.ShapeDtypeStruct((size, width), bf16)),
        in_specs=[vm] * (4 + len(weights)),
        out_specs=(vm, vm),
        scratch_shapes=row_scratch(tokens, size, m_width, width, heads, fold, group)
        + col_scratch(seq, m_width, heads, fold // heads, bq)
        + pair_scratch(seq, size, width, opm, group, bq)
        + [pltpu.SemaphoreType.DMA((15,)), pltpu.SemaphoreType.DMA((15,))],
        compiler_params=pltpu.CompilerParams(collective_id=1, has_side_effects=True, vmem_limit_bytes=63 << 20),
        name='block_update',
    )(m, z, msa_mask, res_mask, *weights)


def solution(mesh):
    dap_size = mesh.shape['dap']
    group_size = mesh.shape['chip'] * dap_size
    rows = P(('data', 'chip', 'dap'))
    in_specs = (rows, rows, P('data'), P('data')) + (P(),) * 13

    def per_device(m_blk, z_blk, msa_mask, res_mask, w_row_in, w_row_bias, w_row_out, w_col_in, w_col_out,
                   w_opm_in, w_opm_out, w_start_in, w_start_bias, w_start_out, w_end_in, w_end_bias, w_end_out):
        seqs, res, width = m_blk.shape
        weights = (w_row_in, w_row_bias.T, w_row_out, w_col_in, w_col_out, w_opm_in.T, w_opm_out,
                   w_start_in, w_start_bias.T, w_start_out, w_end_in, w_end_bias.T, w_end_out)
        slots, z_out = block_update(m_blk.reshape(seqs * res, width), z_blk[0], msa_mask, res_mask[None, :], weights,
                                    w_row_bias.shape[1], group_size, dap_size)
        m_out = jnp.swapaxes(slots, 1, 2).reshape(seqs, res, width)
        return m_out, z_out[None]

    return jax.shard_map(per_device, mesh=mesh, in_specs=in_specs, out_specs=(rows, rows), check_vma=False)
```

```python
import functools

import jax
import jax.numpy as jnp
import numpy as np
from jax import lax
from jax.experimental import pallas as pl
from jax.experimental.pallas import tpu as pltpu
from jax.sharding import PartitionSpec as P

LOG2E = 1.4426950408889634
f32, bf16 = jnp.float32, jnp.bfloat16


def split3(value):
    parts = []
    rest = np.float64(value)
    for _ in range(3):
        part = np.float64(np.asarray(rest, dtype=jnp.bfloat16))
        parts.append(float(part))
        rest = rest - part
    return parts


def norm_rows(x):
    values = x.astype(f32)
    centred = values - jnp.mean(values, axis=-1, keepdims=True)
    variance = jnp.mean(centred * centred, axis=-1, keepdims=True)
    return (centred * lax.rsqrt(variance + 1e-5)).astype(bf16)


def dot_t(w, x):
    return lax.dot_general(w, x, (((0,), (1,)), ((), ())), preferred_element_type=f32)


NT = (((1,), (1,)), ((), ()))
TN = (((0,), (0,)), ((), ()))
NEG = -1e9 * LOG2E


def mm(a, b, dims=(((1,), (0,)), ((), ()))):
    return lax.dot_general(a, b, dims, preferred_element_type=f32)


NN = (((1,), (0,)), ((), ()))
MESH = pl.DeviceIdType.MESH
INNER = 8
SLOT = 8


def place(t, dap):
    return (0, lax.div(t, dap), lax.rem(t, dap))


def pair_project(x, win_ref, fold):
    xn = norm_rows(x)
    k = mm(xn, win_ref[:, fold:2 * fold]).astype(bf16)
    qt = dot_t(win_ref[:, :fold], xn).astype(bf16)
    vt = dot_t(win_ref[:, 2 * fold:3 * fold], xn).astype(bf16)
    gg = dot_t(win_ref[:, 3 * fold:], xn).astype(bf16).astype(f32)
    return k, qt, vt, 1.0 / (1.0 + jnp.exp(-gg))


def pair_attend(x, parts, biases, keep, wout_ref):
    k, qt, vt, sig = parts
    heads = len(biases)
    hd = vt.shape[0] // heads
    c = hd ** -0.5 * LOG2E
    gated = []
    for h in range(heads):
        part = slice(h * hd, (h + 1) * hd)
        t = mm(k[:, part], qt[part]) * c + biases[h] * LOG2E
        t = jnp.where(keep, t, NEG)
        e = jnp.exp2(t - jnp.max(t, axis=0, keepdims=True))
        mixed = mm(vt[part], e.astype(bf16)) / jnp.sum(e, axis=0, keepdims=True)
        gated.append((mixed * sig[part]).astype(bf16))
    up = mm(jnp.concatenate(gated, axis=0), wout_ref[...], TN)
    return (x.astype(f32) + up).astype(bf16)


def col_stage(arrive, load, seq, mrow_ref, win_ref, wout_ref, wopm_ref, emit,
              kaug, qaug, vt, sig, gat, s0, s1, wt, wka):
    heads, hd = vt.shape[0], vt.shape[1]
    fold = heads * hd
    bq = s0.shape[1]
    nq = seq // bq
    kc = 256
    nk = seq // kc
    c = hd ** -0.5 * LOG2E
    masked = split3(-1e9 * LOG2E)

    lane = lax.broadcasted_iota(jnp.int32, (bq, 128), 1)
    row = lax.broadcasted_iota(jnp.int32, (128 - 3 * hd, bq), 0)
    fill = jnp.where(row == 0, masked[0], jnp.where(row == 1, masked[1], jnp.where(row == 2, masked[2], 0.0))).astype(bf16)
    flag = ((lane >= 3 * hd) & (lane < 3 * hd + 3)).astype(f32)
    flag2 = jnp.concatenate([flag, flag], axis=1)

    wt[...] = jnp.transpose(win_ref[...])
    for h in range(heads):
        wk = win_ref[:, fold + h * hd:fold + (h + 1) * hd]
        wka[:, h * 128:(h + 1) * 128] = jnp.concatenate([wk, wk, wk, jnp.zeros_like(wk)], axis=1)

    def project(b, carry):
        rows = pl.ds(pl.multiple_of(b * bq, bq), bq)
        arrive(b)
        xn = norm_rows(load(b))
        keep = jnp.transpose(jnp.broadcast_to(mrow_ref[0:1, rows], (128, bq))) != 0
        keep2 = jnp.concatenate([keep, keep], axis=1)
        for h in range(0, heads, 2):
            k = mm(xn, wka[:, h * 128:(h + 2) * 128])
            k = jnp.where(keep2, k, flag2).astype(bf16)
            kaug[h, rows, :] = k[:, :128]
            kaug[h + 1, rows, :] = k[:, 128:]
        qt = mm(wt[:fold, :], xn, NT).astype(bf16).astype(f32) * c
        hi = qt.astype(bf16)
        rest = qt - hi.astype(f32)
        mid = rest.astype(bf16)
        low = (rest - mid.astype(f32)).astype(bf16)
        vv = mm(wt[2 * fold:3 * fold, :], xn, NT).astype(bf16)
        gg = mm(wt[3 * fold:, :], xn, NT).astype(bf16).astype(f32)
        gg = 1.0 / (1.0 + jnp.exp(-gg))
        for h in range(heads):
            part = slice(h * hd, (h + 1) * hd)
            qaug[h, 0:hd, rows] = hi[part]
            qaug[h, hd:2 * hd, rows] = mid[part]
            qaug[h, 2 * hd:3 * hd, rows] = low[part]
            qaug[h, 3 * hd:, rows] = fill
            vt[h, :, rows] = vv[part]
            sig[h, :, rows] = gg[part]
        return carry

    lax.fori_loop(0, nq, project, 0)

    def fold8(s):
        return s.reshape(kc // 8, 8, bq)

    def chunk_scores(h, q, i, buf, m):
        s = mm(kaug[h, i * kc:(i + 1) * kc, :], q)
        buf[i * kc:(i + 1) * kc, :] = s
        top = jnp.max(fold8(s), axis=0)
        return top if m is None else jnp.maximum(m, top)

    def step(qb, h, cur, nxt, m):
        t = jnp.minimum(qb * heads + h + 1, nq * heads - 1)
        hn = t % heads
        q = qaug[hn, :, pl.ds(pl.multiple_of(t // heads * bq, bq), bq)]
        top = jnp.max(m, axis=0, keepdims=True)
        mn = None
        total = jnp.zeros((8, bq), f32)
        mixed = jnp.zeros((hd, bq), f32)
        held = None
        for i in range(nk):
            mn = chunk_scores(hn, q, i, nxt, mn)
            if held is not None:
                mixed = mixed + mm(vt[h, :, (i - 1) * kc:i * kc], held)
            e = jnp.exp2(cur[i * kc:(i + 1) * kc, :] - top)
            total = total + jnp.sum(fold8(e), axis=0)
            held = e.astype(bf16)
        mixed = mixed + mm(vt[h, :, (nk - 1) * kc:], held)
        cols = pl.ds(pl.multiple_of(qb * bq, bq), bq)
        mixed = mixed / jnp.sum(total, axis=0, keepdims=True)
        gat[pl.ds(pl.multiple_of(h * hd, hd), hd), :] = (mixed * sig[h, :, cols]).astype(bf16)
        return mn

    m = None
    for i in range(nk):
        m = chunk_scores(0, qaug[0, :, 0:bq], i, s0, m)

    def block(qb, m):
        def pair(u, m):
            m = step(qb, 2 * u, s0, s1, m)
            return step(qb, 2 * u + 1, s1, s0, m)

        m = lax.fori_loop(0, heads // 2, pair, m)
        rows = pl.ds(pl.multiple_of(qb * bq, bq), bq)
        y = (load(qb).astype(f32) + mm(gat[...], wout_ref[...], TN)).astype(bf16)
        ac = mm(wopm_ref[...], norm_rows(y), NT).astype(bf16)
        emit(qb, y, (ac.astype(f32) * mrow_ref[0:1, rows]).astype(bf16))
        return m

    lax.fori_loop(0, nq, block, m)


def each(start, stop, one, step=8):
    whole = (stop - start) // step

    def some(i, carry):
        for j in range(step):
            one(start + i * step + j)
        return carry

    lax.fori_loop(0, whole, some, 0)
    for o in range(start + whole * step, stop):
        one(o)


class Links:
    def __init__(self, group, dap, send, recv):
        self.group, self.dap, self.send, self.recv = group, dap, send, recv
        self.me = lax.axis_index('chip') * dap + lax.axis_index('dap')
        self.hi, self.lo = lax.div(self.me, INNER), lax.rem(self.me, INNER)
        self.outer_n = group // INNER

    def greet(self):
        barrier = pltpu.get_barrier_semaphore()

        def one(o):
            t = lax.rem(self.me + o, self.group)
            pl.semaphore_signal(barrier, inc=1, device_id=place(t, self.dap), device_id_type=MESH)

        each(1, self.group, one)

    def ready(self):
        pl.semaphore_wait(pltpu.get_barrier_semaphore(), self.group - 1)

    def copy(self, src, dst, i, t):
        return pltpu.make_async_remote_copy(src_ref=src, dst_ref=dst, send_sem=self.send.at[i], recv_sem=self.recv.at[i],
                                            device_id=place(t, self.dap), device_id_type=MESH)

    def settle(self, part, i):
        done = self.copy(part, part, i, self.me)
        done.wait_send()
        done.wait_recv()

    def to_all(self, make, i):
        def one(o):
            t = lax.rem(self.me + o, self.group)
            src, dst = make(t)
            self.copy(src, dst, i, t).start()

        each(1, self.group, one)

    def to_inner(self, make, i):
        for o in range(1, INNER):
            x = lax.rem(self.lo + o, INNER)
            src, dst = make(x)
            self.copy(src, dst, i, self.hi * INNER + x).start()

    def to_half(self, src, dst, i):
        half = self.outer_n // 2
        base = lax.div(self.hi, half) * half
        for o in range(1, half):
            y = base + lax.rem(lax.rem(self.hi, half) + o, half)
            self.copy(src, dst, i, y * INNER + self.lo).start()

    def to_partner(self, part, i):
        self.copy(part, part, i, lax.rem(self.me + self.group // 2, self.group)).start()


def bias_rows(z, weight):
    rows = mm(weight[...], norm_rows(z), NT).astype(bf16)
    spare = SLOT - rows.shape[0]
    return jnp.concatenate([rows, jnp.zeros((spare, rows.shape[1]), bf16)], axis=0) if spare else rows


def untile(block):
    size = block.shape[0]
    out = jnp.transpose(block)
    row = lax.broadcasted_iota(jnp.int32, (size, size), 0)
    lane = lax.broadcasted_iota(jnp.int32, (size, size), 1)
    step = INNER // 2
    while step:
        low, high = lax.rem(lax.div(row, step), 2), lax.rem(lax.div(lane, step), 2)
        down = pltpu.roll(pltpu.roll(out, size - step, 0), step, 1)
        back = pltpu.roll(pltpu.roll(out, step, 0), size - step, 1)
        out = jnp.where(low == high, out, jnp.where(low < high, down, back))
        step //= 2
    return out


def pair_stage(net, between, collect, z_ref, norm, tnorm, ztbuf, mask_ref, wopm_ref, ws_in, ws_bias, ws_out, we_in, we_bias, we_out, zout,
               abuf, cbuf, oscr, uscr, usend, ubuf, zrow, bsend, bbuf, bscr, esend, ebuf, zsend, zfin):
    me, lo, group, outer_n = net.me, net.lo, net.group, net.outer_n
    blocks, opm = abuf.shape[0], abuf.shape[2]
    heads = ws_bias.shape[0]
    fold = ws_out.shape[0]
    size = z_ref.shape[0]
    keep = jnp.transpose(jnp.broadcast_to(mask_ref[...].astype(f32), (size, size))) != 0

    per = 128 // opm
    outer = None
    for q in range(blocks):
        net.settle(abuf.at[q, pl.ds(0, INNER - 1)], 15 + q)
        net.settle(cbuf.at[q, pl.ds(0, outer_n // 2)], 19 + q)
        term = mm(abuf[q].reshape(INNER * opm, -1), cbuf[q].reshape(outer_n * opm, -1), NT)
        outer = term if outer is None else outer + term
    for g in range(outer_n // per):
        oscr[g] = outer[:, g * 128:(g + 1) * 128]
    lane = lax.broadcasted_iota(jnp.int32, (opm // per * INNER, 128), 1) // opm
    tiles = []
    for g in range(outer_n // per):
        slabs = [jnp.concatenate([oscr[g, pl.ds(b * per + r, INNER, stride=opm), :] for b in range(opm // per)], axis=0)
                 for r in range(per)]
        turned = [[slabs[r] if s == 0 else pltpu.roll(slabs[r], s * opm, 1) for s in range(per)] for r in range(per)]
        for q in range(per):
            pick = turned[0][(0 - q) % per]
            for r in range(1, per):
                pick = jnp.where(lane == r, turned[r][(r - q) % per], pick)
            tiles.append(pick)
    up = None
    for b in range(opm // per):
        block = jnp.concatenate([t[b * INNER:(b + 1) * INNER] for t in tiles], axis=0).astype(bf16)
        term = mm(block, wopm_ref[b * 128:(b + 1) * 128, :])
        up = term if up is None else up + term
    uscr[...] = up
    for x in range(INNER):
        usend[x] = uscr[pl.ds(x, outer_n, stride=INNER), :]
    ubuf[lo] = usend[lo]
    net.to_inner(lambda x: (usend.at[x], ubuf.at[lo]), 3)
    net.settle(ztbuf.at[pl.ds(0, INNER - 1)], 14)
    for x in range(INNER):
        zrow[pl.ds(x, outer_n, stride=INNER), :] = ztbuf[x]
    tile = (zrow[...] + up / (1e-3 + tnorm[...])).astype(bf16)
    bsend[...] = bias_rows(tile, ws_bias)
    bbuf[me] = bsend[...]
    net.to_all(lambda t: (bsend, bbuf.at[me]), 4)
    between()
    net.settle(ubuf.at[pl.ds(0, INNER - 1)], 3)
    for x in range(INNER):
        zrow[pl.ds(x, outer_n, stride=INNER), :] = ubuf[x]
    z1 = (z_ref[...].astype(f32) + zrow[...] / (1e-3 + norm[...])).astype(bf16)

    parts = pair_project(z1, ws_in, fold)
    net.settle(bbuf.at[pl.ds(0, group - 1)], 4)
    bscr[...] = bbuf[...].astype(f32).reshape(group * SLOT, size)
    biases = [untile(bscr[pl.ds(h, size, stride=SLOT), :]) for h in range(heads)]
    z2 = pair_attend(z1, parts, biases, keep, ws_out)

    end_rows = bias_rows(z2, we_bias).astype(f32)
    for h in range(heads):
        bscr[pl.ds(h, size, stride=SLOT), :] = jnp.broadcast_to(end_rows[h:h + 1], (size, size))
    bscr[pl.ds(heads, size, stride=SLOT), :] = z2.astype(f32)
    esend[...] = bscr[...].astype(bf16).reshape(group, SLOT, size)
    ebuf[me] = esend[me]
    net.to_all(lambda t: (esend.at[t], ebuf.at[me]), 5)
    net.settle(ebuf.at[pl.ds(0, group - 1)], 5)
    bscr[...] = ebuf[...].astype(f32).reshape(group * SLOT, size)
    zc = bscr[pl.ds(heads, size, stride=SLOT), :].astype(bf16)
    biases = [bscr[pl.ds(h, size, stride=SLOT), :] for h in range(heads)]
    z3 = pair_attend(zc, pair_project(zc, we_in, fold), biases, keep, we_out)

    zsend[...] = z3.astype(f32)
    zfin[pl.ds(me, 1), :] = zsend[pl.ds(me, 1), :]
    net.to_all(lambda t: (zsend.at[pl.ds(t, 1)], zfin.at[pl.ds(me, 1)]), 6)
    collect()
    net.settle(zfin.at[pl.ds(0, group - 1)], 6)
    zout[...] = zfin[...].astype(bf16)


def row_stage(net, x_ref, z_ref, mask_ref, wb_ref, win_ref, wout_ref, ship, side, stash,
              kk, qt, vt, sig, gat, bias, wt, qd0, qd1, bsend, bbuf, bscr, ytr):
    tokens, width = x_ref.shape
    size = bias.shape[0]
    seqs = tokens // size
    heads = bias.shape[1] // size
    fold = gat.shape[0]
    hd = fold // heads
    c = hd ** -0.5 * LOG2E
    bp = 512
    me, group = net.me, net.group

    net.greet()
    bsend[...] = bias_rows(z_ref[...], wb_ref)
    bbuf[me] = bsend[...]
    wt[...] = jnp.transpose(win_ref[...])
    qd0[...] = jnp.zeros_like(qd0)
    qd1[...] = jnp.zeros_like(qd1)

    def project(b, carry):
        rows = pl.ds(pl.multiple_of(b * bp, bp), bp)
        xn = norm_rows(x_ref[rows, :])
        kk[rows, :] = mm(xn, win_ref[:, fold:2 * fold]).astype(bf16)
        qt[:, rows] = mm(wt[:fold, :], xn, NT).astype(bf16)
        vt[:, rows] = mm(wt[2 * fold:3 * fold, :], xn, NT).astype(bf16)
        gg = mm(wt[3 * fold:, :], xn, NT).astype(bf16).astype(f32)
        sig[:, rows] = 1.0 / (1.0 + jnp.exp(-gg))

        @pl.when(b == 0)
        def _():
            net.ready()
            net.to_all(lambda t: (bsend, bbuf.at[me]), 7)

        return carry

    lax.fori_loop(0, tokens // bp, project, 0)
    slab = heads // 2

    def prescore(s, u, buf, qd):
        cols = pl.ds(pl.multiple_of(s * size, size), size)
        for h in range(heads):
            qd[h * hd:(h + 1) * hd, h * size:(h + 1) * size] = qt[h * hd:(h + 1) * hd, cols]
        for g in range(2):
            out = pl.ds(pl.multiple_of((2 * u + g) * size, size), size)
            buf[out, :] = mm(kk[cols, :], qd[:, g * slab * size:(g + 1) * slab * size]) * c

    for k, buf in enumerate(stash):
        def ahead(u, carry):
            prescore(k * SLOT + 2 * u, 2 * u, buf, qd0)
            prescore(k * SLOT + 2 * u + 1, 2 * u + 1, buf, qd1)
            return carry

        lax.fori_loop(0, SLOT // 2, ahead, 0)
    side()
    net.settle(bbuf.at[pl.ds(0, group - 1)], 7)
    bscr[...] = bbuf[...].astype(f32).reshape(group * SLOT, size)
    for h in range(heads):
        bias[:, h * size:(h + 1) * size] = jnp.transpose(bscr[pl.ds(h, size, stride=SLOT), :] * LOG2E)

    def one(s, u, buf):
        cols = pl.ds(pl.multiple_of(s * size, size), size)
        mrow = mask_ref[pl.ds(me * seqs + s, 1), :]
        keep = jnp.transpose(jnp.broadcast_to(mrow.astype(f32), (size, size))) != 0
        keep2 = jnp.concatenate([keep, keep], axis=1)
        for h in range(0, heads, 2):
            two = slice(h * size, (h + 2) * size)
            rows = pl.ds(pl.multiple_of((2 * u + h // slab) * size, size), size)
            t = buf[rows, h % slab * size:(h % slab + 2) * size] + bias[:, two]
            t = jnp.where(keep2, t, NEG)
            e = jnp.exp2(t - jnp.max(t, axis=0, keepdims=True))
            total = jnp.sum(e, axis=0, keepdims=True)
            mixed = mm(vt[h * hd:(h + 2) * hd, cols], e.astype(bf16)) / total
            gat[h * hd:(h + 1) * hd, cols] = (mixed[:hd, :size] * sig[h * hd:(h + 1) * hd, cols]).astype(bf16)
            gat[(h + 1) * hd:(h + 2) * hd, cols] = (mixed[hd:, size:] * sig[(h + 1) * hd:(h + 2) * hd, cols]).astype(bf16)

    for k, buf in enumerate(stash):
        def several(u, carry):
            for j in range(4):
                one(k * SLOT + 4 * u + j, 4 * u + j, buf)
            return carry

        lax.fori_loop(0, SLOT // 4, several, 0)
        for b in range(SLOT * size // bp):
            rows = slice((k * SLOT * size // bp + b) * bp, (k * SLOT * size // bp + b + 1) * bp)
            y = (x_ref[rows, :].astype(f32) + mm(gat[:, rows], wout_ref[...], TN)).astype(bf16).astype(f32)
            for i in range(bp // size):
                for half in range(width // 128):
                    ytr[half, pl.ds(b * (bp // size) + i, size, stride=SLOT), :] = (
                        y[i * size:(i + 1) * size, half * 128:(half + 1) * 128])
        ship(k, jnp.concatenate([ytr[half] for half in range(width // 128)], axis=1).astype(bf16))


def block_kernel(group, dap, m_ref, z_ref, mask_ref, res_ref, wr_in, wr_bias, wr_out, wc_in, wc_out, wopm_in, wopm_out,
                 ws_in, ws_bias, ws_out, we_in, we_bias, we_out, mout, zout,
                 kk, qt, rvt, rsig, rgat, bias, rwt, qd0, qd1, rsend, rbuf, rscr, ytr, msend, xbuf, mrow, norm, tnorm, zst, ztbuf, mslot,
                 kaug, qaug, vt, sig, gat, s0, s1, wt, wka, ycol, acs, abuf, cbuf,
                 oscr, uscr, usend, ubuf, zrow, bsend, bbuf, bscr, esend, ebuf, zsend, zfin, send, recv):
    net = Links(group, dap, send, recv)
    me, lo, hi = net.me, net.lo, net.hi
    opm = abuf.shape[2]
    seq, size = mask_ref.shape
    chunks = xbuf.shape[0]
    bq = s0.shape[1]
    per = bq // SLOT
    turns = group // per

    def side():
        zrow[...] = z_ref[...].astype(f32)
        for x in range(INNER):
            zst[x] = zrow[pl.ds(x, group // INNER, stride=INNER), :]
        ztbuf[lo] = zst[lo]
        net.to_inner(lambda x: (zst.at[x], ztbuf.at[lo]), 14)
        row = (lax.broadcasted_iota(jnp.int32, (SLOT, size), 1) == me).astype(bf16)
        split = mask_ref[...].reshape(group, chunks, SLOT, size)
        for k in range(chunks):
            mrow[:, k * group * SLOT:(k + 1) * group * SLOT] = mm(
                row, split[:, k].astype(f32).reshape(group * SLOT, size).astype(bf16), NT)

    def normalisers():
        flags = mask_ref[...].astype(bf16)
        source = lax.broadcasted_iota(jnp.int32, (size, size), 0)
        pair = lax.broadcasted_iota(jnp.int32, (size, size), 1)
        rows_i = mm(flags, (source == hi * INNER + lax.rem(pair, INNER)).astype(bf16))
        rows_j = mm(flags, (source == lax.div(pair, INNER) * INNER + lo).astype(bf16))
        tnorm[...] = jnp.transpose(jnp.broadcast_to(jnp.sum(rows_i * rows_j, axis=0, keepdims=True), (size, size)))
        pick = (lax.broadcasted_iota(jnp.int32, (size, size), 0) == me).astype(bf16)
        norm[...] = mm(flags, mm(flags, pick).astype(bf16), TN)

    def ship(k, y):
        msend[k] = y.astype(f32).reshape(group, SLOT, -1).astype(bf16)
        xbuf[k, me] = msend[k, me]
        net.to_all(lambda t: (msend.at[k, t], xbuf.at[k, me]), 8 + k)

    row_stage(net, m_ref, z_ref, mask_ref, wr_bias, wr_in, wr_out, ship, side, (s0, s1),
              kk, qt, rvt, rsig, rgat, bias, rwt, qd0, qd1, rsend, rbuf, rscr, ytr)

    def arrive(b):
        @pl.when(lax.rem(b, turns) == 0)
        def _():
            k = lax.div(b, turns)
            net.settle(xbuf.at[k, pl.ds(0, group - 1)], 8 + k)

    def load(b):
        part = xbuf[b // turns, pl.ds(pl.multiple_of(b % turns * per, per), per)]
        return part.astype(f32).reshape(bq, -1)

    half = pl.ds(pl.multiple_of(lax.div(hi, net.outer_n // 2) * (net.outer_n // 2), net.outer_n // 2), net.outer_n // 2)

    def pass_on(qb):
        net.settle(cbuf.at[qb, pl.ds(0, net.outer_n // 2 - 1)], 10 + qb)
        net.to_partner(cbuf.at[qb, half], 19 + qb)

    last = cbuf.shape[0] - 1

    def give_back(qb):
        def share_m(o):
            i = lax.rem(me + o, per)
            t = lax.rem(qb, turns) * per + i

            @pl.when(t != me)
            def _():
                net.copy(ycol.at[qb, i], mslot.at[lax.div(qb, turns), me], 2, t).start()

        each(0, per, share_m)

    def collect():
        net.settle(mslot.at[:, pl.ds(0, group - 1)], 2)
        for k in range(chunks):
            y = mslot[k].astype(f32).reshape(group * SLOT, -1)
            for side_half in range(ytr.shape[0]):
                lanes = slice(side_half * 128, (side_half + 1) * 128)
                ytr[side_half] = y[:, lanes]
                for r in range(SLOT):
                    at = (k * SLOT + r) * size
                    mout[at:at + size, lanes] = ytr[side_half, pl.ds(r, size, stride=SLOT), :].astype(bf16)

    def emit(qb, y, ac):
        ycol[qb] = y.astype(f32).reshape(per, SLOT, -1).astype(bf16)
        acs[qb] = ac
        abuf[qb, lo] = ac[:opm]
        cbuf[qb, hi] = ac[opm:]
        net.to_half(acs.at[qb, pl.ds(opm, opm)], cbuf.at[qb, hi], 10 + qb)
        net.to_inner(lambda x: (acs.at[qb, pl.ds(0, opm)], abuf.at[qb, lo]), 15 + qb)

        @pl.when(qb > 0)
        def _():
            pass_on(qb - 1)

        @pl.when(qb < last)
        def _():
            give_back(qb)

    col_stage(arrive, load, seq, mrow, wc_in, wc_out, wopm_in, emit, kaug, qaug, vt, sig, gat, s0, s1, wt, wka)
    for k in range(chunks):
        mslot[k, me] = ycol[k * turns + lax.div(me, per), lax.rem(me, per)]
    normalisers()
    pass_on(last)
    pair_stage(net, lambda: give_back(last), collect, z_ref, norm, tnorm, ztbuf, res_ref, wopm_out, ws_in, ws_bias, ws_out, we_in, we_bias, we_out, zout,
               abuf, cbuf, oscr, uscr, usend, ubuf, zrow, bsend, bbuf, bscr, esend, ebuf, zsend, zfin)


def row_scratch(tokens, size, width, z_width, heads, fold, group):
    seqs = tokens // size
    return [
        pltpu.VMEM((tokens, fold), bf16),
        pltpu.VMEM((fold, tokens), bf16),
        pltpu.VMEM((fold, tokens), bf16),
        pltpu.VMEM((fold, tokens), f32),
        pltpu.VMEM((fold, tokens), bf16),
        pltpu.VMEM((size, heads * size), f32),
        pltpu.VMEM((4 * fold, width), bf16),
        pltpu.VMEM((fold, heads * size), bf16),
        pltpu.VMEM((fold, heads * size), bf16),
        pltpu.VMEM((SLOT, size), bf16),
        pltpu.VMEM((group, SLOT, size), bf16),
        pltpu.VMEM((group * SLOT, size), f32),
        pltpu.VMEM((width // 128, SLOT * size, 128), f32),
        pltpu.VMEM((seqs // SLOT, group, SLOT, width), bf16),
        pltpu.VMEM((seqs // SLOT, group, SLOT, width), bf16),
        pltpu.VMEM((SLOT, seqs * group), f32),
        pltpu.VMEM((size, size), f32),
        pltpu.VMEM((size, size), f32),
        pltpu.VMEM((INNER, group // INNER, z_width), f32),
        pltpu.VMEM((INNER, group // INNER, z_width), f32),
        pltpu.VMEM((seqs // SLOT, group, SLOT, width), bf16),
    ]


def col_scratch(seq, width, heads, hd, bq):
    return [
        pltpu.VMEM((heads, seq, 128), bf16),
        pltpu.VMEM((heads, 128, seq), bf16),
        pltpu.VMEM((heads, hd, seq), bf16),
        pltpu.VMEM((heads, hd, seq), f32),
        pltpu.VMEM((heads * hd, bq), bf16),
        pltpu.VMEM((seq, bq), f32),
        pltpu.VMEM((seq, bq), f32),
        pltpu.VMEM((4 * heads * hd, width), bf16),
        pltpu.VMEM((width, heads * 128), bf16),
        pltpu.VMEM((seq // bq, bq // SLOT, SLOT, width), bf16),
    ]


def pair_scratch(seq, size, width, opm, group, bq):
    outer_n = group // INNER
    return [
        pltpu.VMEM((seq // bq, 2 * opm, bq), bf16),
        pltpu.VMEM((seq // bq, INNER, opm, bq), bf16),
        pltpu.VMEM((seq // bq, outer_n, opm, bq), bf16),
        pltpu.VMEM((outer_n * opm // 128, INNER * opm, 128), f32),
        pltpu.VMEM((size, width), f32),
        pltpu.VMEM((INNER, outer_n, width), f32),
        pltpu.VMEM((INNER, outer_n, width), f32),
        pltpu.VMEM((size, width), f32),
        pltpu.VMEM((SLOT, size), bf16),
        pltpu.VMEM((group, SLOT, size), bf16),
        pltpu.VMEM((group * SLOT, size), f32),
        pltpu.VMEM((group, SLOT, size), bf16),
        pltpu.VMEM((group, SLOT, size), bf16),
        pltpu.VMEM((size, width), f32),
        pltpu.VMEM((size, width), f32),
    ]


def block_update(m, z, msa_mask, res_mask, weights, heads, group, dap, bq=512):
    vm = pl.BlockSpec(memory_space=pltpu.VMEM)
    tokens, m_width = m.shape
    size, width = z.shape
    seqs = tokens // size
    seq = seqs * group
    fold = weights[2].shape[0]
    opm = weights[5].shape[0] // 2
    return pl.pallas_call(
        functools.partial(block_kernel, group, dap),
        out_shape=(jax.ShapeDtypeStruct((tokens, m_width), bf16), jax.ShapeDtypeStruct((size, width), bf16)),
        in_specs=[vm] * (4 + len(weights)),
        out_specs=(vm, vm),
        scratch_shapes=row_scratch(tokens, size, m_width, width, heads, fold, group)
        + col_scratch(seq, m_width, heads, fold // heads, bq)
        + pair_scratch(seq, size, width, opm, group, bq)
        + [pltpu.SemaphoreType.DMA((23,)), pltpu.SemaphoreType.DMA((23,))],
        compiler_params=pltpu.CompilerParams(collective_id=1, has_side_effects=True, vmem_limit_bytes=63 << 20),
        name='block_update',
    )(m, z, msa_mask, res_mask, *weights)


def solution(mesh):
    dap_size = mesh.shape['dap']
    group_size = mesh.shape['chip'] * dap_size
    rows = P(('data', 'chip', 'dap'))
    in_specs = (rows, rows, P('data'), P('data')) + (P(),) * 13

    def per_device(m_blk, z_blk, msa_mask, res_mask, w_row_in, w_row_bias, w_row_out, w_col_in, w_col_out,
                   w_opm_in, w_opm_out, w_start_in, w_start_bias, w_start_out, w_end_in, w_end_bias, w_end_out):
        seqs, res, width = m_blk.shape
        weights = (w_row_in, w_row_bias.T, w_row_out, w_col_in, w_col_out, w_opm_in.T, w_opm_out,
                   w_start_in, w_start_bias.T, w_start_out, w_end_in, w_end_bias.T, w_end_out)
        m_out, z_out = block_update(m_blk.reshape(seqs * res, width), z_blk[0], msa_mask, res_mask[None, :], weights,
                                    w_row_bias.shape[1], group_size, dap_size)
        return m_out.reshape(seqs, res, width), z_out[None]

    return jax.shard_map(per_device, mesh=mesh, in_specs=in_specs, out_specs=(rows, rows), check_vma=False)
```

```python
import functools

import jax
import jax.numpy as jnp
import numpy as np
from jax import lax
from jax.experimental import pallas as pl
from jax.experimental.pallas import tpu as pltpu
from jax.sharding import PartitionSpec as P

LOG2E = 1.4426950408889634
f32, bf16 = jnp.float32, jnp.bfloat16


def split3(value):
    parts = []
    rest = np.float64(value)
    for _ in range(3):
        part = np.float64(np.asarray(rest, dtype=jnp.bfloat16))
        parts.append(float(part))
        rest = rest - part
    return parts


def norm_rows(x):
    values = x.astype(f32)
    centred = values - jnp.mean(values, axis=-1, keepdims=True)
    variance = jnp.mean(centred * centred, axis=-1, keepdims=True)
    return (centred * lax.rsqrt(variance + 1e-5)).astype(bf16)


def dot_t(w, x):
    return lax.dot_general(w, x, (((0,), (1,)), ((), ())), preferred_element_type=f32)


NT = (((1,), (1,)), ((), ()))
TN = (((0,), (0,)), ((), ()))
NEG = -1e9 * LOG2E


def mm(a, b, dims=(((1,), (0,)), ((), ()))):
    return lax.dot_general(a, b, dims, preferred_element_type=f32)


NN = (((1,), (0,)), ((), ()))
MESH = pl.DeviceIdType.MESH
INNER = 8
SLOT = 8


def place(t, dap):
    return (0, lax.div(t, dap), lax.rem(t, dap))


def pair_project(x, win_ref, fold):
    xn = norm_rows(x)
    k = mm(xn, win_ref[:, fold:2 * fold]).astype(bf16)
    qt = dot_t(win_ref[:, :fold], xn).astype(bf16)
    vt = dot_t(win_ref[:, 2 * fold:3 * fold], xn).astype(bf16)
    gg = dot_t(win_ref[:, 3 * fold:], xn).astype(bf16).astype(f32)
    return k, qt, vt, 1.0 / (1.0 + jnp.exp(-gg))


def pair_attend(x, parts, biases, keep, wout_ref):
    k, qt, vt, sig = parts
    heads = len(biases)
    hd = vt.shape[0] // heads
    c = hd ** -0.5 * LOG2E
    gated = []
    for h in range(heads):
        part = slice(h * hd, (h + 1) * hd)
        t = mm(k[:, part], qt[part]) * c + biases[h] * LOG2E
        t = jnp.where(keep, t, NEG)
        e = jnp.exp2(t - jnp.max(t, axis=0, keepdims=True))
        mixed = mm(vt[part], e.astype(bf16)) / jnp.sum(e, axis=0, keepdims=True)
        gated.append((mixed * sig[part]).astype(bf16))
    up = mm(jnp.concatenate(gated, axis=0), wout_ref[...], TN)
    return (x.astype(f32) + up).astype(bf16)


def col_stage(arrive, load, seq, mrow_ref, win_ref, wout_ref, wopm_ref, emit,
              kaug, qaug, vt, sig, gat, s0, s1, wt, wka):
    heads, hd = vt.shape[0], vt.shape[1]
    fold = heads * hd
    bq = s0.shape[1]
    nq = seq // bq
    kc = 256
    nk = seq // kc
    c = hd ** -0.5 * LOG2E
    masked = split3(-1e9 * LOG2E)

    lane = lax.broadcasted_iota(jnp.int32, (bq, 128), 1)
    row = lax.broadcasted_iota(jnp.int32, (128 - 3 * hd, bq), 0)
    fill = jnp.where(row == 0, masked[0], jnp.where(row == 1, masked[1], jnp.where(row == 2, masked[2], 0.0))).astype(bf16)
    flag = ((lane >= 3 * hd) & (lane < 3 * hd + 3)).astype(f32)
    flag2 = jnp.concatenate([flag, flag], axis=1)

    wt[...] = jnp.transpose(win_ref[...])
    for h in range(heads):
        wk = win_ref[:, fold + h * hd:fold + (h + 1) * hd]
        wka[:, h * 128:(h + 1) * 128] = jnp.concatenate([wk, wk, wk, jnp.zeros_like(wk)], axis=1)

    def project(b, carry):
        rows = pl.ds(pl.multiple_of(b * bq, bq), bq)
        arrive(b)
        xn = norm_rows(load(b))
        keep = jnp.transpose(jnp.broadcast_to(mrow_ref[0:1, rows], (128, bq))) != 0
        keep2 = jnp.concatenate([keep, keep], axis=1)
        for h in range(0, heads, 2):
            k = mm(xn, wka[:, h * 128:(h + 2) * 128])
            k = jnp.where(keep2, k, flag2).astype(bf16)
            kaug[h, rows, :] = k[:, :128]
            kaug[h + 1, rows, :] = k[:, 128:]
        qt = mm(wt[:fold, :], xn, NT).astype(bf16).astype(f32) * c
        hi = qt.astype(bf16)
        rest = qt - hi.astype(f32)
        mid = rest.astype(bf16)
        low = (rest - mid.astype(f32)).astype(bf16)
        vv = mm(wt[2 * fold:3 * fold, :], xn, NT).astype(bf16)
        gg = mm(wt[3 * fold:, :], xn, NT).astype(bf16).astype(f32)
        gg = 1.0 / (1.0 + jnp.exp(-gg))
        for h in range(heads):
            part = slice(h * hd, (h + 1) * hd)
            qaug[h, 0:hd, rows] = hi[part]
            qaug[h, hd:2 * hd, rows] = mid[part]
            qaug[h, 2 * hd:3 * hd, rows] = low[part]
            qaug[h, 3 * hd:, rows] = fill
            vt[h, :, rows] = vv[part]
            sig[h, :, rows] = gg[part]
        return carry

    lax.fori_loop(0, nq, project, 0)

    def fold8(s):
        return s.reshape(kc // 8, 8, bq)

    def chunk_scores(h, q, i, buf, m):
        s = mm(kaug[h, i * kc:(i + 1) * kc, :], q)
        buf[i * kc:(i + 1) * kc, :] = s
        top = jnp.max(fold8(s), axis=0)
        return top if m is None else jnp.maximum(m, top)

    def step(qb, h, cur, nxt, m):
        t = jnp.minimum(qb * heads + h + 1, nq * heads - 1)
        hn = t % heads
        q = qaug[hn, :, pl.ds(pl.multiple_of(t // heads * bq, bq), bq)]
        top = jnp.max(m, axis=0, keepdims=True)
        mn = None
        total = jnp.zeros((8, bq), f32)
        mixed = jnp.zeros((hd, bq), f32)
        held = None
        for i in range(nk):
            mn = chunk_scores(hn, q, i, nxt, mn)
            if held is not None:
                mixed = mixed + mm(vt[h, :, (i - 1) * kc:i * kc], held)
            e = jnp.exp2(cur[i * kc:(i + 1) * kc, :] - top)
            total = total + jnp.sum(fold8(e), axis=0)
            held = e.astype(bf16)
        mixed = mixed + mm(vt[h, :, (nk - 1) * kc:], held)
        cols = pl.ds(pl.multiple_of(qb * bq, bq), bq)
        mixed = mixed / jnp.sum(total, axis=0, keepdims=True)
        gat[pl.ds(pl.multiple_of(h * hd, hd), hd), :] = (mixed * sig[h, :, cols]).astype(bf16)
        return mn

    m = None
    for i in range(nk):
        m = chunk_scores(0, qaug[0, :, 0:bq], i, s0, m)

    def block(qb, m):
        def pair(u, m):
            m = step(qb, 2 * u, s0, s1, m)
            return step(qb, 2 * u + 1, s1, s0, m)

        m = lax.fori_loop(0, heads // 2, pair, m)
        rows = pl.ds(pl.multiple_of(qb * bq, bq), bq)
        y = (load(qb).astype(f32) + mm(gat[...], wout_ref[...], TN)).astype(bf16)
        ac = mm(wopm_ref[...], norm_rows(y), NT).astype(bf16)
        emit(qb, y, (ac.astype(f32) * mrow_ref[0:1, rows]).astype(bf16))
        return m

    lax.fori_loop(0, nq, block, m)


def each(start, stop, one, step=32):
    whole = (stop - start) // step

    def some(i, carry):
        for j in range(step):
            one(start + i * step + j)
        return carry

    lax.fori_loop(0, whole, some, 0)
    for o in range(start + whole * step, stop):
        one(o)


class Links:
    def __init__(self, group, dap, send, recv):
        self.group, self.dap, self.send, self.recv = group, dap, send, recv
        self.me = lax.axis_index('chip') * dap + lax.axis_index('dap')
        self.hi, self.lo = lax.div(self.me, INNER), lax.rem(self.me, INNER)
        self.outer_n = group // INNER

    def greet(self):
        barrier = pltpu.get_barrier_semaphore()

        def one(o):
            t = lax.rem(self.me + o, self.group)
            pl.semaphore_signal(barrier, inc=1, device_id=place(t, self.dap), device_id_type=MESH)

        each(1, self.group, one)

    def ready(self):
        pl.semaphore_wait(pltpu.get_barrier_semaphore(), self.group - 1)

    def copy(self, src, dst, i, t):
        return pltpu.make_async_remote_copy(src_ref=src, dst_ref=dst, send_sem=self.send.at[i], recv_sem=self.recv.at[i],
                                            device_id=place(t, self.dap), device_id_type=MESH)

    def settle(self, part, i):
        done = self.copy(part, part, i, self.me)
        done.wait_send()
        done.wait_recv()

    def to_all(self, make, i):
        def one(o):
            t = lax.rem(self.me + o, self.group)
            src, dst = make(t)
            self.copy(src, dst, i, t).start()

        each(1, self.group, one)

    def to_inner(self, make, i):
        for o in range(1, INNER):
            x = lax.rem(self.lo + o, INNER)
            src, dst = make(x)
            self.copy(src, dst, i, self.hi * INNER + x).start()

    def to_half(self, src, dst, i):
        half = self.outer_n // 2
        base = lax.div(self.hi, half) * half
        for o in range(1, half):
            y = base + lax.rem(lax.rem(self.hi, half) + o, half)
            self.copy(src, dst, i, y * INNER + self.lo).start()

    def to_partner(self, part, i):
        self.copy(part, part, i, lax.rem(self.me + self.group // 2, self.group)).start()


def bias_rows(z, weight):
    rows = mm(weight[...], norm_rows(z), NT).astype(bf16)
    spare = SLOT - rows.shape[0]
    return jnp.concatenate([rows, jnp.zeros((spare, rows.shape[1]), bf16)], axis=0) if spare else rows


def untile(block):
    size = block.shape[0]
    out = jnp.transpose(block)
    row = lax.broadcasted_iota(jnp.int32, (size, size), 0)
    lane = lax.broadcasted_iota(jnp.int32, (size, size), 1)
    step = INNER // 2
    while step:
        low, high = lax.rem(lax.div(row, step), 2), lax.rem(lax.div(lane, step), 2)
        down = pltpu.roll(pltpu.roll(out, size - step, 0), step, 1)
        back = pltpu.roll(pltpu.roll(out, step, 0), size - step, 1)
        out = jnp.where(low == high, out, jnp.where(low < high, down, back))
        step //= 2
    return out


def pair_stage(net, between, collect, z_ref, norm, tnorm, ztbuf, mask_ref, wopm_ref, ws_in, ws_bias, ws_out, we_in, we_bias, we_out, zout,
               abuf, cbuf, oscr, uscr, usend, ubuf, zrow, bsend, bbuf, bscr, esend, ebuf, zsend, zfin):
    me, lo, group, outer_n = net.me, net.lo, net.group, net.outer_n
    blocks, opm = abuf.shape[0], abuf.shape[2]
    heads = ws_bias.shape[0]
    fold = ws_out.shape[0]
    size = z_ref.shape[0]
    keep = jnp.transpose(jnp.broadcast_to(mask_ref[...].astype(f32), (size, size))) != 0

    per = 128 // opm
    outer = None
    for q in range(blocks):
        net.settle(abuf.at[q, pl.ds(0, INNER - 1)], 15 + q)
        net.settle(cbuf.at[q, pl.ds(0, outer_n // 2)], 19 + q)
        term = mm(abuf[q].reshape(INNER * opm, -1), cbuf[q].reshape(outer_n * opm, -1), NT)
        outer = term if outer is None else outer + term
    for g in range(outer_n // per):
        oscr[g] = outer[:, g * 128:(g + 1) * 128]
    lane = lax.broadcasted_iota(jnp.int32, (opm // per * INNER, 128), 1) // opm
    tiles = []
    for g in range(outer_n // per):
        slabs = [jnp.concatenate([oscr[g, pl.ds(b * per + r, INNER, stride=opm), :] for b in range(opm // per)], axis=0)
                 for r in range(per)]
        turned = [[slabs[r] if s == 0 else pltpu.roll(slabs[r], s * opm, 1) for s in range(per)] for r in range(per)]
        for q in range(per):
            pick = turned[0][(0 - q) % per]
            for r in range(1, per):
                pick = jnp.where(lane == r, turned[r][(r - q) % per], pick)
            tiles.append(pick)
    up = None
    for b in range(opm // per):
        block = jnp.concatenate([t[b * INNER:(b + 1) * INNER] for t in tiles], axis=0).astype(bf16)
        term = mm(block, wopm_ref[b * 128:(b + 1) * 128, :])
        up = term if up is None else up + term
    uscr[...] = up
    for x in range(INNER):
        usend[x] = uscr[pl.ds(x, outer_n, stride=INNER), :]
    ubuf[lo] = usend[lo]
    net.to_inner(lambda x: (usend.at[x], ubuf.at[lo]), 3)
    net.settle(ztbuf.at[pl.ds(0, INNER - 1)], 14)
    for x in range(INNER):
        zrow[pl.ds(x, outer_n, stride=INNER), :] = ztbuf[x]
    tile = (zrow[...] + up / (1e-3 + tnorm[...])).astype(bf16)
    bsend[...] = bias_rows(tile, ws_bias)
    bbuf[me] = bsend[...]
    net.to_all(lambda t: (bsend, bbuf.at[me]), 4)
    between()
    net.settle(ubuf.at[pl.ds(0, INNER - 1)], 3)
    for x in range(INNER):
        zrow[pl.ds(x, outer_n, stride=INNER), :] = ubuf[x]
    z1 = (z_ref[...].astype(f32) + zrow[...] / (1e-3 + norm[...])).astype(bf16)

    parts = pair_project(z1, ws_in, fold)
    net.settle(bbuf.at[pl.ds(0, group - 1)], 4)
    bscr[...] = bbuf[...].astype(f32).reshape(group * SLOT, size)
    biases = [untile(bscr[pl.ds(h, size, stride=SLOT), :]) for h in range(heads)]
    z2 = pair_attend(z1, parts, biases, keep, ws_out)

    end_rows = bias_rows(z2, we_bias).astype(f32)
    for h in range(heads):
        bscr[pl.ds(h, size, stride=SLOT), :] = jnp.broadcast_to(end_rows[h:h + 1], (size, size))
    bscr[pl.ds(heads, size, stride=SLOT), :] = z2.astype(f32)
    esend[...] = bscr[...].astype(bf16).reshape(group, SLOT, size)
    ebuf[me] = esend[me]
    net.to_all(lambda t: (esend.at[t], ebuf.at[me]), 5)
    net.settle(ebuf.at[pl.ds(0, group - 1)], 5)
    bscr[...] = ebuf[...].astype(f32).reshape(group * SLOT, size)
    zc = bscr[pl.ds(heads, size, stride=SLOT), :].astype(bf16)
    biases = [bscr[pl.ds(h, size, stride=SLOT), :] for h in range(heads)]
    z3 = pair_attend(zc, pair_project(zc, we_in, fold), biases, keep, we_out)

    zsend[...] = z3.astype(f32)
    zfin[pl.ds(me, 1), :] = zsend[pl.ds(me, 1), :]
    net.to_all(lambda t: (zsend.at[pl.ds(t, 1)], zfin.at[pl.ds(me, 1)]), 6)
    collect()
    net.settle(zfin.at[pl.ds(0, group - 1)], 6)
    zout[...] = zfin[...].astype(bf16)


def row_stage(net, x_ref, z_ref, mask_ref, wb_ref, win_ref, wout_ref, ship, side, stash,
              kk, qt, vt, sig, gat, bias, wt, qd0, qd1, bsend, bbuf, bscr, ytr):
    tokens, width = x_ref.shape
    size = bias.shape[0]
    seqs = tokens // size
    heads = bias.shape[1] // size
    fold = gat.shape[0]
    hd = fold // heads
    c = hd ** -0.5 * LOG2E
    bp = 512
    me, group = net.me, net.group

    net.greet()
    bsend[...] = bias_rows(z_ref[...], wb_ref)
    bbuf[me] = bsend[...]
    wt[...] = jnp.transpose(win_ref[...])
    qd0[...] = jnp.zeros_like(qd0)
    qd1[...] = jnp.zeros_like(qd1)

    def project(b, carry):
        rows = pl.ds(pl.multiple_of(b * bp, bp), bp)
        xn = norm_rows(x_ref[rows, :])
        kk[rows, :] = mm(xn, win_ref[:, fold:2 * fold]).astype(bf16)
        qt[:, rows] = mm(wt[:fold, :], xn, NT).astype(bf16)
        vt[:, rows] = mm(wt[2 * fold:3 * fold, :], xn, NT).astype(bf16)
        gg = mm(wt[3 * fold:, :], xn, NT).astype(bf16).astype(f32)
        sig[:, rows] = 1.0 / (1.0 + jnp.exp(-gg))

        @pl.when(b == 0)
        def _():
            net.ready()
            net.to_all(lambda t: (bsend, bbuf.at[me]), 7)

        return carry

    lax.fori_loop(0, tokens // bp, project, 0)
    slab = heads // 2

    def prescore(s, u, buf, qd):
        cols = pl.ds(pl.multiple_of(s * size, size), size)
        for h in range(heads):
            qd[h * hd:(h + 1) * hd, h * size:(h + 1) * size] = qt[h * hd:(h + 1) * hd, cols]
        for g in range(2):
            out = pl.ds(pl.multiple_of((2 * u + g) * size, size), size)
            buf[out, :] = mm(kk[cols, :], qd[:, g * slab * size:(g + 1) * slab * size]) * c

    for k, buf in enumerate(stash):
        def ahead(u, carry):
            prescore(k * SLOT + 2 * u, 2 * u, buf, qd0)
            prescore(k * SLOT + 2 * u + 1, 2 * u + 1, buf, qd1)
            return carry

        lax.fori_loop(0, SLOT // 2, ahead, 0)
    side()
    net.settle(bbuf.at[pl.ds(0, group - 1)], 7)
    bscr[...] = bbuf[...].astype(f32).reshape(group * SLOT, size)
    for h in range(heads):
        bias[:, h * size:(h + 1) * size] = jnp.transpose(bscr[pl.ds(h, size, stride=SLOT), :] * LOG2E)

    def one(s, u, buf):
        cols = pl.ds(pl.multiple_of(s * size, size), size)
        mrow = mask_ref[pl.ds(me * seqs + s, 1), :]
        keep = jnp.transpose(jnp.broadcast_to(mrow.astype(f32), (size, size))) != 0
        keep2 = jnp.concatenate([keep, keep], axis=1)
        for h in range(0, heads, 2):
            two = slice(h * size, (h + 2) * size)
            rows = pl.ds(pl.multiple_of((2 * u + h // slab) * size, size), size)
            t = buf[rows, h % slab * size:(h % slab + 2) * size] + bias[:, two]
            t = jnp.where(keep2, t, NEG)
            e = jnp.exp2(t - jnp.max(t, axis=0, keepdims=True))
            total = jnp.sum(e, axis=0, keepdims=True)
            mixed = mm(vt[h * hd:(h + 2) * hd, cols], e.astype(bf16)) / total
            gat[h * hd:(h + 1) * hd, cols] = (mixed[:hd, :size] * sig[h * hd:(h + 1) * hd, cols]).astype(bf16)
            gat[(h + 1) * hd:(h + 2) * hd, cols] = (mixed[hd:, size:] * sig[(h + 1) * hd:(h + 2) * hd, cols]).astype(bf16)

    for k, buf in enumerate(stash):
        for j in range(SLOT):
            one(k * SLOT + j, j, buf)
        for b in range(SLOT * size // bp):
            rows = slice((k * SLOT * size // bp + b) * bp, (k * SLOT * size // bp + b + 1) * bp)
            y = (x_ref[rows, :].astype(f32) + mm(gat[:, rows], wout_ref[...], TN)).astype(bf16).astype(f32)
            for i in range(bp // size):
                for half in range(width // 128):
                    ytr[half, pl.ds(b * (bp // size) + i, size, stride=SLOT), :] = (
                        y[i * size:(i + 1) * size, half * 128:(half + 1) * 128])
        ship(k, jnp.concatenate([ytr[half] for half in range(width // 128)], axis=1).astype(bf16))


def block_kernel(group, dap, m_ref, z_ref, mask_ref, res_ref, wr_in, wr_bias, wr_out, wc_in, wc_out, wopm_in, wopm_out,
                 ws_in, ws_bias, ws_out, we_in, we_bias, we_out, mout, zout,
                 kk, qt, rvt, rsig, rgat, bias, rwt, qd0, qd1, rsend, rbuf, rscr, ytr, msend, xbuf, mrow, norm, tnorm, zst, ztbuf, mslot,
                 kaug, qaug, vt, sig, gat, s0, s1, wt, wka, ycol, acs, abuf, cbuf,
                 oscr, uscr, usend, ubuf, zrow, bsend, bbuf, bscr, esend, ebuf, zsend, zfin, send, recv):
    net = Links(group, dap, send, recv)
    me, lo, hi = net.me, net.lo, net.hi
    opm = abuf.shape[2]
    seq, size = mask_ref.shape
    chunks = xbuf.shape[0]
    bq = s0.shape[1]
    per = bq // SLOT
    turns = group // per

    def side():
        zrow[...] = z_ref[...].astype(f32)
        for x in range(INNER):
            zst[x] = zrow[pl.ds(x, group // INNER, stride=INNER), :]
        ztbuf[lo] = zst[lo]
        net.to_inner(lambda x: (zst.at[x], ztbuf.at[lo]), 14)
        row = (lax.broadcasted_iota(jnp.int32, (SLOT, size), 1) == me).astype(bf16)
        split = mask_ref[...].reshape(group, chunks, SLOT, size)
        for k in range(chunks):
            mrow[:, k * group * SLOT:(k + 1) * group * SLOT] = mm(
                row, split[:, k].astype(f32).reshape(group * SLOT, size).astype(bf16), NT)

    def normalisers():
        flags = mask_ref[...].astype(bf16)
        source = lax.broadcasted_iota(jnp.int32, (size, size), 0)
        pair = lax.broadcasted_iota(jnp.int32, (size, size), 1)
        rows_i = mm(flags, (source == hi * INNER + lax.rem(pair, INNER)).astype(bf16))
        rows_j = mm(flags, (source == lax.div(pair, INNER) * INNER + lo).astype(bf16))
        tnorm[...] = jnp.transpose(jnp.broadcast_to(jnp.sum(rows_i * rows_j, axis=0, keepdims=True), (size, size)))
        pick = (lax.broadcasted_iota(jnp.int32, (size, size), 0) == me).astype(bf16)
        norm[...] = mm(flags, mm(flags, pick).astype(bf16), TN)

    def ship(k, y):
        msend[k] = y.astype(f32).reshape(group, SLOT, -1).astype(bf16)
        xbuf[k, me] = msend[k, me]
        net.to_all(lambda t: (msend.at[k, t], xbuf.at[k, me]), 8 + k)

    row_stage(net, m_ref, z_ref, mask_ref, wr_bias, wr_in, wr_out, ship, side, (s0, s1),
              kk, qt, rvt, rsig, rgat, bias, rwt, qd0, qd1, rsend, rbuf, rscr, ytr)

    def arrive(b):
        @pl.when(lax.rem(b, turns) == 0)
        def _():
            k = lax.div(b, turns)
            net.settle(xbuf.at[k, pl.ds(0, group - 1)], 8 + k)

    def load(b):
        part = xbuf[b // turns, pl.ds(pl.multiple_of(b % turns * per, per), per)]
        return part.astype(f32).reshape(bq, -1)

    half = pl.ds(pl.multiple_of(lax.div(hi, net.outer_n // 2) * (net.outer_n // 2), net.outer_n // 2), net.outer_n // 2)

    def pass_on(qb):
        net.settle(cbuf.at[qb, pl.ds(0, net.outer_n // 2 - 1)], 10 + qb)
        net.to_partner(cbuf.at[qb, half], 19 + qb)

    last = cbuf.shape[0] - 1

    def give_back(qb):
        def share_m(o):
            i = lax.rem(me + o, per)
            t = lax.rem(qb, turns) * per + i

            @pl.when(t != me)
            def _():
                net.copy(ycol.at[qb, i], mslot.at[lax.div(qb, turns), me], 2, t).start()

        each(0, per, share_m)

    def collect():
        net.settle(mslot.at[:, pl.ds(0, group - 1)], 2)
        for k in range(chunks):
            y = mslot[k].astype(f32).reshape(group * SLOT, -1)
            for side_half in range(ytr.shape[0]):
                lanes = slice(side_half * 128, (side_half + 1) * 128)
                ytr[side_half] = y[:, lanes]
                for r in range(SLOT):
                    at = (k * SLOT + r) * size
                    mout[at:at + size, lanes] = ytr[side_half, pl.ds(r, size, stride=SLOT), :].astype(bf16)

    def emit(qb, y, ac):
        ycol[qb] = y.astype(f32).reshape(per, SLOT, -1).astype(bf16)
        acs[qb] = ac
        abuf[qb, lo] = ac[:opm]
        cbuf[qb, hi] = ac[opm:]
        net.to_half(acs.at[qb, pl.ds(opm, opm)], cbuf.at[qb, hi], 10 + qb)
        net.to_inner(lambda x: (acs.at[qb, pl.ds(0, opm)], abuf.at[qb, lo]), 15 + qb)

        @pl.when(qb > 0)
        def _():
            pass_on(qb - 1)

        @pl.when(qb < last - 1)
        def _():
            give_back(qb)

    col_stage(arrive, load, seq, mrow, wc_in, wc_out, wopm_in, emit, kaug, qaug, vt, sig, gat, s0, s1, wt, wka)
    for k in range(chunks):
        mslot[k, me] = ycol[k * turns + lax.div(me, per), lax.rem(me, per)]
    normalisers()
    pass_on(last)
    pair_stage(net, lambda: (give_back(last - 1), give_back(last)), collect, z_ref, norm, tnorm, ztbuf, res_ref, wopm_out, ws_in, ws_bias, ws_out, we_in, we_bias, we_out, zout,
               abuf, cbuf, oscr, uscr, usend, ubuf, zrow, bsend, bbuf, bscr, esend, ebuf, zsend, zfin)


def row_scratch(tokens, size, width, z_width, heads, fold, group):
    seqs = tokens // size
    return [
        pltpu.VMEM((tokens, fold), bf16),
        pltpu.VMEM((fold, tokens), bf16),
        pltpu.VMEM((fold, tokens), bf16),
        pltpu.VMEM((fold, tokens), f32),
        pltpu.VMEM((fold, tokens), bf16),
        pltpu.VMEM((size, heads * size), f32),
        pltpu.VMEM((4 * fold, width), bf16),
        pltpu.VMEM((fold, heads * size), bf16),
        pltpu.VMEM((fold, heads * size), bf16),
        pltpu.VMEM((SLOT, size), bf16),
        pltpu.VMEM((group, SLOT, size), bf16),
        pltpu.VMEM((group * SLOT, size), f32),
        pltpu.VMEM((width // 128, SLOT * size, 128), f32),
        pltpu.VMEM((seqs // SLOT, group, SLOT, width), bf16),
        pltpu.VMEM((seqs // SLOT, group, SLOT, width), bf16),
        pltpu.VMEM((SLOT, seqs * group), f32),
        pltpu.VMEM((size, size), f32),
        pltpu.VMEM((size, size), f32),
        pltpu.VMEM((INNER, group // INNER, z_width), f32),
        pltpu.VMEM((INNER, group // INNER, z_width), f32),
        pltpu.VMEM((seqs // SLOT, group, SLOT, width), bf16),
    ]


def col_scratch(seq, width, heads, hd, bq):
    return [
        pltpu.VMEM((heads, seq, 128), bf16),
        pltpu.VMEM((heads, 128, seq), bf16),
        pltpu.VMEM((heads, hd, seq), bf16),
        pltpu.VMEM((heads, hd, seq), f32),
        pltpu.VMEM((heads * hd, bq), bf16),
        pltpu.VMEM((seq, bq), f32),
        pltpu.VMEM((seq, bq), f32),
        pltpu.VMEM((4 * heads * hd, width), bf16),
        pltpu.VMEM((width, heads * 128), bf16),
        pltpu.VMEM((seq // bq, bq // SLOT, SLOT, width), bf16),
    ]


def pair_scratch(seq, size, width, opm, group, bq):
    outer_n = group // INNER
    return [
        pltpu.VMEM((seq // bq, 2 * opm, bq), bf16),
        pltpu.VMEM((seq // bq, INNER, opm, bq), bf16),
        pltpu.VMEM((seq // bq, outer_n, opm, bq), bf16),
        pltpu.VMEM((outer_n * opm // 128, INNER * opm, 128), f32),
        pltpu.VMEM((size, width), f32),
        pltpu.VMEM((INNER, outer_n, width), f32),
        pltpu.VMEM((INNER, outer_n, width), f32),
        pltpu.VMEM((size, width), f32),
        pltpu.VMEM((SLOT, size), bf16),
        pltpu.VMEM((group, SLOT, size), bf16),
        pltpu.VMEM((group * SLOT, size), f32),
        pltpu.VMEM((group, SLOT, size), bf16),
        pltpu.VMEM((group, SLOT, size), bf16),
        pltpu.VMEM((size, width), f32),
        pltpu.VMEM((size, width), f32),
    ]


def block_update(m, z, msa_mask, res_mask, weights, heads, group, dap, bq=512):
    vm = pl.BlockSpec(memory_space=pltpu.VMEM)
    tokens, m_width = m.shape
    size, width = z.shape
    seqs = tokens // size
    seq = seqs * group
    fold = weights[2].shape[0]
    opm = weights[5].shape[0] // 2
    return pl.pallas_call(
        functools.partial(block_kernel, group, dap),
        out_shape=(jax.ShapeDtypeStruct((tokens, m_width), bf16), jax.ShapeDtypeStruct((size, width), bf16)),
        in_specs=[vm] * (4 + len(weights)),
        out_specs=(vm, vm),
        scratch_shapes=row_scratch(tokens, size, m_width, width, heads, fold, group)
        + col_scratch(seq, m_width, heads, fold // heads, bq)
        + pair_scratch(seq, size, width, opm, group, bq)
        + [pltpu.SemaphoreType.DMA((23,)), pltpu.SemaphoreType.DMA((23,))],
        compiler_params=pltpu.CompilerParams(collective_id=1, has_side_effects=True, vmem_limit_bytes=63 << 20),
        name='block_update',
    )(m, z, msa_mask, res_mask, *weights)


def solution(mesh):
    dap_size = mesh.shape['dap']
    group_size = mesh.shape['chip'] * dap_size
    rows = P(('data', 'chip', 'dap'))
    in_specs = (rows, rows, P('data'), P('data')) + (P(),) * 13

    def per_device(m_blk, z_blk, msa_mask, res_mask, w_row_in, w_row_bias, w_row_out, w_col_in, w_col_out,
                   w_opm_in, w_opm_out, w_start_in, w_start_bias, w_start_out, w_end_in, w_end_bias, w_end_out):
        seqs, res, width = m_blk.shape
        weights = (w_row_in, w_row_bias.T, w_row_out, w_col_in, w_col_out, w_opm_in.T, w_opm_out,
                   w_start_in, w_start_bias.T, w_start_out, w_end_in, w_end_bias.T, w_end_out)
        m_out, z_out = block_update(m_blk.reshape(seqs * res, width), z_blk[0], msa_mask, res_mask[None, :], weights,
                                    w_row_bias.shape[1], group_size, dap_size)
        return m_out.reshape(seqs, res, width), z_out[None]

    return jax.shard_map(per_device, mesh=mesh, in_specs=in_specs, out_specs=(rows, rows), check_vma=False)
```

```python
import functools

import jax
import jax.numpy as jnp
import numpy as np
from jax import lax
from jax.experimental import pallas as pl
from jax.experimental.pallas import tpu as pltpu
from jax.sharding import PartitionSpec as P

LOG2E = 1.4426950408889634
f32, bf16 = jnp.float32, jnp.bfloat16


def split3(value):
    parts = []
    rest = np.float64(value)
    for _ in range(3):
        part = np.float64(np.asarray(rest, dtype=jnp.bfloat16))
        parts.append(float(part))
        rest = rest - part
    return parts


def norm_rows(x):
    values = x.astype(f32)
    centred = values - jnp.mean(values, axis=-1, keepdims=True)
    variance = jnp.mean(centred * centred, axis=-1, keepdims=True)
    return (centred * lax.rsqrt(variance + 1e-5)).astype(bf16)


def dot_t(w, x):
    return lax.dot_general(w, x, (((0,), (1,)), ((), ())), preferred_element_type=f32)


NT = (((1,), (1,)), ((), ()))
TN = (((0,), (0,)), ((), ()))
NEG = -1e9 * LOG2E


def mm(a, b, dims=(((1,), (0,)), ((), ()))):
    return lax.dot_general(a, b, dims, preferred_element_type=f32)


NN = (((1,), (0,)), ((), ()))
MESH = pl.DeviceIdType.MESH
INNER = 8
SLOT = 8


def place(t, dap):
    return (0, lax.div(t, dap), lax.rem(t, dap))


def pair_project(x, win_ref, fold):
    xn = norm_rows(x)
    k = mm(xn, win_ref[:, fold:2 * fold]).astype(bf16)
    qt = dot_t(win_ref[:, :fold], xn).astype(bf16)
    vt = dot_t(win_ref[:, 2 * fold:3 * fold], xn).astype(bf16)
    gg = dot_t(win_ref[:, 3 * fold:], xn).astype(bf16).astype(f32)
    return k, qt, vt, 1.0 / (1.0 + jnp.exp(-gg))


def pair_attend(x, parts, biases, keep, wout_ref):
    k, qt, vt, sig = parts
    heads = len(biases)
    hd = vt.shape[0] // heads
    c = hd ** -0.5 * LOG2E
    gated = []
    for h in range(heads):
        part = slice(h * hd, (h + 1) * hd)
        t = mm(k[:, part], qt[part]) * c + biases[h] * LOG2E
        t = jnp.where(keep, t, NEG)
        e = jnp.exp2(t - jnp.max(t, axis=0, keepdims=True))
        mixed = mm(vt[part], e.astype(bf16)) / jnp.sum(e, axis=0, keepdims=True)
        gated.append((mixed * sig[part]).astype(bf16))
    up = mm(jnp.concatenate(gated, axis=0), wout_ref[...], TN)
    return (x.astype(f32) + up).astype(bf16)


def col_stage(arrive, load, seq, mrow_ref, win_ref, wout_ref, wopm_ref, emit,
              kaug, qaug, vt, sig, gat, s0, s1, wt, wka):
    heads, hd = vt.shape[0], vt.shape[1]
    fold = heads * hd
    bq = s0.shape[1]
    nq = seq // bq
    kc = 256
    nk = seq // kc
    c = hd ** -0.5 * LOG2E
    masked = split3(-1e9 * LOG2E)

    lane = lax.broadcasted_iota(jnp.int32, (bq, 128), 1)
    row = lax.broadcasted_iota(jnp.int32, (128 - 3 * hd, bq), 0)
    fill = jnp.where(row == 0, masked[0], jnp.where(row == 1, masked[1], jnp.where(row == 2, masked[2], 0.0))).astype(bf16)
    flag = ((lane >= 3 * hd) & (lane < 3 * hd + 3)).astype(f32)
    flag2 = jnp.concatenate([flag, flag], axis=1)

    wt[...] = jnp.transpose(win_ref[...])
    for h in range(heads):
        wk = win_ref[:, fold + h * hd:fold + (h + 1) * hd]
        wka[:, h * 128:(h + 1) * 128] = jnp.concatenate([wk, wk, wk, jnp.zeros_like(wk)], axis=1)

    def project(b, carry):
        rows = pl.ds(pl.multiple_of(b * bq, bq), bq)
        arrive(b)
        xn = norm_rows(load(b))
        keep = jnp.transpose(jnp.broadcast_to(mrow_ref[0:1, rows], (128, bq))) != 0
        keep2 = jnp.concatenate([keep, keep], axis=1)
        for h in range(0, heads, 2):
            k = mm(xn, wka[:, h * 128:(h + 2) * 128])
            k = jnp.where(keep2, k, flag2).astype(bf16)
            kaug[h, rows, :] = k[:, :128]
            kaug[h + 1, rows, :] = k[:, 128:]
        qt = mm(wt[:fold, :], xn, NT).astype(bf16).astype(f32) * c
        hi = qt.astype(bf16)
        rest = qt - hi.astype(f32)
        mid = rest.astype(bf16)
        low = (rest - mid.astype(f32)).astype(bf16)
        vv = mm(wt[2 * fold:3 * fold, :], xn, NT).astype(bf16)
        gg = mm(wt[3 * fold:, :], xn, NT).astype(bf16).astype(f32)
        gg = 1.0 / (1.0 + jnp.exp(-gg))
        for h in range(heads):
            part = slice(h * hd, (h + 1) * hd)
            qaug[h, 0:hd, rows] = hi[part]
            qaug[h, hd:2 * hd, rows] = mid[part]
            qaug[h, 2 * hd:3 * hd, rows] = low[part]
            qaug[h, 3 * hd:, rows] = fill
            vt[h, :, rows] = vv[part]
            sig[h, :, rows] = gg[part]
        return carry

    lax.fori_loop(0, nq, project, 0)

    def fold8(s):
        return s.reshape(kc // 8, 8, bq)

    def chunk_scores(h, q, i, buf, m):
        s = mm(kaug[h, i * kc:(i + 1) * kc, :], q)
        buf[i * kc:(i + 1) * kc, :] = s
        top = jnp.max(fold8(s), axis=0)
        return top if m is None else jnp.maximum(m, top)

    def step(qb, h, cur, nxt, m):
        t = jnp.minimum(qb * heads + h + 1, nq * heads - 1)
        hn = t % heads
        q = qaug[hn, :, pl.ds(pl.multiple_of(t // heads * bq, bq), bq)]
        top = jnp.max(m, axis=0, keepdims=True)
        mn = None
        total = jnp.zeros((8, bq), f32)
        mixed = jnp.zeros((hd, bq), f32)
        held = None
        for i in range(nk):
            mn = chunk_scores(hn, q, i, nxt, mn)
            if held is not None:
                mixed = mixed + mm(vt[h, :, (i - 1) * kc:i * kc], held)
            e = jnp.exp2(cur[i * kc:(i + 1) * kc, :] - top)
            total = total + jnp.sum(fold8(e), axis=0)
            held = e.astype(bf16)
        mixed = mixed + mm(vt[h, :, (nk - 1) * kc:], held)
        cols = pl.ds(pl.multiple_of(qb * bq, bq), bq)
        mixed = mixed / jnp.sum(total, axis=0, keepdims=True)
        gat[pl.ds(pl.multiple_of(h * hd, hd), hd), :] = (mixed * sig[h, :, cols]).astype(bf16)
        return mn

    m = None
    for i in range(nk):
        m = chunk_scores(0, qaug[0, :, 0:bq], i, s0, m)

    def block(qb, m):
        def pair(u, m):
            m = step(qb, 2 * u, s0, s1, m)
            return step(qb, 2 * u + 1, s1, s0, m)

        m = lax.fori_loop(0, heads // 2, pair, m)
        rows = pl.ds(pl.multiple_of(qb * bq, bq), bq)
        y = (load(qb).astype(f32) + mm(gat[...], wout_ref[...], TN)).astype(bf16)
        ac = mm(wopm_ref[...], norm_rows(y), NT).astype(bf16)
        emit(qb, y, (ac.astype(f32) * mrow_ref[0:1, rows]).astype(bf16))
        return m

    lax.fori_loop(0, nq, block, m)


def each(start, stop, one, step=32):
    whole = (stop - start) // step

    def some(i, carry):
        for j in range(step):
            one(start + i * step + j)
        return carry

    lax.fori_loop(0, whole, some, 0)
    for o in range(start + whole * step, stop):
        one(o)


class Links:
    def __init__(self, group, dap, send, recv):
        self.group, self.dap, self.send, self.recv = group, dap, send, recv
        self.me = lax.axis_index('chip') * dap + lax.axis_index('dap')
        self.hi, self.lo = lax.div(self.me, INNER), lax.rem(self.me, INNER)
        self.outer_n = group // INNER

    def greet(self):
        barrier = pltpu.get_barrier_semaphore()

        def one(o):
            t = lax.rem(self.me + o, self.group)
            pl.semaphore_signal(barrier, inc=1, device_id=place(t, self.dap), device_id_type=MESH)

        each(1, self.group, one)

    def ready(self):
        pl.semaphore_wait(pltpu.get_barrier_semaphore(), self.group - 1)

    def copy(self, src, dst, i, t):
        return pltpu.make_async_remote_copy(src_ref=src, dst_ref=dst, send_sem=self.send.at[i], recv_sem=self.recv.at[i],
                                            device_id=place(t, self.dap), device_id_type=MESH)

    def settle(self, part, i):
        done = self.copy(part, part, i, self.me)
        done.wait_send()
        done.wait_recv()

    def to_all(self, make, i):
        def one(o):
            t = lax.rem(self.me + o, self.group)
            src, dst = make(t)
            self.copy(src, dst, i, t).start()

        each(1, self.group, one)

    def to_inner(self, make, i):
        for o in range(1, INNER):
            x = lax.rem(self.lo + o, INNER)
            src, dst = make(x)
            self.copy(src, dst, i, self.hi * INNER + x).start()

    def to_half(self, src, dst, i):
        half = self.outer_n // 2
        base = lax.div(self.hi, half) * half
        for o in range(1, half):
            y = base + lax.rem(lax.rem(self.hi, half) + o, half)
            self.copy(src, dst, i, y * INNER + self.lo).start()

    def to_partner(self, part, i):
        self.copy(part, part, i, lax.rem(self.me + self.group // 2, self.group)).start()


def bias_rows(z, weight):
    rows = mm(weight[...], norm_rows(z), NT).astype(bf16)
    spare = SLOT - rows.shape[0]
    return jnp.concatenate([rows, jnp.zeros((spare, rows.shape[1]), bf16)], axis=0) if spare else rows


def untile(block):
    size = block.shape[0]
    out = jnp.transpose(block)
    row = lax.broadcasted_iota(jnp.int32, (size, size), 0)
    lane = lax.broadcasted_iota(jnp.int32, (size, size), 1)
    step = INNER // 2
    while step:
        low, high = lax.rem(lax.div(row, step), 2), lax.rem(lax.div(lane, step), 2)
        down = pltpu.roll(pltpu.roll(out, size - step, 0), step, 1)
        back = pltpu.roll(pltpu.roll(out, step, 0), size - step, 1)
        out = jnp.where(low == high, out, jnp.where(low < high, down, back))
        step //= 2
    return out


def pair_stage(net, between, collect, z_ref, norm, tnorm, ztbuf, mask_ref, wopm_ref, ws_in, ws_bias, ws_out, we_in, we_bias, we_out, zout,
               abuf, cbuf, oscr, uscr, usend, ubuf, zrow, bsend, bbuf, bscr, esend, ebuf, zsend, zfin):
    me, lo, group, outer_n = net.me, net.lo, net.group, net.outer_n
    blocks, opm = abuf.shape[0], abuf.shape[2]
    heads = ws_bias.shape[0]
    fold = ws_out.shape[0]
    size = z_ref.shape[0]
    keep = jnp.transpose(jnp.broadcast_to(mask_ref[...].astype(f32), (size, size))) != 0

    per = 128 // opm
    outer = None
    for q in range(blocks):
        net.settle(abuf.at[q, pl.ds(0, INNER - 1)], 15 + q)
        net.settle(cbuf.at[q, pl.ds(0, outer_n // 2)], 19 + q)
        term = mm(abuf[q].reshape(INNER * opm, -1), cbuf[q].reshape(outer_n * opm, -1), NT)
        outer = term if outer is None else outer + term
    for g in range(outer_n // per):
        oscr[g] = outer[:, g * 128:(g + 1) * 128]
    lane = lax.broadcasted_iota(jnp.int32, (opm // per * INNER, 128), 1) // opm
    tiles = []
    for g in range(outer_n // per):
        slabs = [jnp.concatenate([oscr[g, pl.ds(b * per + r, INNER, stride=opm), :] for b in range(opm // per)], axis=0)
                 for r in range(per)]
        turned = [[slabs[r] if s == 0 else pltpu.roll(slabs[r], s * opm, 1) for s in range(per)] for r in range(per)]
        for q in range(per):
            pick = turned[0][(0 - q) % per]
            for r in range(1, per):
                pick = jnp.where(lane == r, turned[r][(r - q) % per], pick)
            tiles.append(pick)
    up = None
    for b in range(opm // per):
        block = jnp.concatenate([t[b * INNER:(b + 1) * INNER] for t in tiles], axis=0).astype(bf16)
        term = mm(block, wopm_ref[b * 128:(b + 1) * 128, :])
        up = term if up is None else up + term
    uscr[...] = up
    for x in range(INNER):
        usend[x] = uscr[pl.ds(x, outer_n, stride=INNER), :]
    ubuf[lo] = usend[lo]
    net.to_inner(lambda x: (usend.at[x], ubuf.at[lo]), 3)
    net.settle(ztbuf.at[pl.ds(0, INNER - 1)], 14)
    for x in range(INNER):
        zrow[pl.ds(x, outer_n, stride=INNER), :] = ztbuf[x]
    tile = (zrow[...] + up / (1e-3 + tnorm[...])).astype(bf16)
    bsend[...] = bias_rows(tile, ws_bias)
    bbuf[me] = bsend[...]
    net.to_all(lambda t: (bsend, bbuf.at[me]), 4)
    between()
    net.settle(ubuf.at[pl.ds(0, INNER - 1)], 3)
    for x in range(INNER):
        zrow[pl.ds(x, outer_n, stride=INNER), :] = ubuf[x]
    z1 = (z_ref[...].astype(f32) + zrow[...] / (1e-3 + norm[...])).astype(bf16)

    parts = pair_project(z1, ws_in, fold)
    net.settle(bbuf.at[pl.ds(0, group - 1)], 4)
    bscr[...] = bbuf[...].astype(f32).reshape(group * SLOT, size)
    biases = [untile(bscr[pl.ds(h, size, stride=SLOT), :]) for h in range(heads)]
    z2 = pair_attend(z1, parts, biases, keep, ws_out)

    end_rows = bias_rows(z2, we_bias).astype(f32)
    for h in range(heads):
        bscr[pl.ds(h, size, stride=SLOT), :] = jnp.broadcast_to(end_rows[h:h + 1], (size, size))
    bscr[pl.ds(heads, size, stride=SLOT), :] = z2.astype(f32)
    esend[...] = bscr[...].astype(bf16).reshape(group, SLOT, size)
    ebuf[me] = esend[me]
    net.to_all(lambda t: (esend.at[t], ebuf.at[me]), 5)
    net.settle(ebuf.at[pl.ds(0, group - 1)], 5)
    bscr[...] = ebuf[...].astype(f32).reshape(group * SLOT, size)
    zc = bscr[pl.ds(heads, size, stride=SLOT), :].astype(bf16)
    biases = [bscr[pl.ds(h, size, stride=SLOT), :] for h in range(heads)]
    z3 = pair_attend(zc, pair_project(zc, we_in, fold), biases, keep, we_out)

    zsend[...] = z3.astype(f32)
    zfin[pl.ds(me, 1), :] = zsend[pl.ds(me, 1), :]
    net.to_all(lambda t: (zsend.at[pl.ds(t, 1)], zfin.at[pl.ds(me, 1)]), 6)
    collect()
    net.settle(zfin.at[pl.ds(0, group - 1)], 6)
    zout[...] = zfin[...].astype(bf16)


def row_stage(net, x_ref, z_ref, mask_ref, wb_ref, win_ref, wout_ref, ship, side, stash,
              kk, qt, vt, sig, gat, bias, wt, qd0, qd1, bsend, bbuf, bscr, ytr):
    tokens, width = x_ref.shape
    size = bias.shape[0]
    seqs = tokens // size
    heads = bias.shape[1] // size
    fold = gat.shape[0]
    hd = fold // heads
    c = hd ** -0.5 * LOG2E
    bp = 512
    me, group = net.me, net.group

    net.greet()
    bsend[...] = bias_rows(z_ref[...], wb_ref)
    bbuf[me] = bsend[...]
    wt[...] = jnp.transpose(win_ref[...])
    qd0[...] = jnp.zeros_like(qd0)
    qd1[...] = jnp.zeros_like(qd1)

    def project(b, carry):
        rows = pl.ds(pl.multiple_of(b * bp, bp), bp)
        xn = norm_rows(x_ref[rows, :])
        kk[rows, :] = mm(xn, win_ref[:, fold:2 * fold]).astype(bf16)
        qt[:, rows] = mm(wt[:fold, :], xn, NT).astype(bf16)
        vt[:, rows] = mm(wt[2 * fold:3 * fold, :], xn, NT).astype(bf16)
        gg = mm(wt[3 * fold:, :], xn, NT).astype(bf16).astype(f32)
        sig[:, rows] = 1.0 / (1.0 + jnp.exp(-gg))

        @pl.when(b == 0)
        def _():
            net.ready()
            net.to_all(lambda t: (bsend, bbuf.at[me]), 7)

        return carry

    lax.fori_loop(0, tokens // bp, project, 0)
    slab = heads // 2

    def prescore(s, u, buf, qd):
        cols = pl.ds(pl.multiple_of(s * size, size), size)
        for h in range(heads):
            qd[h * hd:(h + 1) * hd, h * size:(h + 1) * size] = qt[h * hd:(h + 1) * hd, cols]
        for g in range(2):
            out = pl.ds(pl.multiple_of((2 * u + g) * size, size), size)
            buf[out, :] = mm(kk[cols, :], qd[:, g * slab * size:(g + 1) * slab * size]) * c

    for k, buf in enumerate(stash):
        for j in range(SLOT):
            prescore(k * SLOT + j, j, buf, (qd0, qd1)[j % 2])

    side()
    net.settle(bbuf.at[pl.ds(0, group - 1)], 7)
    bscr[...] = bbuf[...].astype(f32).reshape(group * SLOT, size)
    for h in range(heads):
        bias[:, h * size:(h + 1) * size] = jnp.transpose(bscr[pl.ds(h, size, stride=SLOT), :] * LOG2E)

    def one(s, u, buf):
        cols = pl.ds(pl.multiple_of(s * size, size), size)
        mrow = mask_ref[pl.ds(me * seqs + s, 1), :]
        keep = jnp.transpose(jnp.broadcast_to(mrow.astype(f32), (size, size))) != 0
        keep2 = jnp.concatenate([keep, keep], axis=1)
        for h in range(0, heads, 2):
            two = slice(h * size, (h + 2) * size)
            rows = pl.ds(pl.multiple_of((2 * u + h // slab) * size, size), size)
            t = buf[rows, h % slab * size:(h % slab + 2) * size] + bias[:, two]
            t = jnp.where(keep2, t, NEG)
            e = jnp.exp2(t - jnp.max(t, axis=0, keepdims=True))
            total = jnp.sum(e, axis=0, keepdims=True)
            mixed = mm(vt[h * hd:(h + 2) * hd, cols], e.astype(bf16)) / total
            gat[h * hd:(h + 1) * hd, cols] = (mixed[:hd, :size] * sig[h * hd:(h + 1) * hd, cols]).astype(bf16)
            gat[(h + 1) * hd:(h + 2) * hd, cols] = (mixed[hd:, size:] * sig[(h + 1) * hd:(h + 2) * hd, cols]).astype(bf16)

    for k, buf in enumerate(stash):
        for j in range(SLOT):
            one(k * SLOT + j, j, buf)
        for b in range(SLOT * size // bp):
            rows = slice((k * SLOT * size // bp + b) * bp, (k * SLOT * size // bp + b + 1) * bp)
            y = (x_ref[rows, :].astype(f32) + mm(gat[:, rows], wout_ref[...], TN)).astype(bf16).astype(f32)
            for i in range(bp // size):
                for half in range(width // 128):
                    ytr[half, pl.ds(b * (bp // size) + i, size, stride=SLOT), :] = (
                        y[i * size:(i + 1) * size, half * 128:(half + 1) * 128])
        ship(k, jnp.concatenate([ytr[half] for half in range(width // 128)], axis=1).astype(bf16))


def block_kernel(group, dap, m_ref, z_ref, mask_ref, res_ref, wr_in, wr_bias, wr_out, wc_in, wc_out, wopm_in, wopm_out,
                 ws_in, ws_bias, ws_out, we_in, we_bias, we_out, mout, zout,
                 kk, qt, rvt, rsig, rgat, bias, rwt, qd0, qd1, rsend, rbuf, rscr, ytr, msend, xbuf, mrow, norm, tnorm, zst, ztbuf, mslot,
                 kaug, qaug, vt, sig, gat, s0, s1, wt, wka, ycol, acs, abuf, cbuf,
                 oscr, uscr, usend, ubuf, zrow, bsend, bbuf, bscr, esend, ebuf, zsend, zfin, send, recv):
    net = Links(group, dap, send, recv)
    me, lo, hi = net.me, net.lo, net.hi
    opm = abuf.shape[2]
    seq, size = mask_ref.shape
    chunks = xbuf.shape[0]
    bq = s0.shape[1]
    per = bq // SLOT
    turns = group // per

    def side():
        zrow[...] = z_ref[...].astype(f32)
        for x in range(INNER):
            zst[x] = zrow[pl.ds(x, group // INNER, stride=INNER), :]
        ztbuf[lo] = zst[lo]
        net.to_inner(lambda x: (zst.at[x], ztbuf.at[lo]), 14)
        row = (lax.broadcasted_iota(jnp.int32, (SLOT, size), 1) == me).astype(bf16)
        split = mask_ref[...].reshape(group, chunks, SLOT, size)
        for k in range(chunks):
            mrow[:, k * group * SLOT:(k + 1) * group * SLOT] = mm(
                row, split[:, k].astype(f32).reshape(group * SLOT, size).astype(bf16), NT)

    def normalisers():
        flags = mask_ref[...].astype(bf16)
        source = lax.broadcasted_iota(jnp.int32, (size, size), 0)
        pair = lax.broadcasted_iota(jnp.int32, (size, size), 1)
        rows_i = mm(flags, (source == hi * INNER + lax.rem(pair, INNER)).astype(bf16))
        rows_j = mm(flags, (source == lax.div(pair, INNER) * INNER + lo).astype(bf16))
        tnorm[...] = jnp.transpose(jnp.broadcast_to(jnp.sum(rows_i * rows_j, axis=0, keepdims=True), (size, size)))
        pick = (lax.broadcasted_iota(jnp.int32, (size, size), 0) == me).astype(bf16)
        norm[...] = mm(flags, mm(flags, pick).astype(bf16), TN)

    def ship(k, y):
        msend[k] = y.astype(f32).reshape(group, SLOT, -1).astype(bf16)
        xbuf[k, me] = msend[k, me]
        net.to_all(lambda t: (msend.at[k, t], xbuf.at[k, me]), 8 + k)

    row_stage(net, m_ref, z_ref, mask_ref, wr_bias, wr_in, wr_out, ship, side, (s0, s1),
              kk, qt, rvt, rsig, rgat, bias, rwt, qd0, qd1, rsend, rbuf, rscr, ytr)

    def arrive(b):
        @pl.when(lax.rem(b, turns) == 0)
        def _():
            k = lax.div(b, turns)
            net.settle(xbuf.at[k, pl.ds(0, group - 1)], 8 + k)

    def load(b):
        part = xbuf[b // turns, pl.ds(pl.multiple_of(b % turns * per, per), per)]
        return part.astype(f32).reshape(bq, -1)

    half = pl.ds(pl.multiple_of(lax.div(hi, net.outer_n // 2) * (net.outer_n // 2), net.outer_n // 2), net.outer_n // 2)

    def pass_on(qb):
        net.settle(cbuf.at[qb, pl.ds(0, net.outer_n // 2 - 1)], 10 + qb)
        net.to_partner(cbuf.at[qb, half], 19 + qb)

    last = cbuf.shape[0] - 1

    def give_back(qb):
        def share_m(o):
            i = lax.rem(me + o, per)
            t = lax.rem(qb, turns) * per + i

            @pl.when(t != me)
            def _():
                net.copy(ycol.at[qb, i], mslot.at[lax.div(qb, turns), me], 2, t).start()

        each(0, per, share_m)

    def collect():
        net.settle(mslot.at[:, pl.ds(0, group - 1)], 2)
        for k in range(chunks):
            y = mslot[k].astype(f32).reshape(group * SLOT, -1)
            for side_half in range(ytr.shape[0]):
                lanes = slice(side_half * 128, (side_half + 1) * 128)
                ytr[side_half] = y[:, lanes]
                for r in range(SLOT):
                    at = (k * SLOT + r) * size
                    mout[at:at + size, lanes] = ytr[side_half, pl.ds(r, size, stride=SLOT), :].astype(bf16)

    def emit(qb, y, ac):
        ycol[qb] = y.astype(f32).reshape(per, SLOT, -1).astype(bf16)
        acs[qb] = ac
        abuf[qb, lo] = ac[:opm]
        cbuf[qb, hi] = ac[opm:]
        net.to_half(acs.at[qb, pl.ds(opm, opm)], cbuf.at[qb, hi], 10 + qb)
        net.to_inner(lambda x: (acs.at[qb, pl.ds(0, opm)], abuf.at[qb, lo]), 15 + qb)

        @pl.when(qb > 0)
        def _():
            pass_on(qb - 1)

        @pl.when(qb < last - 1)
        def _():
            give_back(qb)

    col_stage(arrive, load, seq, mrow, wc_in, wc_out, wopm_in, emit, kaug, qaug, vt, sig, gat, s0, s1, wt, wka)
    for k in range(chunks):
        mslot[k, me] = ycol[k * turns + lax.div(me, per), lax.rem(me, per)]
    normalisers()
    pass_on(last)
    pair_stage(net, lambda: (give_back(last - 1), give_back(last)), collect, z_ref, norm, tnorm, ztbuf, res_ref, wopm_out, ws_in, ws_bias, ws_out, we_in, we_bias, we_out, zout,
               abuf, cbuf, oscr, uscr, usend, ubuf, zrow, bsend, bbuf, bscr, esend, ebuf, zsend, zfin)


def row_scratch(tokens, size, width, z_width, heads, fold, group):
    seqs = tokens // size
    return [
        pltpu.VMEM((tokens, fold), bf16),
        pltpu.VMEM((fold, tokens), bf16),
        pltpu.VMEM((fold, tokens), bf16),
        pltpu.VMEM((fold, tokens), f32),
        pltpu.VMEM((fold, tokens), bf16),
        pltpu.VMEM((size, heads * size), f32),
        pltpu.VMEM((4 * fold, width), bf16),
        pltpu.VMEM((fold, heads * size), bf16),
        pltpu.VMEM((fold, heads * size), bf16),
        pltpu.VMEM((SLOT, size), bf16),
        pltpu.VMEM((group, SLOT, size), bf16),
        pltpu.VMEM((group * SLOT, size), f32),
        pltpu.VMEM((width // 128, SLOT * size, 128), f32),
        pltpu.VMEM((seqs // SLOT, group, SLOT, width), bf16),
        pltpu.VMEM((seqs // SLOT, group, SLOT, width), bf16),
        pltpu.VMEM((SLOT, seqs * group), f32),
        pltpu.VMEM((size, size), f32),
        pltpu.VMEM((size, size), f32),
        pltpu.VMEM((INNER, group // INNER, z_width), f32),
        pltpu.VMEM((INNER, group // INNER, z_width), f32),
        pltpu.VMEM((seqs // SLOT, group, SLOT, width), bf16),
    ]


def col_scratch(seq, width, heads, hd, bq):
    return [
        pltpu.VMEM((heads, seq, 128), bf16),
        pltpu.VMEM((heads, 128, seq), bf16),
        pltpu.VMEM((heads, hd, seq), bf16),
        pltpu.VMEM((heads, hd, seq), f32),
        pltpu.VMEM((heads * hd, bq), bf16),
        pltpu.VMEM((seq, bq), f32),
        pltpu.VMEM((seq, bq), f32),
        pltpu.VMEM((4 * heads * hd, width), bf16),
        pltpu.VMEM((width, heads * 128), bf16),
        pltpu.VMEM((seq // bq, bq // SLOT, SLOT, width), bf16),
    ]


def pair_scratch(seq, size, width, opm, group, bq):
    outer_n = group // INNER
    return [
        pltpu.VMEM((seq // bq, 2 * opm, bq), bf16),
        pltpu.VMEM((seq // bq, INNER, opm, bq), bf16),
        pltpu.VMEM((seq // bq, outer_n, opm, bq), bf16),
        pltpu.VMEM((outer_n * opm // 128, INNER * opm, 128), f32),
        pltpu.VMEM((size, width), f32),
        pltpu.VMEM((INNER, outer_n, width), f32),
        pltpu.VMEM((INNER, outer_n, width), f32),
        pltpu.VMEM((size, width), f32),
        pltpu.VMEM((SLOT, size), bf16),
        pltpu.VMEM((group, SLOT, size), bf16),
        pltpu.VMEM((group * SLOT, size), f32),
        pltpu.VMEM((group, SLOT, size), bf16),
        pltpu.VMEM((group, SLOT, size), bf16),
        pltpu.VMEM((size, width), f32),
        pltpu.VMEM((size, width), f32),
    ]


def block_update(m, z, msa_mask, res_mask, weights, heads, group, dap, bq=512):
    vm = pl.BlockSpec(memory_space=pltpu.VMEM)
    tokens, m_width = m.shape
    size, width = z.shape
    seqs = tokens // size
    seq = seqs * group
    fold = weights[2].shape[0]
    opm = weights[5].shape[0] // 2
    return pl.pallas_call(
        functools.partial(block_kernel, group, dap),
        out_shape=(jax.ShapeDtypeStruct((tokens, m_width), bf16), jax.ShapeDtypeStruct((size, width), bf16)),
        in_specs=[vm] * (4 + len(weights)),
        out_specs=(vm, vm),
        scratch_shapes=row_scratch(tokens, size, m_width, width, heads, fold, group)
        + col_scratch(seq, m_width, heads, fold // heads, bq)
        + pair_scratch(seq, size, width, opm, group, bq)
        + [pltpu.SemaphoreType.DMA((23,)), pltpu.SemaphoreType.DMA((23,))],
        compiler_params=pltpu.CompilerParams(collective_id=1, has_side_effects=True, vmem_limit_bytes=63 << 20),
        name='block_update',
    )(m, z, msa_mask, res_mask, *weights)


def solution(mesh):
    dap_size = mesh.shape['dap']
    group_size = mesh.shape['chip'] * dap_size
    rows = P(('data', 'chip', 'dap'))
    in_specs = (rows, rows, P('data'), P('data')) + (P(),) * 13

    def per_device(m_blk, z_blk, msa_mask, res_mask, w_row_in, w_row_bias, w_row_out, w_col_in, w_col_out,
                   w_opm_in, w_opm_out, w_start_in, w_start_bias, w_start_out, w_end_in, w_end_bias, w_end_out):
        seqs, res, width = m_blk.shape
        weights = (w_row_in, w_row_bias.T, w_row_out, w_col_in, w_col_out, w_opm_in.T, w_opm_out,
                   w_start_in, w_start_bias.T, w_start_out, w_end_in, w_end_bias.T, w_end_out)
        m_out, z_out = block_update(m_blk.reshape(seqs * res, width), z_blk[0], msa_mask, res_mask[None, :], weights,
                                    w_row_bias.shape[1], group_size, dap_size)
        return m_out.reshape(seqs, res, width), z_out[None]

    return jax.shard_map(per_device, mesh=mesh, in_specs=in_specs, out_specs=(rows, rows), check_vma=False)
```
